8 devices in a mesh: dp: 1 (over z), tp: 8 (over y, x, core).
Axes of the slice: x: 2, y: 2, z: 1, core: 2. Of those that a mesh axis runs over, the one named last changes fastest.
Arguments:
- ids: int32 [4, 256], P('dp')
- emb: bfloat16 [65536, 3072], P('tp')
- g: bfloat16 [3072], replicated
- w: bfloat16 [3072, 5120], P(None, 'tp')
- du: bfloat16 [4, 256, 5120], P('dp', None, 'tp')
- dres: bfloat16 [4, 256, 3072], P('dp', 'tp')
Outputs:
- output 1: bfloat16 [4, 256, 5120], P('dp', None, 'tp')
- output 2: bfloat16 [4, 256, 3072], P('dp', 'tp')
- output 3: float32 [65536, 3072], P(('dp', 'tp'))
- output 4: float32 [3072, 5120], P(None, ('dp', 'tp'))
- output 5: float32 [3072], P('dp')
All inputs are finite; a program needn't handle non-finite values.
Results may differ from the reference program's by a relative error of at most 0.00621165.
Values are sent between devices in bfloat16 or wider.
A program may use at most 1 GiB of HBM per device.

```python
import jax
import jax.numpy as jnp
from jax import lax

K = 4
T = 256
V = 65536
D = 3072
FC = 5120
GROUP = 8
EPS = 1e-6
NPOOL = K * T // 16
FCG = FC // GROUP


def setup_inputs(seed: int = 0, part: int = 0) -> dict:
    key = jax.random.key(seed)
    kp = jax.random.fold_in(key, part)
    ke, kg, kw = jax.random.split(key, 3)
    k1, k2, k3, k4, k5, k6 = jax.random.split(kp, 6)
    ka, kb, kc = jax.random.split(jax.random.fold_in(kp, 7), 3)
    a = jax.random.randint(ka, (K, T), 0, V)
    b = jax.random.randint(kb, (K, T), 0, V)
    coin = jax.random.bernoulli(kc, 0.4, (K, T))
    ids = jnp.where(coin, a, jnp.minimum(a, b)).astype(jnp.int32)
    emb = jax.random.normal(ke, (V, D), jnp.float32).astype(jnp.bfloat16)
    g = (1.0 + 0.5 * jax.random.normal(kg, (D,), jnp.float32)).astype(jnp.bfloat16)
    w = (jax.random.normal(kw, (D, FC), jnp.float32) * D ** -0.5).astype(jnp.bfloat16)
    du = (jax.random.normal(k5, (K, T, FC), jnp.float32) * (D / FC) ** 0.5).astype(jnp.bfloat16)
    dres = jax.random.normal(k6, (K, T, D), jnp.float32).astype(jnp.bfloat16)
    return {"ids": ids, "emb": emb, "g": g, "w": w, "du": du, "dres": dres}


def reference(ids, emb, g, w, du, dres):
    gf = g.astype(jnp.float32)

    def micro(carry, inp):
        de, dw, dg = carry
        idm, dum, drm = inp
        x = emb[idm]
        xf = x.astype(jnp.float32)
        rs = lax.rsqrt(jnp.mean(xf * xf, axis=-1, keepdims=True) + EPS)
        nh = xf * rs
        n = (nh * gf).astype(jnp.bfloat16)
        u = jnp.dot(n, w, preferred_element_type=jnp.float32).astype(jnp.bfloat16)
        dn = jnp.zeros((T, D), jnp.float32)
        for j in range(GROUP):
            pb = jnp.dot(dum[:, j * FCG:(j + 1) * FCG], w[:, j * FCG:(j + 1) * FCG].T, preferred_element_type=jnp.float32)
            dn = dn + pb.astype(jnp.bfloat16).astype(jnp.float32)
        gdn = gf * dn
        dxn = rs * (gdn - nh * jnp.mean(nh * gdn, axis=-1, keepdims=True))
        dx = (drm.astype(jnp.float32) + dxn).astype(jnp.bfloat16)
        de = de.at[idm].add(dx.astype(jnp.float32))
        dw = dw + jnp.dot(n.T, dum, preferred_element_type=jnp.float32)
        dg = dg + jnp.sum(dn * nh, axis=0)
        return (de, dw, dg), (u, x)

    init = (jnp.zeros((V, D), jnp.float32), jnp.zeros((D, FC), jnp.float32), jnp.zeros((D,), jnp.float32))
    (de, dw, dg), (u, x) = lax.scan(micro, init, (ids, du, dres))
    return u, x, de, dw, dg
```

```python
import jax
import jax.numpy as jnp
from jax import lax
from jax.experimental import pallas as pl
from jax.experimental.pallas import tpu as pltpu
from jax.sharding import PartitionSpec as P

EPS = 1e-6
ANY = pl.BlockSpec(memory_space=pl.ANY)
VMEM = pl.BlockSpec(memory_space=pltpu.VMEM)
SMEM = pl.BlockSpec(memory_space=pltpu.SMEM)
ZR = 256
BLK = 128


def zero_kernel(de, z, sem):
    z[...] = jnp.zeros_like(z)
    steps = de.shape[0] // ZR

    def copy(i):
        return pltpu.make_async_copy(z, de.at[pl.ds(pl.multiple_of(i * ZR, ZR), ZR)], sem)

    pl.loop(0, steps)(lambda i: copy(i).start())
    pl.loop(0, steps)(lambda i: copy(i).wait())


def pull(me, blocks, buf, sem):
    tl = blocks[0].shape[1]
    copies = []
    for j, b in enumerate(blocks):
        s = pl.multiple_of(jnp.bitwise_xor(me, j) * tl, tl)
        copies.append(pltpu.make_async_copy(b, buf.at[:, pl.ds(s, tl), :], sem.at[j]))
    for c in copies:
        c.start()
    for c in copies:
        c.wait()


def proj_kernel(me_ref, g_ref, w_ref, du_ref, *refs):
    blocks, (u_ref, dw_ref, buf, sem) = refs[:8], refs[8:]
    mb, t, d = buf.shape
    pull(me_ref[0], blocks, buf, sem)
    gf = g_ref[...].astype(jnp.float32)
    rows = 32

    @pl.loop(0, mb * t // rows)
    def _(i):
        m, r = i // (t // rows), i % (t // rows)
        at = (m, pl.ds(pl.multiple_of(r * rows, rows), rows), slice(None))
        xf = buf[at].astype(jnp.float32)
        rs = lax.rsqrt(jnp.mean(xf * xf, axis=-1, keepdims=True) + EPS)
        buf[at] = (xf * rs * gf).astype(jnp.bfloat16)

    @pl.loop(0, mb)
    def _(m):
        u_ref[m] = jnp.dot(buf[m], w_ref[...], preferred_element_type=jnp.float32).astype(jnp.bfloat16)

    dc = 256

    @pl.loop(0, d // dc)
    def _(i):
        c = pl.ds(pl.multiple_of(i * dc, dc), dc)
        acc = jnp.zeros((dc, w_ref.shape[1]), jnp.float32)
        for m in range(mb):
            acc += lax.dot_general(buf[m, :, c], du_ref[m], (((0,), (0,)), ((), ())), preferred_element_type=jnp.float32)
        dw_ref[c, :] = acc


def scatter_kernel(me_ref, rows_ref, cnt_ref, slot_ref, *refs):
    blocks, (de_in, de, buf, stage, sem, out_sem) = refs[:8], refs[8:]
    del de_in
    mb, t, d = buf.shape
    pull(me_ref[0], blocks, buf, sem)
    cnt = cnt_ref[0]
    cc = 512

    def copy(q, r):
        return pltpu.make_async_copy(stage.at[pl.ds(q, 1)], de.at[pl.ds(r, 1)], out_sem)

    @pl.loop(0, (cnt + BLK - 1) // BLK)
    def _(b):
        base = b * BLK
        ids = lax.broadcasted_iota(jnp.int32, (BLK, mb * t), 0) + base
        oh = (ids == slot_ref[...]).astype(jnp.bfloat16)
        for i in range(d // cc):
            acc = jnp.zeros((BLK, cc), jnp.float32)
            for m in range(mb):
                acc += jnp.dot(oh[:, m * t:(m + 1) * t], buf[m, :, i * cc:(i + 1) * cc], preferred_element_type=jnp.float32)
            stage[:, i * cc:(i + 1) * cc] = acc
        n = jnp.minimum(cnt - base, BLK)
        pl.loop(0, n)(lambda q: copy(q, rows_ref[base + q]).start())
        pl.loop(0, n)(lambda q: copy(q, rows_ref[base + q]).wait())


def solution(mesh):
    groups = mesh.shape["tp"]

    def swap(v, bit):
        return lax.ppermute(v, "tp", [(i, i ^ bit) for i in range(groups)])

    def local(ids, emb, g, w, du, dres):
        r = lax.axis_index("tp")
        mb, t = ids.shape
        vl, d = emb.shape
        f = w.shape[1]
        tl = t // groups
        hd = d // 2
        k, c = r & 1, r >> 1
        gf = g.astype(jnp.float32)
        me = r.reshape(1)

        de0 = pl.pallas_call(
            zero_kernel,
            out_shape=jax.ShapeDtypeStruct((vl, d), jnp.float32),
            out_specs=ANY,
            scratch_shapes=[pltpu.VMEM((ZR, d), jnp.float32), pltpu.SemaphoreType.DMA],
            cost_estimate=pl.CostEstimate(flops=80_000_000, bytes_accessed=vl * d * 4, transcendentals=0),
            name="zero_rows",
        )()

        def halves(v):
            v = v.reshape(mb, 4, 2, tl, 2, hd)
            return lax.dynamic_index_in_dim(v, k, 4, False), lax.dynamic_index_in_dim(v, 1 - k, 4, False)

        def reduce_to_home(v, dt):
            mine, theirs = halves(v)
            got = swap(theirs, 1)

            def part(z, h):
                a = lax.dynamic_index_in_dim(mine, z, 1, False)[:, h]
                b = lax.dynamic_index_in_dim(got, z, 1, False)[:, h]
                return a.astype(dt) + b.astype(dt)

            dx_ = swap(part(c ^ 3, 0), 2)
            dy_ = swap(part(c ^ 3, 1), 4)
            ex = swap(part(c ^ 1, 0), 2)
            ey = swap(part(c ^ 2, 1), 4)
            fy = swap(part(c ^ 2, 0) + dx_, 4)
            fx = swap(part(c ^ 1, 1) + dy_, 2)
            s0 = part(c, 0) + ex + fy
            s1 = part(c, 1) + ey + fx
            keep = jnp.where(k == 0, s0, s1)
            give = jnp.where(k == 0, s1, s0)
            other = swap(give, 1)
            return jnp.where(k == 0, jnp.concatenate([keep, other], -1), jnp.concatenate([other, keep], -1))

        def gather_all(v):
            h = v.shape[0] // 2
            vx, vy = swap(v, 2), swap(v, 4)
            d1 = swap(vx[:h], 4)
            d0 = swap(vy[h:], 2)
            vd = jnp.concatenate([d1, d0], 0)
            out = {0: v, 2: vx, 4: vy, 6: vd}
            for j in (0, 2, 4, 6):
                out[j + 1] = swap(out[j], 1)
            return [out[j] for j in range(8)]

        pdn = lax.dot_general(du.reshape(mb * t, f), w, (((1,), (1,)), ((), ())), preferred_element_type=jnp.float32).astype(jnp.bfloat16)
        flat = ids.reshape(-1)
        loc = flat - r * vl
        own = (loc >= 0) & (loc < vl)
        xp = jnp.where(own[:, None], emb[jnp.clip(loc, 0, vl - 1)], jnp.zeros((), emb.dtype))

        dn = reduce_to_home(pdn, jnp.float32)
        x = reduce_to_home(xp, jnp.bfloat16)
        xs = gather_all(x)

        u, dw = pl.pallas_call(
            proj_kernel,
            out_shape=(jax.ShapeDtypeStruct((mb, t, f), jnp.bfloat16), jax.ShapeDtypeStruct((d, f), jnp.float32)),
            in_specs=[SMEM, VMEM, VMEM, VMEM] + [ANY] * 8,
            out_specs=(VMEM, VMEM),
            scratch_shapes=[pltpu.VMEM((mb, t, d), jnp.bfloat16), pltpu.SemaphoreType.DMA((8,))],
            cost_estimate=pl.CostEstimate(flops=60_000_000, bytes_accessed=20_000_000, transcendentals=0),
            compiler_params=pltpu.CompilerParams(vmem_limit_bytes=50 * 2**20),
            name="norm_proj",
        )(me, g.reshape(1, d), w, du, *xs)

        xf = x.astype(jnp.float32)
        rs = lax.rsqrt(jnp.mean(xf * xf, axis=-1, keepdims=True) + EPS)
        nh = xf * rs
        gdn = gf * dn
        dxn = rs * (gdn - nh * jnp.mean(nh * gdn, axis=-1, keepdims=True))
        dx = (dres.astype(jnp.float32) + dxn).astype(jnp.bfloat16)
        dg = lax.psum(jnp.sum(dn * nh, axis=(0, 1)), "tp")
        dxs = gather_all(dx)

        n = flat.shape[0]
        i0 = lax.broadcasted_iota(jnp.int32, (n, n), 0)
        i1 = lax.broadcasted_iota(jnp.int32, (n, n), 1)
        same = flat[:, None] == flat[None, :]
        first = jnp.min(jnp.where(same, i0, n), axis=0)
        lead = own & (first == jnp.arange(n))
        pos = jnp.sum(jnp.where(lead[:, None] & (i0 < i1), 1, 0), axis=0)
        pos_of_first = jnp.sum(jnp.where((i0 == first[None, :]), pos[:, None], 0), axis=0)
        slot = jnp.where(own, pos_of_first, -1).astype(jnp.int32)
        rows = jnp.sum(jnp.where(lead[:, None] & (pos[:, None] == i1), loc[:, None], 0), axis=0).astype(jnp.int32)
        cnt = jnp.sum(lead.astype(jnp.int32)).reshape(1)

        de = pl.pallas_call(
            scatter_kernel,
            out_shape=jax.ShapeDtypeStruct((vl, d), jnp.float32),
            in_specs=[SMEM, SMEM, SMEM, VMEM] + [ANY] * 9,
            out_specs=ANY,
            scratch_shapes=[
                pltpu.VMEM((mb, t, d), jnp.bfloat16),
                pltpu.VMEM((BLK, d), jnp.float32),
                pltpu.SemaphoreType.DMA((8,)),
                pltpu.SemaphoreType.DMA,
            ],
            input_output_aliases={12: 0},
            name="put_rows",
        )(me, rows, cnt, slot.reshape(1, n), *dxs, de0)
        return u, x, de, dw, dg

    return jax.shard_map(
        local,
        mesh=mesh,
        in_specs=(P("dp", None), P("tp", None), P(None), P(None, "tp"), P("dp", None, "tp"), P("dp", "tp", None)),
        out_specs=(P("dp", None, "tp"), P("dp", "tp", None), P(("dp", "tp"), None), P(None, ("dp", "tp")), P("dp")),
        check_vma=False,
    )
```

```python
import functools

import jax
import jax.numpy as jnp
from jax import lax
from jax.experimental import pallas as pl
from jax.experimental.pallas import tpu as pltpu
from jax.sharding import PartitionSpec as P

EPS = 1e-6
ANY = pl.BlockSpec(memory_space=pl.ANY)
VMEM = pl.BlockSpec(memory_space=pltpu.VMEM)
SMEM = pl.BlockSpec(memory_space=pltpu.SMEM)
ZR = 256
BLK = 128


def zero_kernel(first, steps, *refs):
    de, z, sem = refs[-3:]
    z[...] = jnp.zeros_like(z)

    def copy(i):
        return pltpu.make_async_copy(z, de.at[pl.ds(pl.multiple_of((first + i) * ZR, ZR), ZR)], sem)

    pl.loop(0, steps)(lambda i: copy(i).start())
    pl.loop(0, steps)(lambda i: copy(i).wait())


def pdn_kernel(js, kc_ref, du_ref, w_ref, mine_ref, theirs_ref):
    k, c = kc_ref[0], kc_ref[1]
    mb, t, _ = du_ref.shape
    tc = t // 4
    hd = w_ref.shape[0] // 2
    wc = 512
    for i, j in enumerate(js):
        z = pl.multiple_of(jnp.bitwise_xor(c, j) * tc, tc)
        rows = jnp.concatenate([du_ref[m, pl.ds(z, tc), :] for m in range(mb)], axis=0)
        for out, half in ((theirs_ref, 1 - k), (mine_ref, k)):
            for n in range(hd // wc):
                wv = w_ref[pl.ds(pl.multiple_of(half * hd + n * wc, wc), wc), :]
                v = lax.dot_general(rows, wv, (((1,), (1,)), ((), ())), preferred_element_type=jnp.float32)
                out[i, :, :, n * wc:(n + 1) * wc] = v.astype(jnp.bfloat16).reshape(mb, tc, wc)


def lookup_kernel(kc_ref, loc_ref, tgt_ref, emb, mine_ref, theirs_ref, buf, sem):
    k, c = kc_ref[0], kc_ref[1]
    vl, d = emb.shape
    nj, mb, tc, hd = mine_ref.shape
    n = nj * mb * tc
    step = 64

    @pl.loop(0, 2 * n // step)
    def _(i):
        buf[pl.ds(pl.multiple_of(i * step, step), step), :] = jnp.zeros((step, d), buf.dtype)

    def copy(t, l):
        src = emb.at[pl.ds(pl.multiple_of((l >> 1) * 2, 2), 2)]
        return pltpu.make_async_copy(src, buf.at[pl.ds(pl.multiple_of(t * 2, 2), 2)], sem)

    def issue(i, cnt):
        for q in range(8):
            t = i * 8 + q
            l = loc_ref[t]
            own = (l >= 0) & (l < vl)

            @pl.when(own)
            def _():
                copy(t, l).start()

            cnt = cnt + own.astype(jnp.int32)
        return cnt

    cnt = lax.fori_loop(0, n // 8, issue, jnp.int32(0))

    @pl.loop(0, cnt)
    def _(i):
        copy(0, 0).wait()

    for j in range(nj):
        z = jnp.bitwise_xor(c, j)

        @pl.loop(0, mb)
        def _(m):
            t0 = m * (nj * tc) + z * tc
            tgt = tgt_ref[pl.ds(pl.multiple_of(t0, tc), tc), :]
            sel = (lax.broadcasted_iota(jnp.int32, (tc, 2 * tc), 1) == tgt).astype(jnp.bfloat16)
            rows = pl.ds(pl.multiple_of(2 * t0, 2 * tc), 2 * tc)
            for out, half in ((theirs_ref, 1 - k), (mine_ref, k)):
                v = buf[rows, pl.ds(pl.multiple_of(half * hd, 128), hd)]
                out[j, m] = jnp.dot(sel, v, preferred_element_type=jnp.float32).astype(jnp.bfloat16)


def pull(me, blocks, buf, sem):
    tl = blocks[0].shape[1]
    copies = []
    for j, b in enumerate(blocks):
        s = pl.multiple_of(jnp.bitwise_xor(me, j) * tl, tl)
        copies.append(pltpu.make_async_copy(b, buf.at[:, pl.ds(s, tl), :], sem.at[j]))
    for c in copies:
        c.start()
    for c in copies:
        c.wait()


def proj_kernel(me_ref, g_ref, w_ref, du_ref, *refs):
    blocks, (u_ref, dw_ref, buf, sem) = refs[:8], refs[8:]
    mb, t, d = buf.shape
    pull(me_ref[0], blocks, buf, sem)
    gf = g_ref[...].astype(jnp.float32)
    rows = 32

    @pl.loop(0, mb * t // rows)
    def _(i):
        m, r = i // (t // rows), i % (t // rows)
        at = (m, pl.ds(pl.multiple_of(r * rows, rows), rows), slice(None))
        xf = buf[at].astype(jnp.float32)
        rs = lax.rsqrt(jnp.mean(xf * xf, axis=-1, keepdims=True) + EPS)
        buf[at] = (xf * rs * gf).astype(jnp.bfloat16)

    @pl.loop(0, mb)
    def _(m):
        u_ref[m] = jnp.dot(buf[m], w_ref[...], preferred_element_type=jnp.float32).astype(jnp.bfloat16)

    dc = 256

    @pl.loop(0, d // dc)
    def _(i):
        c = pl.ds(pl.multiple_of(i * dc, dc), dc)
        acc = jnp.zeros((dc, w_ref.shape[1]), jnp.float32)
        for m in range(mb):
            acc += lax.dot_general(buf[m, :, c], du_ref[m], (((0,), (0,)), ((), ())), preferred_element_type=jnp.float32)
        dw_ref[c, :] = acc


def scatter_kernel(me_ref, rows_ref, cnt_ref, slot_ref, *refs):
    blocks, (de_in, de, buf, stage, sem, out_sem) = refs[:8], refs[8:]
    del de_in
    mb, t, d = buf.shape
    pull(me_ref[0], blocks, buf, sem)
    cnt = cnt_ref[0]
    cc = 512

    def copy(q, r):
        return pltpu.make_async_copy(stage.at[pl.ds(q, 1)], de.at[pl.ds(r, 1)], out_sem)

    @pl.loop(0, (cnt + BLK - 1) // BLK)
    def _(b):
        base = b * BLK
        ids = lax.broadcasted_iota(jnp.int32, (BLK, mb * t), 0) + base
        oh = (ids == slot_ref[...]).astype(jnp.bfloat16)
        for i in range(d // cc):
            acc = jnp.zeros((BLK, cc), jnp.float32)
            for m in range(mb):
                acc += jnp.dot(oh[:, m * t:(m + 1) * t], buf[m, :, i * cc:(i + 1) * cc], preferred_element_type=jnp.float32)
            stage[:, i * cc:(i + 1) * cc] = acc
        n = jnp.minimum(cnt - base, BLK)
        pl.loop(0, n)(lambda q: copy(q, rows_ref[base + q]).start())
        pl.loop(0, n)(lambda q: copy(q, rows_ref[base + q]).wait())


def solution(mesh):
    groups = mesh.shape["tp"]

    def swap(v, bit):
        return lax.ppermute(v, "tp", [(i, i ^ bit) for i in range(groups)])

    def local(ids, emb, g, w, du, dres):
        r = lax.axis_index("tp")
        mb, t = ids.shape
        vl, d = emb.shape
        f = w.shape[1]
        tl = t // groups
        hd = d // 2
        k, c = r & 1, r >> 1
        gf = g.astype(jnp.float32)
        me = r.reshape(1)

        de0 = None
        parts_of_zero = 4
        for q in range(parts_of_zero):
            steps = vl // ZR // parts_of_zero
            args = () if de0 is None else (de0,)
            de0 = pl.pallas_call(
                functools.partial(zero_kernel, q * steps, steps),
                out_shape=jax.ShapeDtypeStruct((vl, d), jnp.float32),
                in_specs=[ANY] * len(args),
                out_specs=ANY,
                scratch_shapes=[pltpu.VMEM((ZR, d), jnp.float32), pltpu.SemaphoreType.DMA],
                input_output_aliases={0: 0} if args else {},
                cost_estimate=pl.CostEstimate(flops=20_000_000, bytes_accessed=vl * d, transcendentals=0),
                name=f"zero_rows_{q}",
            )(*args)

        kc = jnp.stack([k, c]).astype(jnp.int32)
        tc = t // 4

        def half_shape(nj):
            return jax.ShapeDtypeStruct((nj, mb, tc, hd), jnp.bfloat16)

        def pdn(js):
            mine, theirs = pl.pallas_call(
                functools.partial(pdn_kernel, js),
                out_shape=(half_shape(len(js)),) * 2,
                in_specs=[SMEM, VMEM, VMEM],
                out_specs=(VMEM, VMEM),
                cost_estimate=pl.CostEstimate(flops=5_000_000 * len(js), bytes_accessed=8_000_000, transcendentals=0),
                compiler_params=pltpu.CompilerParams(vmem_limit_bytes=40 * 2**20),
                name=f"pdn_{len(js)}",
            )(kc, du, w)
            got = swap(theirs, 1)
            return {j: (mine[i], got[i]) for i, j in enumerate(js)}

        def reduce_to_home(pairs, dt):
            def part(j, h):
                a, b = pairs[j]
                return a[:, h * tl:(h + 1) * tl].astype(dt) + b[:, h * tl:(h + 1) * tl].astype(dt)

            dx_ = swap(part(3, 0), 2)
            dy_ = swap(part(3, 1), 4)
            ex = swap(part(1, 0), 2)
            ey = swap(part(2, 1), 4)
            fy = swap(part(2, 0) + dx_, 4)
            fx = swap(part(1, 1) + dy_, 2)
            s0 = part(0, 0) + ex + fy
            s1 = part(0, 1) + ey + fx
            keep = jnp.where(k == 0, s0, s1)
            give = jnp.where(k == 0, s1, s0)
            other = swap(give, 1)
            return jnp.where(k == 0, jnp.concatenate([keep, other], -1), jnp.concatenate([other, keep], -1))

        def gather_all(v):
            h = v.shape[0] // 2
            vx, vy = swap(v, 2), swap(v, 4)
            d1 = swap(vx[:h], 4)
            d0 = swap(vy[h:], 2)
            vd = jnp.concatenate([d1, d0], 0)
            out = {0: v, 2: vx, 4: vy, 6: vd}
            for j in (0, 2, 4, 6):
                out[j + 1] = swap(out[j], 1)
            return [out[j] for j in range(8)]

        flat = ids.reshape(-1)
        n = flat.shape[0]
        loc = flat - r * vl
        own = (loc >= 0) & (loc < vl)
        pairs = pdn((3,))
        pairs.update(pdn((1, 2, 0)))
        tgt = jnp.where(own, 2 * (jnp.arange(n) % tc) + (loc & 1), -1).astype(jnp.int32)
        mine, theirs = pl.pallas_call(
            lookup_kernel,
            out_shape=(half_shape(4),) * 2,
            in_specs=[SMEM, SMEM, VMEM, ANY],
            out_specs=(VMEM, VMEM),
            scratch_shapes=[pltpu.VMEM((2 * n, d), jnp.bfloat16), pltpu.SemaphoreType.DMA],
            cost_estimate=pl.CostEstimate(flops=20_000_000, bytes_accessed=12_000_000, transcendentals=0),
            compiler_params=pltpu.CompilerParams(vmem_limit_bytes=40 * 2**20),
            name="lookup",
        )(kc, loc, tgt.reshape(n, 1), emb)
        got = swap(theirs, 1)
        xpairs = {j: (mine[j], got[j]) for j in range(4)}

        dn = reduce_to_home(pairs, jnp.float32)
        x = reduce_to_home(xpairs, jnp.bfloat16)
        xs = gather_all(x)

        u, dw = pl.pallas_call(
            proj_kernel,
            out_shape=(jax.ShapeDtypeStruct((mb, t, f), jnp.bfloat16), jax.ShapeDtypeStruct((d, f), jnp.float32)),
            in_specs=[SMEM, VMEM, VMEM, VMEM] + [ANY] * 8,
            out_specs=(VMEM, VMEM),
            scratch_shapes=[pltpu.VMEM((mb, t, d), jnp.bfloat16), pltpu.SemaphoreType.DMA((8,))],
            cost_estimate=pl.CostEstimate(flops=60_000_000, bytes_accessed=20_000_000, transcendentals=0),
            compiler_params=pltpu.CompilerParams(vmem_limit_bytes=50 * 2**20),
            name="norm_proj",
        )(me, g.reshape(1, d), w, du, *xs)

        xf = x.astype(jnp.float32)
        rs = lax.rsqrt(jnp.mean(xf * xf, axis=-1, keepdims=True) + EPS)
        nh = xf * rs
        gdn = gf * dn
        dxn = rs * (gdn - nh * jnp.mean(nh * gdn, axis=-1, keepdims=True))
        dx = (dres.astype(jnp.float32) + dxn).astype(jnp.bfloat16)
        dg = jnp.sum(dn * nh, axis=(0, 1))
        dxs = gather_all(dx)
        for bit in (1, 2, 4):
            dg = dg + swap(dg, bit)

        i0 = lax.broadcasted_iota(jnp.int32, (n, n), 0)
        i1 = lax.broadcasted_iota(jnp.int32, (n, n), 1)
        same = flat[:, None] == flat[None, :]
        first = jnp.min(jnp.where(same, i0, n), axis=0)
        lead = own & (first == jnp.arange(n))
        pos = jnp.sum(jnp.where(lead[:, None] & (i0 < i1), 1, 0), axis=0)
        pos_of_first = jnp.sum(jnp.where((i0 == first[None, :]), pos[:, None], 0), axis=0)
        slot = jnp.where(own, pos_of_first, -1).astype(jnp.int32)
        rows = jnp.sum(jnp.where(lead[:, None] & (pos[:, None] == i1), loc[:, None], 0), axis=0).astype(jnp.int32)
        cnt = jnp.sum(lead.astype(jnp.int32)).reshape(1)

        de = pl.pallas_call(
            scatter_kernel,
            out_shape=jax.ShapeDtypeStruct((vl, d), jnp.float32),
            in_specs=[SMEM, SMEM, SMEM, VMEM] + [ANY] * 9,
            out_specs=ANY,
            scratch_shapes=[
                pltpu.VMEM((mb, t, d), jnp.bfloat16),
                pltpu.VMEM((BLK, d), jnp.float32),
                pltpu.SemaphoreType.DMA((8,)),
                pltpu.SemaphoreType.DMA,
            ],
            input_output_aliases={12: 0},
            name="put_rows",
        )(me, rows, cnt, slot.reshape(1, n), *dxs, de0)
        return u, x, de, dw, dg

    return jax.shard_map(
        local,
        mesh=mesh,
        in_specs=(P("dp", None), P("tp", None), P(None), P(None, "tp"), P("dp", None, "tp"), P("dp", "tp", None)),
        out_specs=(P("dp", None, "tp"), P("dp", "tp", None), P(("dp", "tp"), None), P(None, ("dp", "tp")), P("dp")),
        check_vma=False,
    )
```

```python
import functools

import jax
import jax.numpy as jnp
from jax import lax
from jax.experimental import pallas as pl
from jax.experimental.pallas import tpu as pltpu
from jax.sharding import PartitionSpec as P

EPS = 1e-6
ANY = pl.BlockSpec(memory_space=pl.ANY)
VMEM = pl.BlockSpec(memory_space=pltpu.VMEM)
SMEM = pl.BlockSpec(memory_space=pltpu.SMEM)
ZR = 128
BLK = 128
LOOKUP_SHARE, NORM_SHARE = 40, 12


def zero_fill(de, z, sem, first, last):
    z[...] = jnp.zeros_like(z)

    def copy(i):
        return pltpu.make_async_copy(z, de.at[pl.ds(pl.multiple_of(i * ZR, ZR), ZR)], sem)

    def start():
        pl.loop(first, last)(lambda i: copy(i).start())

    def wait():
        pl.loop(first, last)(lambda i: copy(i).wait())

    return start, wait


def pdn_kernel(js, kc_ref, du_ref, w_ref, mine_ref, theirs_ref):
    k, c = kc_ref[0], kc_ref[1]
    mb, t, _ = du_ref.shape
    tc = t // 4
    hd = w_ref.shape[0] // 2
    wc = 512
    for i, j in enumerate(js):
        z = pl.multiple_of(jnp.bitwise_xor(c, j) * tc, tc)
        rows = jnp.concatenate([du_ref[m, pl.ds(z, tc), :] for m in range(mb)], axis=0)
        for out, half in ((theirs_ref, 1 - k), (mine_ref, k)):
            for n in range(hd // wc):
                wv = w_ref[pl.ds(pl.multiple_of(half * hd + n * wc, wc), wc), :]
                v = lax.dot_general(rows, wv, (((1,), (1,)), ((), ())), preferred_element_type=jnp.float32)
                out[i, :, :, n * wc:(n + 1) * wc] = v.astype(jnp.bfloat16).reshape(mb, tc, wc)


def lookup_kernel(kc_ref, loc_ref, tgt_ref, emb, mine_ref, theirs_ref, de, buf, sem, z, zsem):
    k, c = kc_ref[0], kc_ref[1]
    vl, d = emb.shape
    nj, mb, tc, hd = mine_ref.shape
    n = nj * mb * tc
    step = 64
    start, wait = zero_fill(de, z, zsem, 0, LOOKUP_SHARE)

    @pl.loop(0, 2 * n // step)
    def _(i):
        buf[pl.ds(pl.multiple_of(i * step, step), step), :] = jnp.zeros((step, d), buf.dtype)

    def copy(t, l):
        src = emb.at[pl.ds(pl.multiple_of((l >> 1) * 2, 2), 2)]
        return pltpu.make_async_copy(src, buf.at[pl.ds(pl.multiple_of(t * 2, 2), 2)], sem)

    def issue(i, cnt):
        for q in range(8):
            t = i * 8 + q
            l = loc_ref[t]
            own = (l >= 0) & (l < vl)

            @pl.when(own)
            def _():
                copy(t, l).start()

            cnt = cnt + own.astype(jnp.int32)
        return cnt

    cnt = lax.fori_loop(0, n // 8, issue, jnp.int32(0))
    start()

    @pl.loop(0, cnt)
    def _(i):
        copy(0, 0).wait()

    for j in range(nj):
        zc = jnp.bitwise_xor(c, j)

        @pl.loop(0, mb)
        def _(m):
            t0 = m * (nj * tc) + zc * tc
            tgt = tgt_ref[pl.ds(pl.multiple_of(t0, tc), tc), :]
            sel = (lax.broadcasted_iota(jnp.int32, (tc, 2 * tc), 1) == tgt).astype(jnp.bfloat16)
            rows = pl.ds(pl.multiple_of(2 * t0, 2 * tc), 2 * tc)
            for out, half in ((theirs_ref, 1 - k), (mine_ref, k)):
                v = buf[rows, pl.ds(pl.multiple_of(half * hd, 128), hd)]
                out[j, m] = jnp.dot(sel, v, preferred_element_type=jnp.float32).astype(jnp.bfloat16)

    wait()


def pull(me, blocks, buf, sem):
    hb, tl = blocks[0].shape[:2]
    copies = []
    for i, b in enumerate(blocks):
        j, h = i // 2, i % 2
        s = pl.multiple_of(jnp.bitwise_xor(me, j) * tl, tl)
        copies.append(pltpu.make_async_copy(b, buf.at[h * hb:(h + 1) * hb, pl.ds(s, tl), :], sem.at[i]))
    for c in copies:
        c.start()
    return copies


def norm_kernel(me_ref, g_ref, w_ref, *refs):
    blocks, (de_in, n_ref, u_ref, de, sem, z, zsem) = refs[:16], refs[16:]
    del de_in
    mb, t, _ = n_ref.shape
    start, wait = zero_fill(de, z, zsem, LOOKUP_SHARE, LOOKUP_SHARE + NORM_SHARE)
    copies = pull(me_ref[0], blocks, n_ref, sem)
    start()
    for c in copies:
        c.wait()
    gf = g_ref[...].astype(jnp.float32)
    rows = 32

    @pl.loop(0, mb)
    def _(m):
        @pl.loop(0, t // rows)
        def _(r):
            at = (m, pl.ds(pl.multiple_of(r * rows, rows), rows), slice(None))
            xf = n_ref[at].astype(jnp.float32)
            rs = lax.rsqrt(jnp.mean(xf * xf, axis=-1, keepdims=True) + EPS)
            n_ref[at] = (xf * rs * gf).astype(jnp.bfloat16)

        u_ref[m] = jnp.dot(n_ref[m], w_ref[...], preferred_element_type=jnp.float32).astype(jnp.bfloat16)

    wait()


def dw_kernel(n_ref, du_ref, de_in, dw_ref, de, z, zsem):
    del de_in
    mb, _, d = n_ref.shape
    start, wait = zero_fill(de, z, zsem, LOOKUP_SHARE + NORM_SHARE, de.shape[0] // ZR)
    start()
    dc = 512

    @pl.loop(0, d // dc)
    def _(i):
        c = pl.ds(pl.multiple_of(i * dc, dc), dc)
        acc = jnp.zeros((dc, du_ref.shape[2]), jnp.float32)
        for m in range(mb):
            acc += lax.dot_general(n_ref[m, :, c], du_ref[m], (((0,), (0,)), ((), ())), preferred_element_type=jnp.float32)
        dw_ref[c, :] = acc

    wait()


def scatter_kernel(me_ref, rows_ref, cnt_ref, slot_ref, *refs):
    blocks, (de_in, de, buf, stage, sem, out_sem) = refs[:16], refs[16:]
    del de_in
    mb, t, d = buf.shape
    for c in pull(me_ref[0], blocks, buf, sem):
        c.wait()
    cnt = cnt_ref[0]
    cc = 512

    def copy(q, r):
        return pltpu.make_async_copy(stage.at[pl.ds(q, 1)], de.at[pl.ds(r, 1)], out_sem)

    @pl.loop(0, (cnt + BLK - 1) // BLK)
    def _(b):
        base = b * BLK
        ids = lax.broadcasted_iota(jnp.int32, (BLK, mb * t), 0) + base
        oh = (ids == slot_ref[...]).astype(jnp.bfloat16)
        for i in range(d // cc):
            acc = jnp.zeros((BLK, cc), jnp.float32)
            for m in range(mb):
                acc += jnp.dot(oh[:, m * t:(m + 1) * t], buf[m, :, i * cc:(i + 1) * cc], preferred_element_type=jnp.float32)
            stage[:, i * cc:(i + 1) * cc] = acc
        n = jnp.minimum(cnt - base, BLK)
        pl.loop(0, n)(lambda q: copy(q, rows_ref[base + q]).start())
        pl.loop(0, n)(lambda q: copy(q, rows_ref[base + q]).wait())


def solution(mesh):
    groups = mesh.shape["tp"]

    def swap(v, bit):
        return lax.ppermute(v, "tp", [(i, i ^ bit) for i in range(groups)])

    def local(ids, emb, g, w, du, dres):
        r = lax.axis_index("tp")
        mb, t = ids.shape
        vl, d = emb.shape
        f = w.shape[1]
        tl = t // groups
        hd = d // 2
        tc = t // 4
        k, c = r & 1, r >> 1
        gf = g.astype(jnp.float32)
        me = r.reshape(1)
        kc = jnp.stack([k, c]).astype(jnp.int32)
        de_shape = jax.ShapeDtypeStruct((vl, d), jnp.float32)
        zero_scratch = [pltpu.VMEM((ZR, d), jnp.float32), pltpu.SemaphoreType.DMA]

        def half_shape(nj):
            return jax.ShapeDtypeStruct((nj, mb, tc, hd), jnp.bfloat16)

        def pdn(js):
            mine, theirs = pl.pallas_call(
                functools.partial(pdn_kernel, js),
                out_shape=(half_shape(len(js)),) * 2,
                in_specs=[SMEM, VMEM, VMEM],
                out_specs=(VMEM, VMEM),
                cost_estimate=pl.CostEstimate(flops=5_000_000 * len(js), bytes_accessed=8_000_000, transcendentals=0),
                compiler_params=pltpu.CompilerParams(vmem_limit_bytes=40 * 2**20),
            )(kc, du, w)
            got = swap(theirs, 1)
            return {j: (mine[i], got[i]) for i, j in enumerate(js)}

        def reduce_to_home(pairs, dt):
            def part(j, h):
                a, b = pairs[j]
                return a[:, h * tl:(h + 1) * tl].astype(dt) + b[:, h * tl:(h + 1) * tl].astype(dt)

            dx_ = swap(part(3, 0), 2)
            dy_ = swap(part(3, 1), 4)
            ex = swap(part(1, 0), 2)
            ey = swap(part(2, 1), 4)
            pairs = dict(pairs)
            pairs[2], dx_ = lax.optimization_barrier((pairs[2], dx_))
            pairs[1], dy_ = lax.optimization_barrier((pairs[1], dy_))
            fy = swap(part(2, 0) + dx_, 4)
            fx = swap(part(1, 1) + dy_, 2)
            pairs[0], ex, ey = lax.optimization_barrier((pairs[0], ex, ey))
            s0 = part(0, 0) + ex + fy
            s1 = part(0, 1) + ey + fx
            keep = jnp.where(k == 0, s0, s1)
            give = jnp.where(k == 0, s1, s0)
            other = swap(give, 1)
            return jnp.where(k == 0, jnp.concatenate([keep, other], -1), jnp.concatenate([other, keep], -1))

        def gather_all(v):
            h = v.shape[0] // 2
            own = (v[:h], v[h:])
            x1, y0 = swap(own[1], 2), swap(own[0], 4)
            x0, y1 = swap(own[0], 2), swap(own[1], 4)
            d1, d0 = swap(x1, 4), swap(y0, 2)
            out = {0: own, 2: (x0, x1), 4: (y0, y1), 6: (d0, d1)}
            for j in (0, 2, 4, 6):
                out[j + 1] = tuple(swap(b, 1) for b in out[j])
            return [b for j in range(8) for b in out[j]]

        flat = ids.reshape(-1)
        n = flat.shape[0]
        loc = flat - r * vl
        own = (loc >= 0) & (loc < vl)
        pairs = pdn((3,))
        pairs.update(pdn((1, 2, 0)))
        tgt = jnp.where(own, 2 * (jnp.arange(n) % tc) + (loc & 1), -1).astype(jnp.int32)
        mine, theirs, de = pl.pallas_call(
            lookup_kernel,
            out_shape=(half_shape(4), half_shape(4), de_shape),
            in_specs=[SMEM, SMEM, VMEM, ANY],
            out_specs=(VMEM, VMEM, ANY),
            scratch_shapes=[pltpu.VMEM((2 * n, d), jnp.bfloat16), pltpu.SemaphoreType.DMA] + zero_scratch,
            cost_estimate=pl.CostEstimate(flops=40_000_000, bytes_accessed=60_000_000, transcendentals=0),
            compiler_params=pltpu.CompilerParams(vmem_limit_bytes=40 * 2**20),
            name="lookup",
        )(kc, loc, tgt.reshape(n, 1), emb)
        got = swap(theirs, 1)
        xpairs = {j: (mine[j], got[j]) for j in range(4)}

        dn = reduce_to_home(pairs, jnp.float32)
        x = reduce_to_home(xpairs, jnp.bfloat16)
        xs = gather_all(x)

        nn, u, de = pl.pallas_call(
            norm_kernel,
            out_shape=(jax.ShapeDtypeStruct((mb, t, d), jnp.bfloat16), jax.ShapeDtypeStruct((mb, t, f), jnp.bfloat16), de_shape),
            in_specs=[SMEM, VMEM, VMEM] + [ANY] * 17,
            out_specs=(VMEM, VMEM, ANY),
            scratch_shapes=[pltpu.SemaphoreType.DMA((16,))] + zero_scratch,
            input_output_aliases={19: 2},
            cost_estimate=pl.CostEstimate(flops=30_000_000, bytes_accessed=40_000_000, transcendentals=0),
            compiler_params=pltpu.CompilerParams(vmem_limit_bytes=40 * 2**20),
            name="norm",
        )(me, g.reshape(1, d), w, *xs, de)
        dw, de = pl.pallas_call(
            dw_kernel,
            out_shape=(jax.ShapeDtypeStruct((d, f), jnp.float32), de_shape),
            in_specs=[VMEM, VMEM, ANY],
            out_specs=(VMEM, ANY),
            scratch_shapes=zero_scratch,
            input_output_aliases={2: 1},
            cost_estimate=pl.CostEstimate(flops=30_000_000, bytes_accessed=40_000_000, transcendentals=0),
            compiler_params=pltpu.CompilerParams(vmem_limit_bytes=40 * 2**20),
            name="dw",
        )(nn, du, de)

        xf = x.astype(jnp.float32)
        rs = lax.rsqrt(jnp.mean(xf * xf, axis=-1, keepdims=True) + EPS)
        nh = xf * rs
        gdn = gf * dn
        dxn = rs * (gdn - nh * jnp.mean(nh * gdn, axis=-1, keepdims=True))
        dx = (dres.astype(jnp.float32) + dxn).astype(jnp.bfloat16)
        dg = jnp.sum(dn * nh, axis=(0, 1))
        dxs = gather_all(dx)
        for bit in (1, 2, 4):
            dg = dg + swap(dg, bit)

        i0 = lax.broadcasted_iota(jnp.int32, (n, n), 0)
        i1 = lax.broadcasted_iota(jnp.int32, (n, n), 1)
        same = flat[:, None] == flat[None, :]
        first = jnp.min(jnp.where(same, i0, n), axis=0)
        lead = own & (first == jnp.arange(n))
        pos = jnp.sum(jnp.where(lead[:, None] & (i0 < i1), 1, 0), axis=0)
        pos_of_first = jnp.sum(jnp.where((i0 == first[None, :]), pos[:, None], 0), axis=0)
        slot = jnp.where(own, pos_of_first, -1).astype(jnp.int32)
        rows = jnp.sum(jnp.where(lead[:, None] & (pos[:, None] == i1), loc[:, None], 0), axis=0).astype(jnp.int32)
        cnt = jnp.sum(lead.astype(jnp.int32)).reshape(1)

        de = pl.pallas_call(
            scatter_kernel,
            out_shape=de_shape,
            in_specs=[SMEM, SMEM, SMEM, VMEM] + [ANY] * 17,
            out_specs=ANY,
            scratch_shapes=[
                pltpu.VMEM((mb, t, d), jnp.bfloat16),
                pltpu.VMEM((BLK, d), jnp.float32),
                pltpu.SemaphoreType.DMA((16,)),
                pltpu.SemaphoreType.DMA,
            ],
            input_output_aliases={20: 0},
            name="put_rows",
        )(me, rows, cnt, slot.reshape(1, n), *dxs, de)
        return u, x, de, dw, dg

    return jax.shard_map(
        local,
        mesh=mesh,
        in_specs=(P("dp", None), P("tp", None), P(None), P(None, "tp"), P("dp", None, "tp"), P("dp", "tp", None)),
        out_specs=(P("dp", None, "tp"), P("dp", "tp", None), P(("dp", "tp"), None), P(None, ("dp", "tp")), P("dp")),
        check_vma=False,
    )
```

```python
import functools

import jax
import jax.numpy as jnp
from jax import lax
from jax.experimental import pallas as pl
from jax.experimental.pallas import tpu as pltpu
from jax.sharding import PartitionSpec as P

EPS = 1e-6
ANY = pl.BlockSpec(memory_space=pl.ANY)
VMEM = pl.BlockSpec(memory_space=pltpu.VMEM)
SMEM = pl.BlockSpec(memory_space=pltpu.SMEM)
ZR = 128
BLK = 256
LOOKUP_EARLY, LOOKUP_SHARE, NORM_SHARE = 14, 28, 20


def zero_fill(de, z, sem, first, last):

    def copy(i):
        return pltpu.make_async_copy(z, de.at[pl.ds(pl.multiple_of(i * ZR, ZR), ZR)], sem)

    def start(clear=True):
        if clear:
            z[...] = jnp.zeros_like(z)
        pl.loop(first, last)(lambda i: copy(i).start())

    def wait():
        pl.loop(first, last)(lambda i: copy(i).wait())

    return start, wait


def pdn_kernel(js, kc_ref, du_ref, w_ref, mine_ref, theirs_ref):
    k, c = kc_ref[0], kc_ref[1]
    mb, t, _ = du_ref.shape
    tc = t // 4
    hd = w_ref.shape[0] // 2
    wc = 512
    for i, j in enumerate(js):
        z = pl.multiple_of(jnp.bitwise_xor(c, j) * tc, tc)
        rows = jnp.concatenate([du_ref[m, pl.ds(z, tc), :] for m in range(mb)], axis=0)
        for out, half in ((theirs_ref, 1 - k), (mine_ref, k)):
            for n in range(hd // wc):
                wv = w_ref[pl.ds(pl.multiple_of(half * hd + n * wc, wc), wc), :]
                v = lax.dot_general(rows, wv, (((1,), (1,)), ((), ())), preferred_element_type=jnp.float32)
                out[i, :, :, n * wc:(n + 1) * wc] = v.astype(jnp.bfloat16).reshape(mb, tc, wc)


def lookup_kernel(kc_ref, loc_ref, tgt_ref, emb, mine_ref, theirs_ref, de, buf, sem, z, zsem):
    k, c = kc_ref[0], kc_ref[1]
    vl, d = emb.shape
    nj, mb, tc, hd = mine_ref.shape
    n = nj * mb * tc
    step = 64
    start, wait = zero_fill(de, z, zsem, 0, LOOKUP_EARLY)
    late_start, late_wait = zero_fill(de, z, zsem, LOOKUP_EARLY, LOOKUP_SHARE)
    start()

    @pl.loop(0, 2 * n // step)
    def _(i):
        buf[pl.ds(pl.multiple_of(i * step, step), step), :] = jnp.zeros((step, d), buf.dtype)

    def copy(t, l):
        src = emb.at[pl.ds(pl.multiple_of((l >> 1) * 2, 2), 2)]
        return pltpu.make_async_copy(src, buf.at[pl.ds(pl.multiple_of(t * 2, 2), 2)], sem)

    def issue(i, cnt):
        for q in range(8):
            t = i * 8 + q
            l = loc_ref[t]
            own = (l >= 0) & (l < vl)

            @pl.when(own)
            def _():
                copy(t, l).start()

            cnt = cnt + own.astype(jnp.int32)
        return cnt

    cnt = lax.fori_loop(0, n // 8, issue, jnp.int32(0))

    @pl.loop(0, cnt)
    def _(i):
        copy(0, 0).wait()

    late_start(False)

    for j in range(nj):
        zc = jnp.bitwise_xor(c, j)

        @pl.loop(0, mb)
        def _(m):
            t0 = m * (nj * tc) + zc * tc
            tgt = tgt_ref[pl.ds(pl.multiple_of(t0, tc), tc), :]
            sel = (lax.broadcasted_iota(jnp.int32, (tc, 2 * tc), 1) == tgt).astype(jnp.bfloat16)
            rows = pl.ds(pl.multiple_of(2 * t0, 2 * tc), 2 * tc)
            for out, half in ((theirs_ref, 1 - k), (mine_ref, k)):
                v = buf[rows, pl.ds(pl.multiple_of(half * hd, 128), hd)]
                out[j, m] = jnp.dot(sel, v, preferred_element_type=jnp.float32).astype(jnp.bfloat16)

    wait()
    late_wait()


def pull(me, blocks, buf, sem):
    hb, tl = blocks[0].shape[:2]
    copies = []
    for i, b in enumerate(blocks):
        j, h = i // 2, i % 2
        s = pl.multiple_of(jnp.bitwise_xor(me, j) * tl, tl)
        copies.append(pltpu.make_async_copy(b, buf.at[h * hb:(h + 1) * hb, pl.ds(s, tl), :], sem.at[i]))
    for c in copies:
        c.start()
    return copies


def pull_halves(k, c, blocks, buf, sem):
    tl, hd = blocks[0].shape[1:]
    copies = []
    for i, b in enumerate(blocks):
        j, h, q = i // 4, (i // 2) % 2, i % 2
        s = pl.multiple_of((2 * jnp.bitwise_xor(c, j) + h) * tl, tl)
        o = pl.multiple_of(jnp.bitwise_xor(k, q) * hd, 128)
        copies.append(pltpu.make_async_copy(b, buf.at[:, pl.ds(s, tl), pl.ds(o, hd)], sem.at[i]))
    for c in copies:
        c.start()
    return copies


def norm_kernel(kc_ref, g_ref, w_ref, *refs):
    blocks, (de_in, n_ref, u_ref, de, sem, z, zsem) = refs[:16], refs[16:]
    del de_in
    mb, t, _ = n_ref.shape
    start, wait = zero_fill(de, z, zsem, LOOKUP_SHARE, LOOKUP_SHARE + NORM_SHARE)
    copies = pull_halves(kc_ref[0], kc_ref[1], blocks, n_ref, sem)
    start()
    for c in copies:
        c.wait()
    gf = g_ref[...].astype(jnp.float32)
    rows = 32

    @pl.loop(0, mb)
    def _(m):
        @pl.loop(0, t // rows)
        def _(r):
            at = (m, pl.ds(pl.multiple_of(r * rows, rows), rows), slice(None))
            xf = n_ref[at].astype(jnp.float32)
            rs = lax.rsqrt(jnp.mean(xf * xf, axis=-1, keepdims=True) + EPS)
            n_ref[at] = (xf * rs * gf).astype(jnp.bfloat16)

        u_ref[m] = jnp.dot(n_ref[m], w_ref[...], preferred_element_type=jnp.float32).astype(jnp.bfloat16)

    wait()


def dw_kernel(n_ref, du_ref, de_in, dw_ref, de, z, zsem):
    del de_in
    mb, _, d = n_ref.shape
    start, wait = zero_fill(de, z, zsem, LOOKUP_SHARE + NORM_SHARE, de.shape[0] // ZR)
    start()
    dc = 512

    @pl.loop(0, d // dc)
    def _(i):
        c = pl.ds(pl.multiple_of(i * dc, dc), dc)
        acc = jnp.zeros((dc, du_ref.shape[2]), jnp.float32)
        for m in range(mb):
            acc += lax.dot_general(n_ref[m, :, c], du_ref[m], (((0,), (0,)), ((), ())), preferred_element_type=jnp.float32)
        dw_ref[c, :] = acc

    wait()


def scatter_kernel(me_ref, rows_ref, cnt_ref, slot_ref, *refs):
    blocks, (de_in, de, buf, stage, sem, out_sem) = refs[:16], refs[16:]
    del de_in
    mb, t, d = buf.shape
    for c in pull(me_ref[0], blocks, buf, sem):
        c.wait()
    cnt = cnt_ref[0]
    cc = 512

    def copy(q, r):
        return pltpu.make_async_copy(stage.at[pl.ds(q, 1)], de.at[pl.ds(r, 1)], out_sem)

    @pl.loop(0, (cnt + BLK - 1) // BLK)
    def _(b):
        base = b * BLK
        ids = lax.broadcasted_iota(jnp.int32, (BLK, mb * t), 0) + base
        oh = (ids == slot_ref[...]).astype(jnp.bfloat16)
        for i in range(d // cc):
            acc = jnp.zeros((BLK, cc), jnp.float32)
            for m in range(mb):
                acc += jnp.dot(oh[:, m * t:(m + 1) * t], buf[m, :, i * cc:(i + 1) * cc], preferred_element_type=jnp.float32)
            stage[:, i * cc:(i + 1) * cc] = acc
        n = jnp.minimum(cnt - base, BLK)
        pl.loop(0, n)(lambda q: copy(q, rows_ref[base + q]).start())
        pl.loop(0, n)(lambda q: copy(q, rows_ref[base + q]).wait())


def solution(mesh):
    groups = mesh.shape["tp"]

    def swap(v, bit):
        return lax.ppermute(v, "tp", [(i, i ^ bit) for i in range(groups)])

    def local(ids, emb, g, w, du, dres):
        r = lax.axis_index("tp")
        mb, t = ids.shape
        vl, d = emb.shape
        f = w.shape[1]
        tl = t // groups
        hd = d // 2
        tc = t // 4
        k, c = r & 1, r >> 1
        gf = g.astype(jnp.float32)
        me = r.reshape(1)
        kc = jnp.stack([k, c]).astype(jnp.int32)
        de_shape = jax.ShapeDtypeStruct((vl, d), jnp.float32)
        zero_scratch = [pltpu.VMEM((ZR, d), jnp.float32), pltpu.SemaphoreType.DMA]

        def half_shape(nj):
            return jax.ShapeDtypeStruct((nj, mb, tc, hd), jnp.bfloat16)

        def pdn(js):
            mine, theirs = pl.pallas_call(
                functools.partial(pdn_kernel, js),
                out_shape=(half_shape(len(js)),) * 2,
                in_specs=[SMEM, VMEM, VMEM],
                out_specs=(VMEM, VMEM),
                cost_estimate=pl.CostEstimate(flops=5_000_000 * len(js), bytes_accessed=8_000_000, transcendentals=0),
                compiler_params=pltpu.CompilerParams(vmem_limit_bytes=40 * 2**20),
            )(kc, du, w)
            got = swap(theirs, 1)
            return {j: (mine[i], got[i]) for i, j in enumerate(js)}

        def reduce_to_home(pairs, dt):
            def part(j, h):
                a, b = pairs[j]
                return a[:, h * tl:(h + 1) * tl].astype(dt) + b[:, h * tl:(h + 1) * tl].astype(dt)

            dx_ = swap(part(3, 0), 2)
            dy_ = swap(part(3, 1), 4)
            ex = swap(part(1, 0), 2)
            ey = swap(part(2, 1), 4)
            pairs = dict(pairs)
            pairs[2], dx_ = lax.optimization_barrier((pairs[2], dx_))
            pairs[1], dy_ = lax.optimization_barrier((pairs[1], dy_))
            fy = swap(part(2, 0) + dx_, 4)
            fx = swap(part(1, 1) + dy_, 2)
            pairs[0], ex, ey = lax.optimization_barrier((pairs[0], ex, ey))
            return part(0, 0) + ex + fy, part(0, 1) + ey + fx

        def to_rows(mine, other):
            return jnp.where(k == 0, jnp.concatenate([mine, other], -1), jnp.concatenate([other, mine], -1))

        def go_home(s0, s1):
            keep = jnp.where(k == 0, s0, s1)
            give = jnp.where(k == 0, s1, s0)
            return to_rows(keep, swap(give, 1))

        def gather_all(own):
            x1, y0 = swap(own[1], 2), swap(own[0], 4)
            x0, y1 = swap(own[0], 2), swap(own[1], 4)
            d1, d0 = swap(x1, 4), swap(y0, 2)
            out = {0: own, 2: (x0, x1), 4: (y0, y1), 6: (d0, d1)}
            for j in (0, 2, 4, 6):
                out[j + 1] = tuple(swap(b, 1) for b in out[j])
            return out

        flat = ids.reshape(-1)
        n = flat.shape[0]
        loc = flat - r * vl
        own = (loc >= 0) & (loc < vl)
        pairs = pdn((3,))
        pairs.update(pdn((1, 2, 0)))
        tgt = jnp.where(own, 2 * (jnp.arange(n) % tc) + (loc & 1), -1).astype(jnp.int32)
        mine, theirs, de = pl.pallas_call(
            lookup_kernel,
            out_shape=(half_shape(4), half_shape(4), de_shape),
            in_specs=[SMEM, SMEM, VMEM, ANY],
            out_specs=(VMEM, VMEM, ANY),
            scratch_shapes=[pltpu.VMEM((2 * n, d), jnp.bfloat16), pltpu.SemaphoreType.DMA] + zero_scratch,
            cost_estimate=pl.CostEstimate(flops=40_000_000, bytes_accessed=60_000_000, transcendentals=0),
            compiler_params=pltpu.CompilerParams(vmem_limit_bytes=40 * 2**20),
            name="lookup",
        )(kc, loc, tgt.reshape(n, 1), emb)
        got = swap(theirs, 1)
        xpairs = {j: (mine[j], got[j]) for j in range(4)}

        dn = go_home(*reduce_to_home(pairs, jnp.float32))
        i0 = lax.broadcasted_iota(jnp.int32, (n, n), 0)
        i1 = lax.broadcasted_iota(jnp.int32, (n, n), 1)
        same = flat[:, None] == flat[None, :]
        first = jnp.min(jnp.where(same, i0, n), axis=0)
        lead = own & (first == jnp.arange(n))
        pos = jnp.sum(jnp.where(lead[:, None] & (i0 < i1), 1, 0), axis=0)
        pos_of_first = jnp.sum(jnp.where((i0 == first[None, :]), pos[:, None], 0), axis=0)
        slot = jnp.where(own, pos_of_first, -1).astype(jnp.int32)
        rows = jnp.sum(jnp.where(lead[:, None] & (pos[:, None] == i1), loc[:, None], 0), axis=0).astype(jnp.int32)
        cnt = jnp.sum(lead.astype(jnp.int32)).reshape(1)
        x0, x1 = reduce_to_home(xpairs, jnp.bfloat16)
        x0, x1, slot, rows, cnt = lax.optimization_barrier((x0, x1, slot, rows, cnt))
        xo = gather_all((x0, x1))
        xs = [xo[2 * j + q][h] for j in range(4) for h in range(2) for q in range(2)]
        x = to_rows(jnp.where(k == 0, x0, x1), jnp.where(k == 0, xo[1][0], xo[1][1]))

        nn, u, de = pl.pallas_call(
            norm_kernel,
            out_shape=(jax.ShapeDtypeStruct((mb, t, d), jnp.bfloat16), jax.ShapeDtypeStruct((mb, t, f), jnp.bfloat16), de_shape),
            in_specs=[SMEM, VMEM, VMEM] + [ANY] * 17,
            out_specs=(VMEM, VMEM, ANY),
            scratch_shapes=[pltpu.SemaphoreType.DMA((16,))] + zero_scratch,
            input_output_aliases={19: 2},
            cost_estimate=pl.CostEstimate(flops=30_000_000, bytes_accessed=40_000_000, transcendentals=0),
            compiler_params=pltpu.CompilerParams(vmem_limit_bytes=40 * 2**20),
            name="norm",
        )(kc, g.reshape(1, d), w, *xs, de)
        dw, de = pl.pallas_call(
            dw_kernel,
            out_shape=(jax.ShapeDtypeStruct((d, f), jnp.float32), de_shape),
            in_specs=[VMEM, VMEM, ANY],
            out_specs=(VMEM, ANY),
            scratch_shapes=zero_scratch,
            input_output_aliases={2: 1},
            cost_estimate=pl.CostEstimate(flops=30_000_000, bytes_accessed=40_000_000, transcendentals=0),
            compiler_params=pltpu.CompilerParams(vmem_limit_bytes=40 * 2**20),
            name="dw",
        )(nn, du, de)

        xf = x.astype(jnp.float32)
        rs = lax.rsqrt(jnp.mean(xf * xf, axis=-1, keepdims=True) + EPS)
        nh = xf * rs
        gdn = gf * dn
        dxn = rs * (gdn - nh * jnp.mean(nh * gdn, axis=-1, keepdims=True))
        dx = (dres.astype(jnp.float32) + dxn).astype(jnp.bfloat16)
        dg = jnp.sum(dn * nh, axis=(0, 1))
        dxo = gather_all((dx[:mb // 2], dx[mb // 2:]))
        dxs = [b for j in range(8) for b in dxo[j]]
        for bit in (1, 2, 4):
            dg = dg + swap(dg, bit)

        de = pl.pallas_call(
            scatter_kernel,
            out_shape=de_shape,
            in_specs=[SMEM, SMEM, SMEM, VMEM] + [ANY] * 17,
            out_specs=ANY,
            scratch_shapes=[
                pltpu.VMEM((mb, t, d), jnp.bfloat16),
                pltpu.VMEM((BLK, d), jnp.float32),
                pltpu.SemaphoreType.DMA((16,)),
                pltpu.SemaphoreType.DMA,
            ],
            input_output_aliases={20: 0},
            name="put_rows",
        )(me, rows, cnt, slot.reshape(1, n), *dxs, de)
        return u, x, de, dw, dg

    return jax.shard_map(
        local,
        mesh=mesh,
        in_specs=(P("dp", None), P("tp", None), P(None), P(None, "tp"), P("dp", None, "tp"), P("dp", "tp", None)),
        out_specs=(P("dp", None, "tp"), P("dp", "tp", None), P(("dp", "tp"), None), P(None, ("dp", "tp")), P("dp")),
        check_vma=False,
    )
```

```python
import functools

import jax
import jax.numpy as jnp
from jax import lax
from jax.experimental import pallas as pl
from jax.experimental.pallas import tpu as pltpu
from jax.sharding import PartitionSpec as P

EPS = 1e-6
ANY = pl.BlockSpec(memory_space=pl.ANY)
VMEM = pl.BlockSpec(memory_space=pltpu.VMEM)
SMEM = pl.BlockSpec(memory_space=pltpu.SMEM)
ZR = 128
BLK = 256
LOOKUP_EARLY, LOOKUP_SHARE, NORM_SHARE = 14, 28, 5


def zero_fill(de, z, sem, first, last):

    def copy(i):
        return pltpu.make_async_copy(z, de.at[pl.ds(pl.multiple_of(i * ZR, ZR), ZR)], sem)

    def start(clear=True):
        if clear:
            z[...] = jnp.zeros_like(z)
        pl.loop(first, last)(lambda i: copy(i).start())

    def wait():
        pl.loop(first, last)(lambda i: copy(i).wait())

    return start, wait


def pdn_kernel(js, c_ref, du_ref, w_ref, *outs):
    c = c_ref[0]
    mb, t, _ = du_ref.shape
    tc, wc = t // 4, 512
    tl = tc // 2
    for i, j in enumerate(js):
        z = pl.multiple_of(jnp.bitwise_xor(c, j) * tc, tc)
        rows = jnp.concatenate([du_ref[m, pl.ds(z, tc), :] for m in range(mb)], axis=0)
        for n in range(w_ref.shape[0] // wc):
            cols = slice(n * wc, (n + 1) * wc)
            v = lax.dot_general(rows, w_ref[cols, :], (((1,), (1,)), ((), ())), preferred_element_type=jnp.float32)
            v = v.astype(jnp.bfloat16).reshape(mb, tc, wc)
            for h in range(2):
                outs[2 * i + h][:, :, cols] = v[:, h * tl:(h + 1) * tl]


def lookup_kernel(kc_ref, loc_ref, tgt_ref, emb, mine_ref, theirs_ref, de, buf, sem, z, zsem):
    k, c = kc_ref[0], kc_ref[1]
    vl, d = emb.shape
    nj, mb, tc, hd = mine_ref.shape
    n = nj * mb * tc
    step = 64
    start, wait = zero_fill(de, z, zsem, 0, LOOKUP_EARLY)
    late_start, late_wait = zero_fill(de, z, zsem, LOOKUP_EARLY, LOOKUP_SHARE)
    start()

    @pl.loop(0, 2 * n // step)
    def _(i):
        buf[pl.ds(pl.multiple_of(i * step, step), step), :] = jnp.zeros((step, d), buf.dtype)

    def copy(t, l):
        src = emb.at[pl.ds(pl.multiple_of((l >> 1) * 2, 2), 2)]
        return pltpu.make_async_copy(src, buf.at[pl.ds(pl.multiple_of(t * 2, 2), 2)], sem)

    def issue(i, cnt):
        for q in range(8):
            t = i * 8 + q
            l = loc_ref[t]
            own = (l >= 0) & (l < vl)

            @pl.when(own)
            def _():
                copy(t, l).start()

            cnt = cnt + own.astype(jnp.int32)
        return cnt

    cnt = lax.fori_loop(0, n // 8, issue, jnp.int32(0))

    @pl.loop(0, cnt)
    def _(i):
        copy(0, 0).wait()

    late_start(False)

    for j in range(nj):
        zc = jnp.bitwise_xor(c, j)

        @pl.loop(0, mb)
        def _(m):
            t0 = m * (nj * tc) + zc * tc
            tgt = tgt_ref[pl.ds(pl.multiple_of(t0, tc), tc), :]
            sel = (lax.broadcasted_iota(jnp.int32, (tc, 2 * tc), 1) == tgt).astype(jnp.bfloat16)
            rows = pl.ds(pl.multiple_of(2 * t0, 2 * tc), 2 * tc)
            for out, half in ((theirs_ref, 1 - k), (mine_ref, k)):
                v = buf[rows, pl.ds(pl.multiple_of(half * hd, 128), hd)]
                out[j, m] = jnp.dot(sel, v, preferred_element_type=jnp.float32).astype(jnp.bfloat16)

    wait()
    late_wait()


def norm_kernel(j, kc_ref, g_ref, w_ref, *refs):
    blocks, (n_ref, u_ref, de, stage, sem, z, zsem) = refs[:4], refs[-7:]
    k = kc_ref[0]
    mb, tc, d = n_ref.shape
    tl, hd = blocks[0].shape[1:]
    first = LOOKUP_SHARE + j * NORM_SHARE
    start, wait = zero_fill(de, z, zsem, first, first + NORM_SHARE)
    start()
    at = [pl.ds(pl.multiple_of(jnp.bitwise_xor(k, q) * hd, 128), hd) for q in range(2)]
    gf = [g_ref[:, at[q]].astype(jnp.float32) for q in range(2)]

    @pl.loop(0, mb)
    def _(m):
        for h in range(2):
            xf = [blocks[2 * h + q][m].astype(jnp.float32) for q in range(2)]
            total = sum(jnp.sum(v * v, axis=-1, keepdims=True) for v in xf)
            rs = lax.rsqrt(total * (1.0 / d) + EPS)
            for q in range(2):
                n_ref[m, h * tl:(h + 1) * tl, at[q]] = (xf[q] * rs * gf[q]).astype(jnp.bfloat16)

    v = jnp.dot(n_ref[...].reshape(mb * tc, d), w_ref[...], preferred_element_type=jnp.float32)
    stage[...] = v.astype(jnp.bfloat16).reshape(stage.shape)
    rows = pl.ds(pl.multiple_of(jnp.bitwise_xor(kc_ref[1], j) * tc, tc), tc)
    copy = pltpu.make_async_copy(stage, u_ref.at[:, rows, :], sem)
    copy.start()
    copy.wait()
    wait()


def dw_kernel(c_ref, du_ref, *refs):
    ns, (dw_ref, de, z, zsem) = refs[:4], refs[-4:]
    mb, tc, d = ns[0].shape
    start, wait = zero_fill(de, z, zsem, LOOKUP_SHARE + 4 * NORM_SHARE, de.shape[0] // ZR)
    start()
    dc = 512

    @pl.loop(0, d // dc)
    def _(i):
        c = pl.ds(pl.multiple_of(i * dc, dc), dc)
        acc = jnp.zeros((dc, du_ref.shape[2]), jnp.float32)
        for j, n_ref in enumerate(ns):
            rows = pl.ds(pl.multiple_of(jnp.bitwise_xor(c_ref[0], j) * tc, tc), tc)
            left = jnp.concatenate([n_ref[m, :, c] for m in range(mb)], axis=0)
            right = jnp.concatenate([du_ref[m, rows, :] for m in range(mb)], axis=0)
            acc += lax.dot_general(left, right, (((0,), (0,)), ((), ())), preferred_element_type=jnp.float32)
        dw_ref[c, :] = acc

    wait()


def scatter_kernel(me_ref, rows_ref, cnt_ref, slot_ref, *refs):
    blocks, (de, buf, stage, out_sem) = refs[:16], refs[-4:]
    mb, t, d = buf.shape
    hb, tl = blocks[0].shape[:2]
    for i, b in enumerate(blocks):
        at = pl.ds(pl.multiple_of(jnp.bitwise_xor(me_ref[0], i // 2) * tl, tl), tl)
        for m in range(hb):
            buf[(i % 2) * hb + m, at, :] = b[m]
    cnt = cnt_ref[0]
    cc = 512

    def copy(q, r):
        return pltpu.make_async_copy(stage.at[pl.ds(q, 1)], de.at[pl.ds(r, 1)], out_sem)

    @pl.loop(0, (cnt + BLK - 1) // BLK)
    def _(b):
        base = b * BLK
        ids = lax.broadcasted_iota(jnp.int32, (BLK, mb * t), 0) + base
        oh = (ids == slot_ref[...]).astype(jnp.bfloat16)
        for i in range(d // cc):
            acc = jnp.zeros((BLK, cc), jnp.float32)
            for m in range(mb):
                acc += jnp.dot(oh[:, m * t:(m + 1) * t], buf[m, :, i * cc:(i + 1) * cc], preferred_element_type=jnp.float32)
            stage[:, i * cc:(i + 1) * cc] = acc
        n = jnp.minimum(cnt - base, BLK)
        pl.loop(0, n)(lambda q: copy(q, rows_ref[base + q]).start())
        pl.loop(0, n)(lambda q: copy(q, rows_ref[base + q]).wait())


def solution(mesh):
    groups = mesh.shape["tp"]

    def swap(v, bit):
        return lax.ppermute(v, "tp", [(i, i ^ bit) for i in range(groups)])

    def local(ids, emb, g, w, du, dres):
        r = lax.axis_index("tp")
        mb, t = ids.shape
        vl, d = emb.shape
        f = w.shape[1]
        tl = t // groups
        hd = d // 2
        tc = t // 4
        k, c = r & 1, r >> 1
        gf = g.astype(jnp.float32)
        me = r.reshape(1)
        kc = jnp.stack([k, c]).astype(jnp.int32)
        de_shape = jax.ShapeDtypeStruct((vl, d), jnp.float32)
        zero_scratch = [pltpu.VMEM((ZR, d), jnp.float32), pltpu.SemaphoreType.DMA]

        def half_shape(nj):
            return jax.ShapeDtypeStruct((nj, mb, tc, hd), jnp.bfloat16)

        def pdn(js):
            out = pl.pallas_call(
                functools.partial(pdn_kernel, js),
                out_shape=(jax.ShapeDtypeStruct((mb, tl, d), jnp.bfloat16),) * (2 * len(js)),
                in_specs=[SMEM, VMEM, VMEM],
                out_specs=(VMEM,) * (2 * len(js)),
                cost_estimate=pl.CostEstimate(flops=5_000_000 * len(js), bytes_accessed=8_000_000, transcendentals=0),
                compiler_params=pltpu.CompilerParams(vmem_limit_bytes=40 * 2**20),
            )(c.reshape(1), du, w)
            return {j: out[2 * i:2 * i + 2] for i, j in enumerate(js)}

        def pick(a, b):
            return jnp.where(k == 0, a, b)

        def f32(v):
            return v.astype(jnp.float32)

        def reduce_to_home(pairs, dt):
            def part(j, h):
                a, b = pairs[j]
                return a[:, h * tl:(h + 1) * tl].astype(dt) + b[:, h * tl:(h + 1) * tl].astype(dt)

            dx_ = swap(part(3, 0), 2)
            dy_ = swap(part(3, 1), 4)
            ex = swap(part(1, 0), 2)
            ey = swap(part(2, 1), 4)
            pairs = dict(pairs)
            pairs[2], dx_ = lax.optimization_barrier((pairs[2], dx_))
            pairs[1], dy_ = lax.optimization_barrier((pairs[1], dy_))
            fy = swap(part(2, 0) + dx_, 4)
            fx = swap(part(1, 1) + dy_, 2)
            pairs[0], ex, ey = lax.optimization_barrier((pairs[0], ex, ey))
            return part(0, 0) + ex + fy, part(0, 1) + ey + fx

        def to_rows(mine, other):
            return jnp.where(k == 0, jnp.concatenate([mine, other], -1), jnp.concatenate([other, mine], -1))

        def gather_all(own):
            x1, y0 = swap(own[1], 2), swap(own[0], 4)
            x0, y1 = swap(own[0], 2), swap(own[1], 4)
            d1, d0 = swap(x1, 4), swap(y0, 2)
            out = {0: own, 2: (x0, x1), 4: (y0, y1), 6: (d0, d1)}
            for j in (0, 2, 4, 6):
                out[j + 1] = tuple(swap(b, 1) for b in out[j])
            return out

        flat = ids.reshape(-1)
        n = flat.shape[0]
        loc = flat - r * vl
        own = (loc >= 0) & (loc < vl)
        part = pdn((3,))
        part.update(pdn((1, 2)))
        part.update(pdn((0,)))
        d0, d1 = swap(part[3][0], 2), swap(part[3][1], 4)
        ex, ey = swap(part[1][0], 2), swap(part[2][1], 4)
        tgt = jnp.where(own, 2 * (jnp.arange(n) % tc) + (loc & 1), -1).astype(jnp.int32)
        i0 = lax.broadcasted_iota(jnp.int32, (n, n), 0)
        i1 = lax.broadcasted_iota(jnp.int32, (n, n), 1)
        same = flat[:, None] == flat[None, :]
        first = jnp.min(jnp.where(same, i0, n), axis=0)
        lead = own & (first == jnp.arange(n))
        pos = jnp.sum(jnp.where(lead[:, None] & (i0 < i1), 1, 0), axis=0)
        pos_of_first = jnp.sum(jnp.where((i0 == first[None, :]), pos[:, None], 0), axis=0)
        slot = jnp.where(own, pos_of_first, -1).astype(jnp.int32)
        rows = jnp.sum(jnp.where(lead[:, None] & (pos[:, None] == i1), loc[:, None], 0), axis=0).astype(jnp.int32)
        cnt = jnp.sum(lead.astype(jnp.int32)).reshape(1)
        d0, d1, loc, tgt, slot, rows, cnt = lax.optimization_barrier((d0, d1, loc, tgt, slot, rows, cnt))
        ty, tx = f32(part[2][0]) + f32(d0), f32(part[1][1]) + f32(d1)
        gy = swap(pick(ty[..., hd:], ty[..., :hd]), 1)
        gx = swap(pick(tx[..., hd:], tx[..., :hd]), 1)
        fy = swap(pick(ty[..., :hd], ty[..., hd:]) + gy, 4)
        fx = swap(pick(tx[..., :hd], tx[..., hd:]) + gx, 2)

        mine, theirs, de = pl.pallas_call(
            lookup_kernel,
            out_shape=(half_shape(4), half_shape(4), de_shape),
            in_specs=[SMEM, SMEM, VMEM, ANY],
            out_specs=(VMEM, VMEM, ANY),
            scratch_shapes=[pltpu.VMEM((2 * n, d), jnp.bfloat16), pltpu.SemaphoreType.DMA] + zero_scratch,
            cost_estimate=pl.CostEstimate(flops=40_000_000, bytes_accessed=60_000_000, transcendentals=0),
            compiler_params=pltpu.CompilerParams(vmem_limit_bytes=40 * 2**20),
            name="lookup",
        )(kc, loc, tgt.reshape(n, 1), emb)
        got = swap(theirs, 1)
        xpairs = {j: (mine[j], got[j]) for j in range(4)}

        def widen(v):
            o = jnp.zeros_like(v)
            return to_rows(v, o)

        v0 = f32(part[0][0]) + f32(ex) + widen(fy)
        v1 = f32(part[0][1]) + f32(ey) + widen(fx)
        dn = pick(v0, v1) + swap(pick(v1, v0), 1)
        x0, x1 = reduce_to_home(xpairs, jnp.bfloat16)
        xo = gather_all((x0, x1))
        x = to_rows(jnp.where(k == 0, x0, x1), jnp.where(k == 0, xo[1][0], xo[1][1]))

        ns, u = [], None
        for j in range(4):
            more = (de,) if u is None else (u, de)
            nj, u, de = pl.pallas_call(
                functools.partial(norm_kernel, j),
                out_shape=(jax.ShapeDtypeStruct((mb, tc, d), jnp.bfloat16), jax.ShapeDtypeStruct((mb, t, f), jnp.bfloat16), de_shape),
                in_specs=[SMEM] + [VMEM] * 6 + [ANY] * len(more),
                out_specs=(VMEM, ANY, ANY),
                scratch_shapes=[pltpu.VMEM((mb, tc, f), jnp.bfloat16), pltpu.SemaphoreType.DMA] + zero_scratch,
                input_output_aliases={7 + i: 3 - len(more) + i for i in range(len(more))},
                cost_estimate=pl.CostEstimate(flops=8_000_000, bytes_accessed=12_000_000, transcendentals=0),
                compiler_params=pltpu.CompilerParams(vmem_limit_bytes=40 * 2**20),
            )(kc, g.reshape(1, d), w, *(xo[2 * j + q][h] for h in range(2) for q in range(2)), *more)
            ns.append(nj)
        dw, de = pl.pallas_call(
            dw_kernel,
            out_shape=(jax.ShapeDtypeStruct((d, f), jnp.float32), de_shape),
            in_specs=[SMEM] + [VMEM] * 5 + [ANY],
            out_specs=(VMEM, ANY),
            scratch_shapes=zero_scratch,
            input_output_aliases={6: 1},
            cost_estimate=pl.CostEstimate(flops=30_000_000, bytes_accessed=40_000_000, transcendentals=0),
            compiler_params=pltpu.CompilerParams(vmem_limit_bytes=40 * 2**20),
            name="dw",
        )(c.reshape(1), du, *ns, de)

        xf = x.astype(jnp.float32)
        rs = lax.rsqrt(jnp.mean(xf * xf, axis=-1, keepdims=True) + EPS)
        nh = xf * rs
        gdn = gf * dn
        dxn = rs * (gdn - nh * jnp.mean(nh * gdn, axis=-1, keepdims=True))
        dx = (dres.astype(jnp.float32) + dxn).astype(jnp.bfloat16)
        dg = jnp.sum(dn * nh, axis=(0, 1))
        dxo = gather_all((dx[:mb // 2], dx[mb // 2:]))
        dxs = [b for j in range(8) for b in dxo[j]]
        for bit in (1, 2, 4):
            dg = dg + swap(dg, bit)

        de = pl.pallas_call(
            scatter_kernel,
            out_shape=de_shape,
            in_specs=[SMEM, SMEM, SMEM, VMEM] + [VMEM] * 16 + [ANY],
            out_specs=ANY,
            scratch_shapes=[
                pltpu.VMEM((mb, t, d), jnp.bfloat16),
                pltpu.VMEM((BLK, d), jnp.float32),
                pltpu.SemaphoreType.DMA,
            ],
            input_output_aliases={20: 0},
            compiler_params=pltpu.CompilerParams(vmem_limit_bytes=40 * 2**20),
            name="put_rows",
        )(me, rows, cnt, slot.reshape(1, n), *dxs, de)
        return u, x, de, dw, dg

    return jax.shard_map(
        local,
        mesh=mesh,
        in_specs=(P("dp", None), P("tp", None), P(None), P(None, "tp"), P("dp", None, "tp"), P("dp", "tp", None)),
        out_specs=(P("dp", None, "tp"), P("dp", "tp", None), P(("dp", "tp"), None), P(None, ("dp", "tp")), P("dp")),
        check_vma=False,
    )
```

```python
import functools

import jax
import jax.numpy as jnp
from jax import lax
from jax.experimental import pallas as pl
from jax.experimental.pallas import tpu as pltpu
from jax.sharding import PartitionSpec as P

EPS = 1e-6
ANY = pl.BlockSpec(memory_space=pl.ANY)
VMEM = pl.BlockSpec(memory_space=pltpu.VMEM)
SMEM = pl.BlockSpec(memory_space=pltpu.SMEM)
HBM = pl.BlockSpec(memory_space=pltpu.HBM)
ZR = 128
BLK = 256
LOOKUP_EARLY, LOOKUP_SHARE, NORM_SHARE = 14, 28, 5


def zero_fill(de, z, sem, first, last):

    def copy(i):
        return pltpu.make_async_copy(z, de.at[pl.ds(pl.multiple_of(i * ZR, ZR), ZR)], sem)

    def start(clear=True):
        if clear:
            z[...] = jnp.zeros_like(z)
        pl.loop(first, last)(lambda i: copy(i).start())

    def wait():
        pl.loop(first, last)(lambda i: copy(i).wait())

    return start, wait


def pdn_first_kernel(j, c_ref, du_hbm, w_hbm, h0, h1, du_ref, w_ref, sem, wsem):
    c = c_ref[0]
    mb, tc, _ = du_ref.shape
    tl = tc // 2
    wc = 512
    steps = w_hbm.shape[0] // wc
    z = pl.multiple_of(jnp.bitwise_xor(c, j) * tc, tc)
    rows_in = pltpu.make_async_copy(du_hbm.at[:, pl.ds(z, tc), :], du_ref, sem)
    rows_in.start()
    loads = [pltpu.make_async_copy(w_hbm.at[pl.ds(n * wc, wc)], w_ref.at[pl.ds(n * wc, wc)], wsem.at[n]) for n in range(steps)]
    for cp in loads:
        cp.start()
    rows_in.wait()
    rows = du_ref[...].reshape(mb * tc, du_ref.shape[2])
    for n in range(steps):
        loads[n].wait()
        cols = slice(n * wc, (n + 1) * wc)
        v = lax.dot_general(rows, w_ref[cols, :], (((1,), (1,)), ((), ())), preferred_element_type=jnp.float32)
        v = v.astype(jnp.bfloat16).reshape(mb, tc, wc)
        h0[:, :, cols] = v[:, :tl]
        h1[:, :, cols] = v[:, tl:]


def pdn_kernel(js, c_ref, du_ref, w_ref, *outs):
    c = c_ref[0]
    mb, t, _ = du_ref.shape
    tc, wc = t // 4, 512
    tl = tc // 2
    for i, j in enumerate(js):
        z = pl.multiple_of(jnp.bitwise_xor(c, j) * tc, tc)
        rows = jnp.concatenate([du_ref[m, pl.ds(z, tc), :] for m in range(mb)], axis=0)
        for n in range(w_ref.shape[0] // wc):
            cols = slice(n * wc, (n + 1) * wc)
            v = lax.dot_general(rows, w_ref[cols, :], (((1,), (1,)), ((), ())), preferred_element_type=jnp.float32)
            v = v.astype(jnp.bfloat16).reshape(mb, tc, wc)
            for h in range(2):
                outs[2 * i + h][:, :, cols] = v[:, h * tl:(h + 1) * tl]


def lookup_kernel(kc_ref, loc_ref, tgt_ref, emb, mine_ref, far_ref, near_ref, de, buf, sem, z, zsem):
    k, c = kc_ref[0], kc_ref[1]
    vl, d = emb.shape
    nj, mb, tc, hd = mine_ref.shape
    n = nj * mb * tc
    step = 64
    start, wait = zero_fill(de, z, zsem, 0, LOOKUP_EARLY)
    late_start, late_wait = zero_fill(de, z, zsem, LOOKUP_EARLY, LOOKUP_SHARE)
    start()

    @pl.loop(0, 2 * n // step)
    def _(i):
        buf[pl.ds(pl.multiple_of(i * step, step), step), :] = jnp.zeros((step, d), buf.dtype)

    def copy(t, l):
        src = emb.at[pl.ds(pl.multiple_of((l >> 1) * 2, 2), 2)]
        return pltpu.make_async_copy(src, buf.at[pl.ds(pl.multiple_of(t * 2, 2), 2)], sem)

    def issue(i, cnt):
        for q in range(8):
            t = i * 8 + q
            l = loc_ref[t]
            own = (l >= 0) & (l < vl)

            @pl.when(own)
            def _():
                copy(t, l).start()

            cnt = cnt + own.astype(jnp.int32)
        return cnt

    cnt = lax.fori_loop(0, n // 8, issue, jnp.int32(0))

    @pl.loop(0, cnt)
    def _(i):
        copy(0, 0).wait()

    late_start(False)

    for j in range(nj):
        theirs = far_ref.at[0] if j == 3 else near_ref.at[j]
        zc = jnp.bitwise_xor(c, j)

        @pl.loop(0, mb)
        def _(m):
            t0 = m * (nj * tc) + zc * tc
            tgt = tgt_ref[pl.ds(pl.multiple_of(t0, tc), tc), :]
            sel = (lax.broadcasted_iota(jnp.int32, (tc, 2 * tc), 1) == tgt).astype(jnp.bfloat16)
            rows = pl.ds(pl.multiple_of(2 * t0, 2 * tc), 2 * tc)
            for out, half in ((theirs, 1 - k), (mine_ref.at[j], k)):
                v = buf[rows, pl.ds(pl.multiple_of(half * hd, 128), hd)]
                out[m] = jnp.dot(sel, v, preferred_element_type=jnp.float32).astype(jnp.bfloat16)

    wait()
    late_wait()


def norm_kernel(j, kc_ref, g_ref, w_ref, *refs):
    blocks, (n_ref, u_ref, de, stage, sem, z, zsem) = refs[:4], refs[-7:]
    k = kc_ref[0]
    mb, tc, d = n_ref.shape
    tl, hd = blocks[0].shape[1:]
    first = LOOKUP_SHARE + j * NORM_SHARE
    start, wait = zero_fill(de, z, zsem, first, first + NORM_SHARE)
    start()
    at = [pl.ds(pl.multiple_of(jnp.bitwise_xor(k, q) * hd, 128), hd) for q in range(2)]
    gf = [g_ref[:, at[q]].astype(jnp.float32) for q in range(2)]

    @pl.loop(0, mb)
    def _(m):
        for h in range(2):
            xf = [blocks[2 * h + q][m].astype(jnp.float32) for q in range(2)]
            total = sum(jnp.sum(v * v, axis=-1, keepdims=True) for v in xf)
            rs = lax.rsqrt(total * (1.0 / d) + EPS)
            for q in range(2):
                n_ref[m, h * tl:(h + 1) * tl, at[q]] = (xf[q] * rs * gf[q]).astype(jnp.bfloat16)

    v = jnp.dot(n_ref[...].reshape(mb * tc, d), w_ref[...], preferred_element_type=jnp.float32)
    stage[...] = v.astype(jnp.bfloat16).reshape(stage.shape)
    rows = pl.ds(pl.multiple_of(jnp.bitwise_xor(kc_ref[1], j) * tc, tc), tc)
    copy = pltpu.make_async_copy(stage, u_ref.at[:, rows, :], sem)
    copy.start()
    copy.wait()
    wait()


def dw_kernel(c_ref, du_ref, *refs):
    ns, (dw, de, stage, sem, z, zsem) = refs[:4], refs[-6:]
    mb, tc, d = ns[0].shape
    start, wait = zero_fill(de, z, zsem, LOOKUP_SHARE + 4 * NORM_SHARE, de.shape[0] // ZR)
    start()
    dc = stage.shape[1]
    copies = []
    for i in range(d // dc):
        acc = jnp.zeros(stage.shape[1:], jnp.float32)
        for j, n_ref in enumerate(ns):
            rows = pl.ds(pl.multiple_of(jnp.bitwise_xor(c_ref[0], j) * tc, tc), tc)
            left = jnp.concatenate([n_ref[m, :, i * dc:(i + 1) * dc] for m in range(mb)], axis=0)
            right = jnp.concatenate([du_ref[m, rows, :] for m in range(mb)], axis=0)
            acc += lax.dot_general(left, right, (((0,), (0,)), ((), ())), preferred_element_type=jnp.float32)
        if i >= 2:
            copies[i - 2].wait()
        stage[i % 2] = acc
        copies.append(pltpu.make_async_copy(stage.at[i % 2], dw.at[pl.ds(i * dc, dc)], sem.at[i % 2]))
        copies[i].start()
    for cp in copies[-2:]:
        cp.wait()
    wait()


def scatter_kernel(me_ref, rows_ref, cnt_ref, slot_ref, *refs):
    blocks, (de, buf, stage, out_sem) = refs[:16], refs[-4:]
    mb, t, d = buf.shape
    hb, tl = blocks[0].shape[:2]
    for i, b in enumerate(blocks):
        at = pl.ds(pl.multiple_of(jnp.bitwise_xor(me_ref[0], i // 2) * tl, tl), tl)
        for m in range(hb):
            buf[(i % 2) * hb + m, at, :] = b[m]
    cnt = cnt_ref[0]
    cc = 512

    def copy(q, r):
        return pltpu.make_async_copy(stage.at[pl.ds(q, 1)], de.at[pl.ds(r, 1)], out_sem)

    @pl.loop(0, (cnt + BLK - 1) // BLK)
    def _(b):
        base = b * BLK
        ids = lax.broadcasted_iota(jnp.int32, (BLK, mb * t), 0) + base
        oh = (ids == slot_ref[...]).astype(jnp.bfloat16)
        for i in range(d // cc):
            acc = jnp.zeros((BLK, cc), jnp.float32)
            for m in range(mb):
                acc += jnp.dot(oh[:, m * t:(m + 1) * t], buf[m, :, i * cc:(i + 1) * cc], preferred_element_type=jnp.float32)
            stage[:, i * cc:(i + 1) * cc] = acc
        n = jnp.minimum(cnt - base, BLK)
        pl.loop(0, n)(lambda q: copy(q, rows_ref[base + q]).start())
        pl.loop(0, n)(lambda q: copy(q, rows_ref[base + q]).wait())


def solution(mesh):
    groups = mesh.shape["tp"]

    def swap(v, bit):
        return lax.ppermute(v, "tp", [(i, i ^ bit) for i in range(groups)])

    def local(ids, emb, g, w, du, dres):
        r = lax.axis_index("tp")
        mb, t = ids.shape
        vl, d = emb.shape
        f = w.shape[1]
        tl = t // groups
        hd = d // 2
        tc = t // 4
        k, c = r & 1, r >> 1
        gf = g.astype(jnp.float32)
        me = r.reshape(1)
        kc = jnp.stack([k, c]).astype(jnp.int32)
        de_shape = jax.ShapeDtypeStruct((vl, d), jnp.float32)
        zero_scratch = [pltpu.VMEM((ZR, d), jnp.float32), pltpu.SemaphoreType.DMA]

        def half_shape(nj):
            return jax.ShapeDtypeStruct((nj, mb, tc, hd), jnp.bfloat16)

        def pdn(js):
            out = pl.pallas_call(
                functools.partial(pdn_kernel, js),
                out_shape=(jax.ShapeDtypeStruct((mb, tl, d), jnp.bfloat16),) * (2 * len(js)),
                in_specs=[SMEM, VMEM, VMEM],
                out_specs=(VMEM,) * (2 * len(js)),
                cost_estimate=pl.CostEstimate(flops=5_000_000 * len(js), bytes_accessed=8_000_000, transcendentals=0),
                compiler_params=pltpu.CompilerParams(vmem_limit_bytes=40 * 2**20),
            )(c.reshape(1), du, w)
            return {j: out[2 * i:2 * i + 2] for i, j in enumerate(js)}

        def pick(a, b):
            return jnp.where(k == 0, a, b)

        def f32(v):
            return v.astype(jnp.float32)

        def reduce_to_home(pairs, dt):
            def part(j, h):
                a, b = pairs[j]
                return a[:, h * tl:(h + 1) * tl].astype(dt) + b[:, h * tl:(h + 1) * tl].astype(dt)

            dx_ = swap(part(3, 0), 2)
            dy_ = swap(part(3, 1), 4)
            ex = swap(part(1, 0), 2)
            ey = swap(part(2, 1), 4)
            pairs = dict(pairs)
            pairs[2], dx_ = lax.optimization_barrier((pairs[2], dx_))
            pairs[1], dy_ = lax.optimization_barrier((pairs[1], dy_))
            fy = swap(part(2, 0) + dx_, 4)
            fx = swap(part(1, 1) + dy_, 2)
            pairs[0], ex, ey = lax.optimization_barrier((pairs[0], ex, ey))
            return part(0, 0) + ex + fy, part(0, 1) + ey + fx

        def to_rows(mine, other):
            return jnp.where(k == 0, jnp.concatenate([mine, other], -1), jnp.concatenate([other, mine], -1))

        def gather_all(own):
            x1, y0 = swap(own[1], 2), swap(own[0], 4)
            x0, y1 = swap(own[0], 2), swap(own[1], 4)
            d1, d0 = swap(x1, 4), swap(y0, 2)
            out = {0: own, 2: (x0, x1), 4: (y0, y1), 6: (d0, d1)}
            for j in (0, 2, 4, 6):
                out[j + 1] = tuple(swap(b, 1) for b in out[j])
            return out

        flat = ids.reshape(-1)
        n = flat.shape[0]
        loc = flat - r * vl
        own = (loc >= 0) & (loc < vl)
        part = {3: pl.pallas_call(
            functools.partial(pdn_first_kernel, 3),
            out_shape=(jax.ShapeDtypeStruct((mb, tl, d), jnp.bfloat16),) * 2,
            in_specs=[SMEM, HBM, HBM],
            out_specs=(VMEM, VMEM),
            scratch_shapes=[
                pltpu.VMEM((mb, tc, f), jnp.bfloat16),
                pltpu.VMEM((d, f), jnp.bfloat16),
                pltpu.SemaphoreType.DMA,
                pltpu.SemaphoreType.DMA((6,)),
            ],
            cost_estimate=pl.CostEstimate(flops=5_000_000, bytes_accessed=8_000_000, transcendentals=0),
            compiler_params=pltpu.CompilerParams(vmem_limit_bytes=63 * 2**20),
            name="pdn_a",
        )(c.reshape(1), du, w)}
        part.update(pdn((1, 2)))
        part.update(pdn((0,)))
        d0, d1 = swap(part[3][0], 2), swap(part[3][1], 4)
        ex, ey = swap(part[1][0], 2), swap(part[2][1], 4)
        tgt = jnp.where(own, 2 * (jnp.arange(n) % tc) + (loc & 1), -1).astype(jnp.int32)
        i0 = lax.broadcasted_iota(jnp.int32, (n, n), 0)
        i1 = lax.broadcasted_iota(jnp.int32, (n, n), 1)
        same = flat[:, None] == flat[None, :]
        first = jnp.min(jnp.where(same, i0, n), axis=0)
        lead = own & (first == jnp.arange(n))
        pos = jnp.sum(jnp.where(lead[:, None] & (i0 < i1), 1, 0), axis=0)
        pos_of_first = jnp.sum(jnp.where((i0 == first[None, :]), pos[:, None], 0), axis=0)
        slot = jnp.where(own, pos_of_first, -1).astype(jnp.int32)
        rows = jnp.sum(jnp.where(lead[:, None] & (pos[:, None] == i1), loc[:, None], 0), axis=0).astype(jnp.int32)
        cnt = jnp.sum(lead.astype(jnp.int32)).reshape(1)
        d0, d1, loc, tgt, slot, rows, cnt = lax.optimization_barrier((d0, d1, loc, tgt, slot, rows, cnt))
        ty, tx = f32(part[2][0]) + f32(d0), f32(part[1][1]) + f32(d1)
        gy = swap(pick(ty[..., hd:], ty[..., :hd]), 1)
        gx = swap(pick(tx[..., hd:], tx[..., :hd]), 1)
        fy = swap(pick(ty[..., :hd], ty[..., hd:]) + gy, 4)
        fx = swap(pick(tx[..., :hd], tx[..., hd:]) + gx, 2)

        mine, far, near, de = pl.pallas_call(
            lookup_kernel,
            out_shape=(half_shape(4), half_shape(1), half_shape(3), de_shape),
            in_specs=[SMEM, SMEM, VMEM, ANY],
            out_specs=(VMEM, VMEM, VMEM, ANY),
            scratch_shapes=[pltpu.VMEM((2 * n, d), jnp.bfloat16), pltpu.SemaphoreType.DMA] + zero_scratch,
            cost_estimate=pl.CostEstimate(flops=40_000_000, bytes_accessed=60_000_000, transcendentals=0),
            compiler_params=pltpu.CompilerParams(vmem_limit_bytes=40 * 2**20),
            name="lookup",
        )(kc, loc, tgt.reshape(n, 1), emb)
        far, near = swap(far, 1), swap(near, 1)
        xpairs = {j: (mine[j], far[0] if j == 3 else near[j]) for j in range(4)}

        def widen(v):
            o = jnp.zeros_like(v)
            return to_rows(v, o)

        v0 = f32(part[0][0]) + f32(ex) + widen(fy)
        v1 = f32(part[0][1]) + f32(ey) + widen(fx)
        dn = pick(v0, v1) + swap(pick(v1, v0), 1)
        x0, x1 = reduce_to_home(xpairs, jnp.bfloat16)
        xo = gather_all((x0, x1))
        x = to_rows(jnp.where(k == 0, x0, x1), jnp.where(k == 0, xo[1][0], xo[1][1]))

        ns, u = [], None
        for j in range(4):
            more = (de,) if u is None else (u, de)
            nj, u, de = pl.pallas_call(
                functools.partial(norm_kernel, j),
                out_shape=(jax.ShapeDtypeStruct((mb, tc, d), jnp.bfloat16), jax.ShapeDtypeStruct((mb, t, f), jnp.bfloat16), de_shape),
                in_specs=[SMEM] + [VMEM] * 6 + [ANY] * len(more),
                out_specs=(VMEM, ANY, ANY),
                scratch_shapes=[pltpu.VMEM((mb, tc, f), jnp.bfloat16), pltpu.SemaphoreType.DMA] + zero_scratch,
                input_output_aliases={7 + i: 3 - len(more) + i for i in range(len(more))},
                cost_estimate=pl.CostEstimate(flops=8_000_000, bytes_accessed=12_000_000, transcendentals=0),
                compiler_params=pltpu.CompilerParams(vmem_limit_bytes=40 * 2**20),
            )(kc, g.reshape(1, d), w, *(xo[2 * j + q][h] for h in range(2) for q in range(2)), *more)
            ns.append(nj)
        dw, de = pl.pallas_call(
            dw_kernel,
            out_shape=(jax.ShapeDtypeStruct((d, f), jnp.float32), de_shape),
            in_specs=[SMEM] + [VMEM] * 5 + [ANY],
            out_specs=(ANY, ANY),
            scratch_shapes=[pltpu.VMEM((2, 512, f), jnp.float32), pltpu.SemaphoreType.DMA((2,))] + zero_scratch,
            input_output_aliases={6: 1},
            cost_estimate=pl.CostEstimate(flops=30_000_000, bytes_accessed=40_000_000, transcendentals=0),
            compiler_params=pltpu.CompilerParams(vmem_limit_bytes=40 * 2**20),
            name="dw",
        )(c.reshape(1), du, *ns, de)

        xf = x.astype(jnp.float32)
        rs = lax.rsqrt(jnp.mean(xf * xf, axis=-1, keepdims=True) + EPS)
        nh = xf * rs
        gdn = gf * dn
        dxn = rs * (gdn - nh * jnp.mean(nh * gdn, axis=-1, keepdims=True))
        dx = (dres.astype(jnp.float32) + dxn).astype(jnp.bfloat16)
        dg = jnp.sum(dn * nh, axis=(0, 1))
        dxo = gather_all((dx[:mb // 2], dx[mb // 2:]))
        dxs = [b for j in range(8) for b in dxo[j]]
        for bit in (1, 2, 4):
            dg = dg + swap(dg, bit)

        de = pl.pallas_call(
            scatter_kernel,
            out_shape=de_shape,
            in_specs=[SMEM, SMEM, SMEM, VMEM] + [VMEM] * 16 + [ANY],
            out_specs=ANY,
            scratch_shapes=[
                pltpu.VMEM((mb, t, d), jnp.bfloat16),
                pltpu.VMEM((BLK, d), jnp.float32),
                pltpu.SemaphoreType.DMA,
            ],
            input_output_aliases={20: 0},
            compiler_params=pltpu.CompilerParams(vmem_limit_bytes=40 * 2**20),
            name="put_rows",
        )(me, rows, cnt, slot.reshape(1, n), *dxs, de)
        return u, x, de, dw, dg

    return jax.shard_map(
        local,
        mesh=mesh,
        in_specs=(P("dp", None), P("tp", None), P(None), P(None, "tp"), P("dp", None, "tp"), P("dp", "tp", None)),
        out_specs=(P("dp", None, "tp"), P("dp", "tp", None), P(("dp", "tp"), None), P(None, ("dp", "tp")), P("dp")),
        check_vma=False,
    )
```

```python
import functools

import jax
import jax.numpy as jnp
from jax import lax
from jax.experimental import pallas as pl
from jax.experimental.pallas import tpu as pltpu
from jax.sharding import PartitionSpec as P

EPS = 1e-6
ANY = pl.BlockSpec(memory_space=pl.ANY)
VMEM = pl.BlockSpec(memory_space=pltpu.VMEM)
SMEM = pl.BlockSpec(memory_space=pltpu.SMEM)
HBM = pl.BlockSpec(memory_space=pltpu.HBM)
ZR = 128
BLK = 256
LOOKUP_EARLY, LOOKUP_SHARE, NORM_SHARE = 8, 26, 6


def zero_fill(de, z, sem, first, last):

    def copy(i):
        return pltpu.make_async_copy(z, de.at[pl.ds(pl.multiple_of(i * ZR, ZR), ZR)], sem)

    def start(clear=True):
        if clear:
            z[...] = jnp.zeros_like(z)
        pl.loop(first, last)(lambda i: copy(i).start())

    def wait():
        pl.loop(first, last)(lambda i: copy(i).wait())

    return start, wait


def pdn_first_kernel(j, c_ref, du_hbm, w_hbm, h0, h1, du_ref, w_ref, sem, wsem):
    c = c_ref[0]
    mb, tc, _ = du_ref.shape
    tl = tc // 2
    wc = 512
    steps = w_hbm.shape[0] // wc
    z = pl.multiple_of(jnp.bitwise_xor(c, j) * tc, tc)
    rows_in = pltpu.make_async_copy(du_hbm.at[:, pl.ds(z, tc), :], du_ref, sem)
    rows_in.start()
    loads = [pltpu.make_async_copy(w_hbm.at[pl.ds(n * wc, wc)], w_ref.at[pl.ds(n * wc, wc)], wsem.at[n]) for n in range(steps)]
    for cp in loads:
        cp.start()
    rows_in.wait()
    rows = du_ref[...].reshape(mb * tc, du_ref.shape[2])
    for n in range(steps):
        loads[n].wait()
        cols = slice(n * wc, (n + 1) * wc)
        v = lax.dot_general(rows, w_ref[cols, :], (((1,), (1,)), ((), ())), preferred_element_type=jnp.float32)
        v = v.astype(jnp.bfloat16).reshape(mb, tc, wc)
        h0[:, :, cols] = v[:, :tl]
        h1[:, :, cols] = v[:, tl:]


def pdn_kernel(js, c_ref, du_ref, w_ref, *outs):
    c = c_ref[0]
    mb, t, _ = du_ref.shape
    tc, wc = t // 4, 512
    tl = tc // 2
    for i, j in enumerate(js):
        z = pl.multiple_of(jnp.bitwise_xor(c, j) * tc, tc)
        rows = jnp.concatenate([du_ref[m, pl.ds(z, tc), :] for m in range(mb)], axis=0)
        for n in range(w_ref.shape[0] // wc):
            cols = slice(n * wc, (n + 1) * wc)
            v = lax.dot_general(rows, w_ref[cols, :], (((1,), (1,)), ((), ())), preferred_element_type=jnp.float32)
            v = v.astype(jnp.bfloat16).reshape(mb, tc, wc)
            for h in range(2):
                outs[2 * i + h][:, :, cols] = v[:, h * tl:(h + 1) * tl]


def lookup_kernel(kc_ref, list_ref, cnt_ref, loc_ref, tgt_ref, emb, mine_ref, far_ref, near_ref, de, buf, sem, z, zsem):
    k, c = kc_ref[0], kc_ref[1]
    _, d = emb.shape
    nj, mb, tc, hd = mine_ref.shape
    n = nj * mb * tc
    step = 64
    start, wait = zero_fill(de, z, zsem, 0, LOOKUP_EARLY)
    late_start, late_wait = zero_fill(de, z, zsem, LOOKUP_EARLY, LOOKUP_SHARE)
    start()

    @pl.loop(0, 2 * n // step)
    def _(i):
        buf[pl.ds(pl.multiple_of(i * step, step), step), :] = jnp.zeros((step, d), buf.dtype)

    def copy(t, l):
        src = emb.at[pl.ds(pl.multiple_of((l >> 1) * 2, 2), 2)]
        return pltpu.make_async_copy(src, buf.at[pl.ds(pl.multiple_of(t * 2, 2), 2)], sem)

    cnt = cnt_ref[0]

    @pl.loop(0, cnt)
    def _(q):
        t = list_ref[q]
        copy(t, loc_ref[t]).start()

    @pl.loop(0, cnt)
    def _(i):
        copy(0, 0).wait()

    late_start(False)

    for j in range(nj):
        theirs = far_ref.at[0] if j == 3 else near_ref.at[j]
        zc = jnp.bitwise_xor(c, j)

        @pl.loop(0, mb)
        def _(m):
            t0 = m * (nj * tc) + zc * tc
            tgt = tgt_ref[pl.ds(pl.multiple_of(t0, tc), tc), :]
            sel = (lax.broadcasted_iota(jnp.int32, (tc, 2 * tc), 1) == tgt).astype(jnp.bfloat16)
            rows = pl.ds(pl.multiple_of(2 * t0, 2 * tc), 2 * tc)
            for out, half in ((theirs, 1 - k), (mine_ref.at[j], k)):
                v = buf[rows, pl.ds(pl.multiple_of(half * hd, 128), hd)]
                out[m] = jnp.dot(sel, v, preferred_element_type=jnp.float32).astype(jnp.bfloat16)

    wait()
    late_wait()


def norm_kernel(j, kc_ref, g_ref, w_ref, *refs):
    blocks, (nt_ref, u_ref, de, n_ref, stage, sem, z, zsem) = refs[:4], refs[-8:]
    k = kc_ref[0]
    d = nt_ref.shape[0]
    mb, tl, hd = blocks[0].shape
    tc = 2 * tl
    first = LOOKUP_SHARE + j * NORM_SHARE
    start, wait = zero_fill(de, z, zsem, first, first + NORM_SHARE)
    start()
    at = [pl.ds(pl.multiple_of(jnp.bitwise_xor(k, q) * hd, 128), hd) for q in range(2)]
    gf = [g_ref[:, at[q]].astype(jnp.float32) for q in range(2)]

    @pl.loop(0, mb)
    def _(m):
        for h in range(2):
            xf = [blocks[2 * h + q][m].astype(jnp.float32) for q in range(2)]
            total = sum(jnp.sum(v * v, axis=-1, keepdims=True) for v in xf)
            rs = lax.rsqrt(total * (1.0 / d) + EPS)
            for q in range(2):
                to = pl.ds(pl.multiple_of(m * tc + h * tl, tl), tl)
                n_ref[to, at[q]] = (xf[q] * rs * gf[q]).astype(jnp.bfloat16)

    v = jnp.dot(n_ref[...], w_ref[...], preferred_element_type=jnp.float32)
    stage[...] = v.astype(jnp.bfloat16).reshape(stage.shape)
    rows = pl.ds(pl.multiple_of(jnp.bitwise_xor(kc_ref[1], j) * tc, tc), tc)
    copy = pltpu.make_async_copy(stage, u_ref.at[:, rows, :], sem)
    copy.start()
    wc = 512

    @pl.loop(0, d // wc)
    def _(i):
        c = pl.ds(pl.multiple_of(i * wc, wc), wc)
        nt_ref[c, :] = n_ref[:, c].T

    copy.wait()
    wait()


def dw_kernel(c_ref, du_ref, *refs):
    ns, (dw, de, right, stage, sem, z, zsem) = refs[:4], refs[-7:]
    mb, _, _ = du_ref.shape
    d, kj = ns[0].shape
    tc = kj // mb
    start, wait = zero_fill(de, z, zsem, LOOKUP_SHARE + 4 * NORM_SHARE, de.shape[0] // ZR)
    start()
    for j in range(4):
        rows = pl.ds(pl.multiple_of(jnp.bitwise_xor(c_ref[0], j) * tc, tc), tc)
        for m in range(mb):
            right[j * kj + m * tc:j * kj + (m + 1) * tc, :] = du_ref[m, rows, :]
    dc = stage.shape[1]

    def copy(i, q):
        return pltpu.make_async_copy(stage.at[q], dw.at[pl.ds(pl.multiple_of(i * dc, dc), dc)], sem.at[q])

    @pl.loop(0, d // dc)
    def _(i):
        q = lax.rem(i, 2)

        @pl.when(i >= 2)
        def _():
            copy(i - 2, q).wait()

        c = pl.ds(pl.multiple_of(i * dc, dc), dc)
        left = jnp.concatenate([n[c, :] for n in ns], axis=1)
        stage[q] = jnp.dot(left, right[...], preferred_element_type=jnp.float32)
        copy(i, q).start()

    for q in range(2):
        copy(d // dc - 2 + q, q).wait()
    wait()


def scatter_kernel(me_ref, rows_ref, cnt_ref, slot_ref, *refs):
    blocks, (de, buf, stage, out_sem) = refs[:16], refs[-4:]
    mb, t, d = buf.shape
    hb, tl = blocks[0].shape[:2]
    for i, b in enumerate(blocks):
        at = pl.ds(pl.multiple_of(jnp.bitwise_xor(me_ref[0], i // 2) * tl, tl), tl)
        for m in range(hb):
            buf[(i % 2) * hb + m, at, :] = b[m]
    cnt = cnt_ref[0]
    cc = 512

    def copy(q, r):
        return pltpu.make_async_copy(stage.at[pl.ds(q, 1)], de.at[pl.ds(r, 1)], out_sem)

    @pl.loop(0, (cnt + BLK - 1) // BLK)
    def _(b):
        base = b * BLK
        ids = lax.broadcasted_iota(jnp.int32, (BLK, mb * t), 0) + base
        oh = (ids == slot_ref[...]).astype(jnp.bfloat16)
        for i in range(d // cc):
            acc = jnp.zeros((BLK, cc), jnp.float32)
            for m in range(mb):
                acc += jnp.dot(oh[:, m * t:(m + 1) * t], buf[m, :, i * cc:(i + 1) * cc], preferred_element_type=jnp.float32)
            stage[:, i * cc:(i + 1) * cc] = acc
        n = jnp.minimum(cnt - base, BLK)
        pl.loop(0, n)(lambda q: copy(q, rows_ref[base + q]).start())
        pl.loop(0, n)(lambda q: copy(q, rows_ref[base + q]).wait())


def solution(mesh):
    groups = mesh.shape["tp"]

    def swap(v, bit):
        return lax.ppermute(v, "tp", [(i, i ^ bit) for i in range(groups)])

    def local(ids, emb, g, w, du, dres):
        r = lax.axis_index("tp")
        mb, t = ids.shape
        vl, d = emb.shape
        f = w.shape[1]
        tl = t // groups
        hd = d // 2
        tc = t // 4
        k, c = r & 1, r >> 1
        gf = g.astype(jnp.float32)
        me = r.reshape(1)
        kc = jnp.stack([k, c]).astype(jnp.int32)
        de_shape = jax.ShapeDtypeStruct((vl, d), jnp.float32)
        zero_scratch = [pltpu.VMEM((ZR, d), jnp.float32), pltpu.SemaphoreType.DMA]

        def half_shape(nj):
            return jax.ShapeDtypeStruct((nj, mb, tc, hd), jnp.bfloat16)

        def pdn(js):
            out = pl.pallas_call(
                functools.partial(pdn_kernel, js),
                out_shape=(jax.ShapeDtypeStruct((mb, tl, d), jnp.bfloat16),) * (2 * len(js)),
                in_specs=[SMEM, VMEM, VMEM],
                out_specs=(VMEM,) * (2 * len(js)),
                cost_estimate=pl.CostEstimate(flops=5_000_000 * len(js), bytes_accessed=8_000_000, transcendentals=0),
                compiler_params=pltpu.CompilerParams(vmem_limit_bytes=40 * 2**20),
            )(c.reshape(1), du, w)
            return {j: out[2 * i:2 * i + 2] for i, j in enumerate(js)}

        def pick(a, b):
            return jnp.where(k == 0, a, b)

        def f32(v):
            return v.astype(jnp.float32)

        def reduce_to_home(pairs, dt):
            def part(j, h):
                a, b = pairs[j]
                return a[:, h * tl:(h + 1) * tl].astype(dt) + b[:, h * tl:(h + 1) * tl].astype(dt)

            dx_ = swap(part(3, 0), 2)
            dy_ = swap(part(3, 1), 4)
            ex = swap(part(1, 0), 2)
            ey = swap(part(2, 1), 4)
            pairs = dict(pairs)
            pairs[2], dx_ = lax.optimization_barrier((pairs[2], dx_))
            pairs[1], dy_ = lax.optimization_barrier((pairs[1], dy_))
            fy = swap(part(2, 0) + dx_, 4)
            fx = swap(part(1, 1) + dy_, 2)
            pairs[0], ex, ey = lax.optimization_barrier((pairs[0], ex, ey))
            return part(0, 0) + ex + fy, part(0, 1) + ey + fx

        def to_rows(mine, other):
            return jnp.where(k == 0, jnp.concatenate([mine, other], -1), jnp.concatenate([other, mine], -1))

        def gather_all(own):
            x1, y0 = swap(own[1], 2), swap(own[0], 4)
            x0, y1 = swap(own[0], 2), swap(own[1], 4)
            d1, d0 = swap(x1, 4), swap(y0, 2)
            out = {0: own, 2: (x0, x1), 4: (y0, y1), 6: (d0, d1)}
            for j in (0, 2, 4, 6):
                out[j + 1] = tuple(swap(b, 1) for b in out[j])
            return out

        flat = ids.reshape(-1)
        n = flat.shape[0]
        loc = flat - r * vl
        own = (loc >= 0) & (loc < vl)
        part = {3: pl.pallas_call(
            functools.partial(pdn_first_kernel, 3),
            out_shape=(jax.ShapeDtypeStruct((mb, tl, d), jnp.bfloat16),) * 2,
            in_specs=[SMEM, HBM, HBM],
            out_specs=(VMEM, VMEM),
            scratch_shapes=[
                pltpu.VMEM((mb, tc, f), jnp.bfloat16),
                pltpu.VMEM((d, f), jnp.bfloat16),
                pltpu.SemaphoreType.DMA,
                pltpu.SemaphoreType.DMA((6,)),
            ],
            cost_estimate=pl.CostEstimate(flops=5_000_000, bytes_accessed=8_000_000, transcendentals=0),
            compiler_params=pltpu.CompilerParams(vmem_limit_bytes=63 * 2**20),
            name="pa",
        )(c.reshape(1), du, w)}
        part.update(pdn((1, 2)))
        part.update(pdn((0,)))
        d0, d1 = swap(part[3][0], 2), swap(part[3][1], 4)
        ex, ey = swap(part[1][0], 2), swap(part[2][1], 4)
        tgt = jnp.where(own, 2 * (jnp.arange(n) % tc) + (loc & 1), -1).astype(jnp.int32)
        i0 = lax.broadcasted_iota(jnp.int32, (n, n), 0)
        i1 = lax.broadcasted_iota(jnp.int32, (n, n), 1)
        same = flat[:, None] == flat[None, :]
        first = jnp.min(jnp.where(same, i0, n), axis=0)
        lead = own & (first == jnp.arange(n))
        pos = jnp.sum(jnp.where(lead[:, None] & (i0 < i1), 1, 0), axis=0)
        pos_of_first = jnp.sum(jnp.where((i0 == first[None, :]), pos[:, None], 0), axis=0)
        slot = jnp.where(own, pos_of_first, -1).astype(jnp.int32)
        rows = jnp.sum(jnp.where(lead[:, None] & (pos[:, None] == i1), loc[:, None], 0), axis=0).astype(jnp.int32)
        cnt = jnp.sum(lead.astype(jnp.int32)).reshape(1)
        n_owned = jnp.sum(own.astype(jnp.int32)).reshape(1)
        own_pos = jnp.sum(jnp.where(own[:, None] & (i0 < i1), 1, 0), axis=0)
        owned = jnp.sum(jnp.where(own[:, None] & (own_pos[:, None] == i1), i0, 0), axis=0).astype(jnp.int32)
        d0, d1, loc, tgt, slot, rows, cnt, owned, n_owned = lax.optimization_barrier(
            (d0, d1, loc, tgt, slot, rows, cnt, owned, n_owned)
        )
        ty, tx = f32(part[2][0]) + f32(d0), f32(part[1][1]) + f32(d1)
        gy = swap(pick(ty[..., hd:], ty[..., :hd]), 1)
        gx = swap(pick(tx[..., hd:], tx[..., :hd]), 1)
        fy = swap(pick(ty[..., :hd], ty[..., hd:]) + gy, 4)
        fx = swap(pick(tx[..., :hd], tx[..., hd:]) + gx, 2)

        mine, far, near, de = pl.pallas_call(
            lookup_kernel,
            out_shape=(half_shape(4), half_shape(1), half_shape(3), de_shape),
            in_specs=[SMEM, SMEM, SMEM, SMEM, VMEM, ANY],
            out_specs=(VMEM, VMEM, VMEM, ANY),
            scratch_shapes=[pltpu.VMEM((2 * n, d), jnp.bfloat16), pltpu.SemaphoreType.DMA] + zero_scratch,
            cost_estimate=pl.CostEstimate(flops=40_000_000, bytes_accessed=60_000_000, transcendentals=0),
            compiler_params=pltpu.CompilerParams(vmem_limit_bytes=40 * 2**20),
            name="look",
        )(kc, owned, n_owned, loc, tgt.reshape(n, 1), emb)
        far, near = swap(far, 1), swap(near, 1)
        xpairs = {j: (mine[j], far[0] if j == 3 else near[j]) for j in range(4)}

        def widen(v):
            o = jnp.zeros_like(v)
            return to_rows(v, o)

        v0 = f32(part[0][0]) + f32(ex) + widen(fy)
        v1 = f32(part[0][1]) + f32(ey) + widen(fx)
        dn = pick(v0, v1) + swap(pick(v1, v0), 1)
        x0, x1 = reduce_to_home(xpairs, jnp.bfloat16)
        xo = gather_all((x0, x1))
        x = to_rows(jnp.where(k == 0, x0, x1), jnp.where(k == 0, xo[1][0], xo[1][1]))

        ns, u = [], None
        for j in range(4):
            more = (de,) if u is None else (u, de)
            nj, u, de = pl.pallas_call(
                functools.partial(norm_kernel, j),
                out_shape=(jax.ShapeDtypeStruct((d, mb * tc), jnp.bfloat16), jax.ShapeDtypeStruct((mb, t, f), jnp.bfloat16), de_shape),
                in_specs=[SMEM] + [VMEM] * 6 + [ANY] * len(more),
                out_specs=(VMEM, ANY, ANY),
                scratch_shapes=[
                    pltpu.VMEM((mb * tc, d), jnp.bfloat16),
                    pltpu.VMEM((mb, tc, f), jnp.bfloat16),
                    pltpu.SemaphoreType.DMA,
                ] + zero_scratch,
                input_output_aliases={7 + i: 3 - len(more) + i for i in range(len(more))},
                cost_estimate=pl.CostEstimate(flops=8_000_000, bytes_accessed=12_000_000, transcendentals=0),
                compiler_params=pltpu.CompilerParams(vmem_limit_bytes=40 * 2**20),
            )(kc, g.reshape(1, d), w, *(xo[2 * j + q][h] for h in range(2) for q in range(2)), *more)
            ns.append(nj)
        dw, de = pl.pallas_call(
            dw_kernel,
            out_shape=(jax.ShapeDtypeStruct((d, f), jnp.float32), de_shape),
            in_specs=[SMEM] + [VMEM] * 5 + [ANY],
            out_specs=(ANY, ANY),
            scratch_shapes=[
                pltpu.VMEM((n, f), jnp.bfloat16),
                pltpu.VMEM((2, 512, f), jnp.float32),
                pltpu.SemaphoreType.DMA((2,)),
            ] + zero_scratch,
            input_output_aliases={6: 1},
            cost_estimate=pl.CostEstimate(flops=30_000_000, bytes_accessed=40_000_000, transcendentals=0),
            compiler_params=pltpu.CompilerParams(vmem_limit_bytes=40 * 2**20),
            name="dw",
        )(c.reshape(1), du, *ns, de)

        xf = x.astype(jnp.float32)
        rs = lax.rsqrt(jnp.mean(xf * xf, axis=-1, keepdims=True) + EPS)
        nh = xf * rs
        gdn = gf * dn
        dxn = rs * (gdn - nh * jnp.mean(nh * gdn, axis=-1, keepdims=True))
        dx = (dres.astype(jnp.float32) + dxn).astype(jnp.bfloat16)
        dg = jnp.sum(dn * nh, axis=(0, 1))
        dxo = gather_all((dx[:mb // 2], dx[mb // 2:]))
        dxs = [b for j in range(8) for b in dxo[j]]
        for bit in (1, 2, 4):
            dg = dg + swap(dg, bit)

        de = pl.pallas_call(
            scatter_kernel,
            out_shape=de_shape,
            in_specs=[SMEM, SMEM, SMEM, VMEM] + [VMEM] * 16 + [ANY],
            out_specs=ANY,
            scratch_shapes=[
                pltpu.VMEM((mb, t, d), jnp.bfloat16),
                pltpu.VMEM((BLK, d), jnp.float32),
                pltpu.SemaphoreType.DMA,
            ],
            input_output_aliases={20: 0},
            compiler_params=pltpu.CompilerParams(vmem_limit_bytes=40 * 2**20),
            name="put",
        )(me, rows, cnt, slot.reshape(1, n), *dxs, de)
        return u, x, de, dw, dg

    return jax.shard_map(
        local,
        mesh=mesh,
        in_specs=(P("dp", None), P("tp", None), P(None), P(None, "tp"), P("dp", None, "tp"), P("dp", "tp", None)),
        out_specs=(P("dp", None, "tp"), P("dp", "tp", None), P(("dp", "tp"), None), P(None, ("dp", "tp")), P("dp")),
        check_vma=False,
    )
```

```python
import functools

import jax
import jax.numpy as jnp
from jax import lax
from jax.experimental import pallas as pl
from jax.experimental.pallas import tpu as pltpu
from jax.sharding import PartitionSpec as P

EPS = 1e-6
ANY = pl.BlockSpec(memory_space=pl.ANY)
VMEM = pl.BlockSpec(memory_space=pltpu.VMEM)
SMEM = pl.BlockSpec(memory_space=pltpu.SMEM)
HBM = pl.BlockSpec(memory_space=pltpu.HBM)
ZR = 128
BLK = 256
LOOKUP_EARLY, LOOKUP_SHARE, ZERO_A, ZERO_B, NORM_SHARE = 8, 22, 33, 48, 3


def zero_fill(de, z, sem, first, last):

    def copy(i):
        return pltpu.make_async_copy(z, de.at[pl.ds(pl.multiple_of(i * ZR, ZR), ZR)], sem)

    def start(clear=True):
        if clear:
            z[...] = jnp.zeros_like(z)
        pl.loop(first, last)(lambda i: copy(i).start())

    def wait():
        pl.loop(first, last)(lambda i: copy(i).wait())

    return start, wait


def zero_kernel(first, last, de_in, de, z, sem):
    del de_in
    start, wait = zero_fill(de, z, sem, first, last)
    start()
    wait()


def pdn_first_kernel(j, c_ref, du_hbm, w_hbm, h0, h1, du_ref, w_ref, sem, wsem):
    c = c_ref[0]
    mb, tc, _ = du_ref.shape
    tl = tc // 2
    wc = 512
    steps = w_hbm.shape[0] // wc
    z = pl.multiple_of(jnp.bitwise_xor(c, j) * tc, tc)
    rows_in = pltpu.make_async_copy(du_hbm.at[:, pl.ds(z, tc), :], du_ref, sem)
    rows_in.start()
    loads = [pltpu.make_async_copy(w_hbm.at[pl.ds(n * wc, wc)], w_ref.at[pl.ds(n * wc, wc)], wsem.at[n]) for n in range(steps)]
    for cp in loads:
        cp.start()
    rows_in.wait()
    rows = du_ref[...].reshape(mb * tc, du_ref.shape[2])
    for n in range(steps):
        loads[n].wait()
        cols = slice(n * wc, (n + 1) * wc)
        v = lax.dot_general(rows, w_ref[cols, :], (((1,), (1,)), ((), ())), preferred_element_type=jnp.float32)
        v = v.astype(jnp.bfloat16).reshape(mb, tc, wc)
        h0[:, :, cols] = v[:, :tl]
        h1[:, :, cols] = v[:, tl:]


def pdn_kernel(js, c_ref, du_ref, w_ref, *outs):
    c = c_ref[0]
    mb, t, _ = du_ref.shape
    tc, wc = t // 4, 512
    tl = tc // 2
    for i, j in enumerate(js):
        z = pl.multiple_of(jnp.bitwise_xor(c, j) * tc, tc)
        rows = jnp.concatenate([du_ref[m, pl.ds(z, tc), :] for m in range(mb)], axis=0)
        for n in range(w_ref.shape[0] // wc):
            cols = slice(n * wc, (n + 1) * wc)
            v = lax.dot_general(rows, w_ref[cols, :], (((1,), (1,)), ((), ())), preferred_element_type=jnp.float32)
            v = v.astype(jnp.bfloat16).reshape(mb, tc, wc)
            for h in range(2):
                outs[2 * i + h][:, :, cols] = v[:, h * tl:(h + 1) * tl]


def lookup_kernel(kc_ref, list_ref, cnt_ref, loc_ref, tgt_ref, emb, mine_ref, far_ref, near_ref, de, buf, sem, z, zsem):
    k, c = kc_ref[0], kc_ref[1]
    _, d = emb.shape
    nj, mb, tc, hd = mine_ref.shape
    n = nj * mb * tc
    step = 64
    start, wait = zero_fill(de, z, zsem, 0, LOOKUP_EARLY)
    late_start, late_wait = zero_fill(de, z, zsem, LOOKUP_EARLY, LOOKUP_SHARE)
    start()

    @pl.loop(0, 2 * n // step)
    def _(i):
        buf[pl.ds(pl.multiple_of(i * step, step), step), :] = jnp.zeros((step, d), buf.dtype)

    def copy(t, l):
        src = emb.at[pl.ds(pl.multiple_of((l >> 1) * 2, 2), 2)]
        return pltpu.make_async_copy(src, buf.at[pl.ds(pl.multiple_of(t * 2, 2), 2)], sem)

    cnt = cnt_ref[0]

    @pl.loop(0, cnt)
    def _(q):
        t = list_ref[q]
        copy(t, loc_ref[t]).start()

    @pl.loop(0, cnt)
    def _(i):
        copy(0, 0).wait()

    late_start(False)

    for j in range(nj):
        theirs = far_ref.at[0] if j == 3 else near_ref.at[j]
        zc = jnp.bitwise_xor(c, j)

        @pl.loop(0, mb)
        def _(m):
            t0 = m * (nj * tc) + zc * tc
            tgt = tgt_ref[pl.ds(pl.multiple_of(t0, tc), tc), :]
            sel = (lax.broadcasted_iota(jnp.int32, (tc, 2 * tc), 1) == tgt).astype(jnp.bfloat16)
            rows = pl.ds(pl.multiple_of(2 * t0, 2 * tc), 2 * tc)
            for out, half in ((theirs, 1 - k), (mine_ref.at[j], k)):
                v = buf[rows, pl.ds(pl.multiple_of(half * hd, 128), hd)]
                out[m] = jnp.dot(sel, v, preferred_element_type=jnp.float32).astype(jnp.bfloat16)

    wait()
    late_wait()


def norm_kernel(j, kc_ref, g_ref, w_ref, *refs):
    blocks, (nt_ref, u_ref, de, n_ref, stage, sem, z, zsem) = refs[:4], refs[-8:]
    k = kc_ref[0]
    d = nt_ref.shape[0]
    mb, tl, hd = blocks[0].shape
    tc = 2 * tl
    first = ZERO_B + j * NORM_SHARE
    start, wait = zero_fill(de, z, zsem, first, first + NORM_SHARE)
    start()
    at = [pl.ds(pl.multiple_of(jnp.bitwise_xor(k, q) * hd, 128), hd) for q in range(2)]
    gf = [g_ref[:, at[q]].astype(jnp.float32) for q in range(2)]

    @pl.loop(0, mb)
    def _(m):
        for h in range(2):
            xf = [blocks[2 * h + q][m].astype(jnp.float32) for q in range(2)]
            total = sum(jnp.sum(v * v, axis=-1, keepdims=True) for v in xf)
            rs = lax.rsqrt(total * (1.0 / d) + EPS)
            for q in range(2):
                to = pl.ds(pl.multiple_of(m * tc + h * tl, tl), tl)
                n_ref[to, at[q]] = (xf[q] * rs * gf[q]).astype(jnp.bfloat16)

    v = jnp.dot(n_ref[...], w_ref[...], preferred_element_type=jnp.float32)
    stage[...] = v.astype(jnp.bfloat16).reshape(stage.shape)
    rows = pl.ds(pl.multiple_of(jnp.bitwise_xor(kc_ref[1], j) * tc, tc), tc)
    copy = pltpu.make_async_copy(stage, u_ref.at[:, rows, :], sem)
    copy.start()
    wc = 512

    @pl.loop(0, d // wc)
    def _(i):
        c = pl.ds(pl.multiple_of(i * wc, wc), wc)
        nt_ref[c, :] = n_ref[:, c].T

    copy.wait()
    wait()


def dw_kernel(c_ref, du_ref, *refs):
    ns, (dw, de, right, stage, sem, z, zsem) = refs[:4], refs[-7:]
    mb, _, _ = du_ref.shape
    d, kj = ns[0].shape
    tc = kj // mb
    start, wait = zero_fill(de, z, zsem, ZERO_B + 4 * NORM_SHARE, de.shape[0] // ZR)
    start()
    for j in range(4):
        rows = pl.ds(pl.multiple_of(jnp.bitwise_xor(c_ref[0], j) * tc, tc), tc)
        for m in range(mb):
            right[j * kj + m * tc:j * kj + (m + 1) * tc, :] = du_ref[m, rows, :]
    dc = stage.shape[1]

    def copy(i, q):
        return pltpu.make_async_copy(stage.at[q], dw.at[pl.ds(pl.multiple_of(i * dc, dc), dc)], sem.at[q])

    @pl.loop(0, d // dc)
    def _(i):
        q = lax.rem(i, 2)

        @pl.when(i >= 2)
        def _():
            copy(i - 2, q).wait()

        c = pl.ds(pl.multiple_of(i * dc, dc), dc)
        left = jnp.concatenate([n[c, :] for n in ns], axis=1)
        stage[q] = jnp.dot(left, right[...], preferred_element_type=jnp.float32)
        copy(i, q).start()

    for q in range(2):
        copy(d // dc - 2 + q, q).wait()
    wait()


def scatter_kernel(me_ref, rows_ref, cnt_ref, slot_ref, *refs):
    blocks, (de, buf, stage, out_sem) = refs[:16], refs[-4:]
    mb, t, d = buf.shape
    hb, tl = blocks[0].shape[:2]
    for i, b in enumerate(blocks):
        at = pl.ds(pl.multiple_of(jnp.bitwise_xor(me_ref[0], i // 2) * tl, tl), tl)
        for m in range(hb):
            buf[(i % 2) * hb + m, at, :] = b[m]
    cnt = cnt_ref[0]
    cc = 512

    def copy(q, r):
        return pltpu.make_async_copy(stage.at[pl.ds(q, 1)], de.at[pl.ds(r, 1)], out_sem)

    @pl.loop(0, (cnt + BLK - 1) // BLK)
    def _(b):
        base = b * BLK
        ids = lax.broadcasted_iota(jnp.int32, (BLK, mb * t), 0) + base
        oh = (ids == slot_ref[...]).astype(jnp.bfloat16)
        for i in range(d // cc):
            acc = jnp.zeros((BLK, cc), jnp.float32)
            for m in range(mb):
                acc += jnp.dot(oh[:, m * t:(m + 1) * t], buf[m, :, i * cc:(i + 1) * cc], preferred_element_type=jnp.float32)
            stage[:, i * cc:(i + 1) * cc] = acc
        n = jnp.minimum(cnt - base, BLK)
        pl.loop(0, n)(lambda q: copy(q, rows_ref[base + q]).start())
        pl.loop(0, n)(lambda q: copy(q, rows_ref[base + q]).wait())


def solution(mesh):
    groups = mesh.shape["tp"]

    def swap(v, bit):
        return lax.ppermute(v, "tp", [(i, i ^ bit) for i in range(groups)])

    def local(ids, emb, g, w, du, dres):
        r = lax.axis_index("tp")
        mb, t = ids.shape
        vl, d = emb.shape
        f = w.shape[1]
        tl = t // groups
        hd = d // 2
        tc = t // 4
        k, c = r & 1, r >> 1
        gf = g.astype(jnp.float32)
        me = r.reshape(1)
        kc = jnp.stack([k, c]).astype(jnp.int32)
        de_shape = jax.ShapeDtypeStruct((vl, d), jnp.float32)
        zero_scratch = [pltpu.VMEM((ZR, d), jnp.float32), pltpu.SemaphoreType.DMA]

        def half_shape(nj):
            return jax.ShapeDtypeStruct((nj, mb, tc, hd), jnp.bfloat16)

        def pdn(js):
            out = pl.pallas_call(
                functools.partial(pdn_kernel, js),
                out_shape=(jax.ShapeDtypeStruct((mb, tl, d), jnp.bfloat16),) * (2 * len(js)),
                in_specs=[SMEM, VMEM, VMEM],
                out_specs=(VMEM,) * (2 * len(js)),
                cost_estimate=pl.CostEstimate(flops=5_000_000 * len(js), bytes_accessed=8_000_000, transcendentals=0),
                compiler_params=pltpu.CompilerParams(vmem_limit_bytes=20 * 2**20),
            )(c.reshape(1), du, w)
            return {j: out[2 * i:2 * i + 2] for i, j in enumerate(js)}

        def pick(a, b):
            return jnp.where(k == 0, a, b)

        def f32(v):
            return v.astype(jnp.float32)

        def reduce_to_home(pairs, dt):
            def part(j, h):
                a, b = pairs[j]
                return a[:, h * tl:(h + 1) * tl].astype(dt) + b[:, h * tl:(h + 1) * tl].astype(dt)

            dx_ = swap(part(3, 0), 2)
            dy_ = swap(part(3, 1), 4)
            ex = swap(part(1, 0), 2)
            ey = swap(part(2, 1), 4)
            pairs = dict(pairs)
            pairs[2], dx_ = lax.optimization_barrier((pairs[2], dx_))
            pairs[1], dy_ = lax.optimization_barrier((pairs[1], dy_))
            fy = swap(part(2, 0) + dx_, 4)
            fx = swap(part(1, 1) + dy_, 2)
            pairs[0], ex, ey = lax.optimization_barrier((pairs[0], ex, ey))
            return part(0, 0) + ex + fy, part(0, 1) + ey + fx

        def to_rows(mine, other):
            return jnp.where(k == 0, jnp.concatenate([mine, other], -1), jnp.concatenate([other, mine], -1))

        def gather_all(own):
            x1, y0 = swap(own[1], 2), swap(own[0], 4)
            x0, y1 = swap(own[0], 2), swap(own[1], 4)
            d1, d0 = swap(x1, 4), swap(y0, 2)
            out = {0: own, 2: (x0, x1), 4: (y0, y1), 6: (d0, d1)}
            for j in (0, 2, 4, 6):
                out[j + 1] = tuple(swap(b, 1) for b in out[j])
            return out

        flat = ids.reshape(-1)
        n = flat.shape[0]
        loc = flat - r * vl
        own = (loc >= 0) & (loc < vl)
        part = {3: pl.pallas_call(
            functools.partial(pdn_first_kernel, 3),
            out_shape=(jax.ShapeDtypeStruct((mb, tl, d), jnp.bfloat16),) * 2,
            in_specs=[SMEM, HBM, HBM],
            out_specs=(VMEM, VMEM),
            scratch_shapes=[
                pltpu.VMEM((mb, tc, f), jnp.bfloat16),
                pltpu.VMEM((d, f), jnp.bfloat16),
                pltpu.SemaphoreType.DMA,
                pltpu.SemaphoreType.DMA((6,)),
            ],
            cost_estimate=pl.CostEstimate(flops=5_000_000, bytes_accessed=8_000_000, transcendentals=0),
            compiler_params=pltpu.CompilerParams(vmem_limit_bytes=60 * 2**20),
            name="pa",
        )(c.reshape(1), du, w)}
        part.update(pdn((1, 2)))
        part.update(pdn((0,)))
        d0, d1 = swap(part[3][0], 2), swap(part[3][1], 4)
        ex, ey = swap(part[1][0], 2), swap(part[2][1], 4)
        tgt = jnp.where(own, 2 * (jnp.arange(n) % tc) + (loc & 1), -1).astype(jnp.int32)
        i0 = lax.broadcasted_iota(jnp.int32, (n, n), 0)
        i1 = lax.broadcasted_iota(jnp.int32, (n, n), 1)
        same = flat[:, None] == flat[None, :]
        first = jnp.min(jnp.where(same, i0, n), axis=0)
        lead = own & (first == jnp.arange(n))
        pos = jnp.sum(jnp.where(lead[:, None] & (i0 < i1), 1, 0), axis=0)
        pos_of_first = jnp.sum(jnp.where((i0 == first[None, :]), pos[:, None], 0), axis=0)
        slot = jnp.where(own, pos_of_first, -1).astype(jnp.int32)
        rows = jnp.sum(jnp.where(lead[:, None] & (pos[:, None] == i1), loc[:, None], 0), axis=0).astype(jnp.int32)
        cnt = jnp.sum(lead.astype(jnp.int32)).reshape(1)
        n_owned = jnp.sum(own.astype(jnp.int32)).reshape(1)
        own_pos = jnp.sum(jnp.where(own[:, None] & (i0 < i1), 1, 0), axis=0)
        owned = jnp.sum(jnp.where(own[:, None] & (own_pos[:, None] == i1), i0, 0), axis=0).astype(jnp.int32)
        d0, d1, loc, tgt, slot, rows, cnt, owned, n_owned = lax.optimization_barrier(
            (d0, d1, loc, tgt, slot, rows, cnt, owned, n_owned)
        )
        ty, tx = f32(part[2][0]) + f32(d0), f32(part[1][1]) + f32(d1)
        gy = swap(pick(ty[..., hd:], ty[..., :hd]), 1)
        gx = swap(pick(tx[..., hd:], tx[..., :hd]), 1)
        fy = swap(pick(ty[..., :hd], ty[..., hd:]) + gy, 4)
        fx = swap(pick(tx[..., :hd], tx[..., hd:]) + gx, 2)

        mine, far, near, de = pl.pallas_call(
            lookup_kernel,
            out_shape=(half_shape(4), half_shape(1), half_shape(3), de_shape),
            in_specs=[SMEM, SMEM, SMEM, SMEM, VMEM, ANY],
            out_specs=(VMEM, VMEM, VMEM, ANY),
            scratch_shapes=[pltpu.VMEM((2 * n, d), jnp.bfloat16), pltpu.SemaphoreType.DMA] + zero_scratch,
            cost_estimate=pl.CostEstimate(flops=40_000_000, bytes_accessed=60_000_000, transcendentals=0),
            compiler_params=pltpu.CompilerParams(vmem_limit_bytes=32 * 2**20),
            name="look",
        )(kc, owned, n_owned, loc, tgt.reshape(n, 1), emb)
        for first, last in ((LOOKUP_SHARE, ZERO_A), (ZERO_A, ZERO_B)):
            de = pl.pallas_call(
                functools.partial(zero_kernel, first, last),
                out_shape=de_shape,
                in_specs=[ANY],
                out_specs=ANY,
                scratch_shapes=zero_scratch,
                input_output_aliases={0: 0},
                cost_estimate=pl.CostEstimate(flops=10_000_000, bytes_accessed=20_000_000, transcendentals=0),
                compiler_params=pltpu.CompilerParams(vmem_limit_bytes=4 * 2**20),
            )(de)
        far, near = swap(far, 1), swap(near, 1)
        xpairs = {j: (mine[j], far[0] if j == 3 else near[j]) for j in range(4)}

        def widen(v):
            o = jnp.zeros_like(v)
            return to_rows(v, o)

        v0 = f32(part[0][0]) + f32(ex) + widen(fy)
        v1 = f32(part[0][1]) + f32(ey) + widen(fx)
        dn = pick(v0, v1) + swap(pick(v1, v0), 1)
        x0, x1 = reduce_to_home(xpairs, jnp.bfloat16)
        xo = gather_all((x0, x1))
        x = to_rows(jnp.where(k == 0, x0, x1), jnp.where(k == 0, xo[1][0], xo[1][1]))

        ns, u = [], None
        for j in range(4):
            more = (de,) if u is None else (u, de)
            nj, u, de = pl.pallas_call(
                functools.partial(norm_kernel, j),
                out_shape=(jax.ShapeDtypeStruct((d, mb * tc), jnp.bfloat16), jax.ShapeDtypeStruct((mb, t, f), jnp.bfloat16), de_shape),
                in_specs=[SMEM] + [VMEM] * 6 + [ANY] * len(more),
                out_specs=(VMEM, ANY, ANY),
                scratch_shapes=[
                    pltpu.VMEM((mb * tc, d), jnp.bfloat16),
                    pltpu.VMEM((mb, tc, f), jnp.bfloat16),
                    pltpu.SemaphoreType.DMA,
                ] + zero_scratch,
                input_output_aliases={7 + i: 3 - len(more) + i for i in range(len(more))},
                cost_estimate=pl.CostEstimate(flops=8_000_000, bytes_accessed=12_000_000, transcendentals=0),
                compiler_params=pltpu.CompilerParams(vmem_limit_bytes=24 * 2**20),
            )(kc, g.reshape(1, d), w, *(xo[2 * j + q][h] for h in range(2) for q in range(2)), *more)
            ns.append(nj)
        dw, de = pl.pallas_call(
            dw_kernel,
            out_shape=(jax.ShapeDtypeStruct((d, f), jnp.float32), de_shape),
            in_specs=[SMEM] + [VMEM] * 5 + [ANY],
            out_specs=(ANY, ANY),
            scratch_shapes=[
                pltpu.VMEM((n, f), jnp.bfloat16),
                pltpu.VMEM((2, 512, f), jnp.float32),
                pltpu.SemaphoreType.DMA((2,)),
            ] + zero_scratch,
            input_output_aliases={6: 1},
            cost_estimate=pl.CostEstimate(flops=30_000_000, bytes_accessed=40_000_000, transcendentals=0),
            compiler_params=pltpu.CompilerParams(vmem_limit_bytes=24 * 2**20),
            name="dw",
        )(c.reshape(1), du, *ns, de)

        xf = x.astype(jnp.float32)
        rs = lax.rsqrt(jnp.mean(xf * xf, axis=-1, keepdims=True) + EPS)
        nh = xf * rs
        gdn = gf * dn
        dxn = rs * (gdn - nh * jnp.mean(nh * gdn, axis=-1, keepdims=True))
        dx = (dres.astype(jnp.float32) + dxn).astype(jnp.bfloat16)
        dg = jnp.sum(dn * nh, axis=(0, 1))
        dxo = gather_all((dx[:mb // 2], dx[mb // 2:]))
        dxs = [b for j in range(8) for b in dxo[j]]
        for bit in (1, 2, 4):
            dg = dg + swap(dg, bit)

        de = pl.pallas_call(
            scatter_kernel,
            out_shape=de_shape,
            in_specs=[SMEM, SMEM, SMEM, VMEM] + [VMEM] * 16 + [ANY],
            out_specs=ANY,
            scratch_shapes=[
                pltpu.VMEM((mb, t, d), jnp.bfloat16),
                pltpu.VMEM((BLK, d), jnp.float32),
                pltpu.SemaphoreType.DMA,
            ],
            input_output_aliases={20: 0},
            compiler_params=pltpu.CompilerParams(vmem_limit_bytes=28 * 2**20),
            name="put",
        )(me, rows, cnt, slot.reshape(1, n), *dxs, de)
        return u, x, de, dw, dg

    return jax.shard_map(
        local,
        mesh=mesh,
        in_specs=(P("dp", None), P("tp", None), P(None), P(None, "tp"), P("dp", None, "tp"), P("dp", "tp", None)),
        out_specs=(P("dp", None, "tp"), P("dp", "tp", None), P(("dp", "tp"), None), P(None, ("dp", "tp")), P("dp")),
        check_vma=False,
    )
```

```python
import functools

import jax
import jax.numpy as jnp
from jax import lax
from jax.experimental import pallas as pl
from jax.experimental.pallas import tpu as pltpu
from jax.sharding import PartitionSpec as P

EPS = 1e-6
ANY = pl.BlockSpec(memory_space=pl.ANY)
VMEM = pl.BlockSpec(memory_space=pltpu.VMEM)
SMEM = pl.BlockSpec(memory_space=pltpu.SMEM)
HBM = pl.BlockSpec(memory_space=pltpu.HBM)
ZR = 128
CUT = 3
BLK = 256
LOOKUP_EARLY, LOOKUP_SHARE, ZERO_A, ZERO_B, NORM_SHARE = 8, 22, 34, 52, 3


def zero_fill(de, z, sem, first, last):

    def copy(i):
        return pltpu.make_async_copy(z, de.at[pl.ds(pl.multiple_of(i * ZR, ZR), ZR)], sem)

    def start(clear=True):
        if clear:
            z[...] = jnp.zeros_like(z)
        pl.loop(first, last)(lambda i: copy(i).start())

    def wait():
        pl.loop(first, last)(lambda i: copy(i).wait())

    return start, wait


def zero_kernel(first, last, de_in, de, z, sem):
    del de_in
    start, wait = zero_fill(de, z, sem, first, last)
    start()
    wait()


def pdn_first_kernel(j, col0, c_ref, du_hbm, w_hbm, h0, h1, du_ref, w_ref, sem, wsem):
    c = c_ref[0]
    mb, tc, _ = du_ref.shape
    tl = tc // 2
    wc = 512
    steps = w_ref.shape[0] // wc
    z = pl.multiple_of(jnp.bitwise_xor(c, j) * tc, tc)
    rows_in = pltpu.make_async_copy(du_hbm.at[:, pl.ds(z, tc), :], du_ref, sem)
    rows_in.start()
    loads = [
        pltpu.make_async_copy(w_hbm.at[pl.ds(col0 + n * wc, wc)], w_ref.at[pl.ds(n * wc, wc)], wsem.at[n]) for n in range(steps)
    ]
    for cp in loads:
        cp.start()
    rows_in.wait()
    rows = du_ref[...].reshape(mb * tc, du_ref.shape[2])
    for n in range(steps):
        loads[n].wait()
        cols = slice(n * wc, (n + 1) * wc)
        v = lax.dot_general(rows, w_ref[cols, :], (((1,), (1,)), ((), ())), preferred_element_type=jnp.float32)
        v = v.astype(jnp.bfloat16).reshape(mb, tc, wc)
        h0[:, :, cols] = v[:, :tl]
        h1[:, :, cols] = v[:, tl:]


def pdn_kernel(js, c_ref, du_ref, w_ref, *outs):
    c = c_ref[0]
    mb, t, _ = du_ref.shape
    tc, wc = t // 4, 512
    tl = tc // 2
    for i, j in enumerate(js):
        z = pl.multiple_of(jnp.bitwise_xor(c, j) * tc, tc)
        rows = jnp.concatenate([du_ref[m, pl.ds(z, tc), :] for m in range(mb)], axis=0)
        for n in range(w_ref.shape[0] // wc):
            cols = slice(n * wc, (n + 1) * wc)
            v = lax.dot_general(rows, w_ref[cols, :], (((1,), (1,)), ((), ())), preferred_element_type=jnp.float32)
            v = v.astype(jnp.bfloat16).reshape(mb, tc, wc)
            for h in range(2):
                outs[2 * i + h][:, :, cols] = v[:, h * tl:(h + 1) * tl]


def lookup_kernel(kc_ref, list_ref, cnt_ref, loc_ref, tgt_ref, emb, mine_ref, far_ref, near_ref, de, buf, sem, z, zsem):
    k, c = kc_ref[0], kc_ref[1]
    _, d = emb.shape
    nj, mb, tc, hd = mine_ref.shape
    n = nj * mb * tc
    step = 64
    start, wait = zero_fill(de, z, zsem, 0, LOOKUP_EARLY)
    late_start, late_wait = zero_fill(de, z, zsem, LOOKUP_EARLY, LOOKUP_SHARE)
    start()

    @pl.loop(0, 2 * n // step)
    def _(i):
        buf[pl.ds(pl.multiple_of(i * step, step), step), :] = jnp.zeros((step, d), buf.dtype)

    def copy(t, l):
        src = emb.at[pl.ds(pl.multiple_of((l >> 1) * 2, 2), 2)]
        return pltpu.make_async_copy(src, buf.at[pl.ds(pl.multiple_of(t * 2, 2), 2)], sem)

    cnt = cnt_ref[0]

    @pl.loop(0, cnt)
    def _(q):
        t = list_ref[q]
        copy(t, loc_ref[t]).start()

    @pl.loop(0, cnt)
    def _(i):
        copy(0, 0).wait()

    late_start(False)

    for j in range(nj):
        theirs = far_ref.at[0] if j == 3 else near_ref.at[j]
        zc = jnp.bitwise_xor(c, j)

        @pl.loop(0, mb)
        def _(m):
            t0 = m * (nj * tc) + zc * tc
            tgt = tgt_ref[pl.ds(pl.multiple_of(t0, tc), tc), :]
            sel = (lax.broadcasted_iota(jnp.int32, (tc, 2 * tc), 1) == tgt).astype(jnp.bfloat16)
            rows = pl.ds(pl.multiple_of(2 * t0, 2 * tc), 2 * tc)
            for out, half in ((theirs, 1 - k), (mine_ref.at[j], k)):
                v = buf[rows, pl.ds(pl.multiple_of(half * hd, 128), hd)]
                out[m] = jnp.dot(sel, v, preferred_element_type=jnp.float32).astype(jnp.bfloat16)

    wait()
    late_wait()


def norm_kernel(j, kc_ref, g_ref, w_ref, *refs):
    blocks, (nt_ref, u_ref, de, n_ref, stage, sem, z, zsem) = refs[:4], refs[-8:]
    k = kc_ref[0]
    d = nt_ref.shape[0]
    mb, tl, hd = blocks[0].shape
    tc = 2 * tl
    first = ZERO_B + j * NORM_SHARE
    start, wait = zero_fill(de, z, zsem, first, first + NORM_SHARE)
    start()
    at = [pl.ds(pl.multiple_of(jnp.bitwise_xor(k, q) * hd, 128), hd) for q in range(2)]
    gf = [g_ref[:, at[q]].astype(jnp.float32) for q in range(2)]

    @pl.loop(0, mb)
    def _(m):
        for h in range(2):
            xf = [blocks[2 * h + q][m].astype(jnp.float32) for q in range(2)]
            total = sum(jnp.sum(v * v, axis=-1, keepdims=True) for v in xf)
            rs = lax.rsqrt(total * (1.0 / d) + EPS)
            for q in range(2):
                to = pl.ds(pl.multiple_of(m * tc + h * tl, tl), tl)
                n_ref[to, at[q]] = (xf[q] * rs * gf[q]).astype(jnp.bfloat16)

    v = jnp.dot(n_ref[...], w_ref[...], preferred_element_type=jnp.float32)
    stage[...] = v.astype(jnp.bfloat16).reshape(stage.shape)
    rows = pl.ds(pl.multiple_of(jnp.bitwise_xor(kc_ref[1], j) * tc, tc), tc)
    copy = pltpu.make_async_copy(stage, u_ref.at[:, rows, :], sem)
    copy.start()
    wc = 512

    @pl.loop(0, d // wc)
    def _(i):
        c = pl.ds(pl.multiple_of(i * wc, wc), wc)
        nt_ref[c, :] = n_ref[:, c].T

    copy.wait()
    wait()


def dw_kernel(c_ref, du_ref, *refs):
    ns, (dw, right, stage, sem) = refs[:4], refs[-4:]
    mb, _, _ = du_ref.shape
    d, kj = ns[0].shape
    tc = kj // mb
    for j in range(4):
        rows = pl.ds(pl.multiple_of(jnp.bitwise_xor(c_ref[0], j) * tc, tc), tc)
        for m in range(mb):
            right[j * kj + m * tc:j * kj + (m + 1) * tc, :] = du_ref[m, rows, :]
    dc = stage.shape[1]

    def copy(i, q):
        return pltpu.make_async_copy(stage.at[q], dw.at[pl.ds(pl.multiple_of(i * dc, dc), dc)], sem.at[q])

    @pl.loop(0, d // dc)
    def _(i):
        q = lax.rem(i, 2)

        @pl.when(i >= 2)
        def _():
            copy(i - 2, q).wait()

        c = pl.ds(pl.multiple_of(i * dc, dc), dc)
        left = jnp.concatenate([n[c, :] for n in ns], axis=1)
        stage[q] = jnp.dot(left, right[...], preferred_element_type=jnp.float32)
        copy(i, q).start()

    for q in range(2):
        copy(d // dc - 2 + q, q).wait()


def scatter_kernel(rows_ref, cnt_ref, slot_ref, *refs):
    blocks, (de, stage, out_sem) = refs[:16], refs[-3:]
    hb, tl, d = blocks[0].shape
    kb = hb * tl
    cnt = cnt_ref[0]
    cc = 512

    def copy(q, r, size=1):
        return pltpu.make_async_copy(stage.at[pl.ds(q, size)], de.at[pl.ds(r, size)], out_sem)

    @pl.loop(0, (cnt + BLK - 1) // BLK)
    def _(b):
        base = b * BLK
        ids = lax.broadcasted_iota(jnp.int32, (BLK, len(blocks) * kb), 0) + base
        oh = (ids == slot_ref[...]).astype(jnp.bfloat16)
        for i in range(d // cc):
            cols = slice(i * cc, (i + 1) * cc)
            right = jnp.concatenate([v[:, :, cols].reshape(kb, cc) for v in blocks], axis=0)
            stage[:, cols] = jnp.dot(oh, right, preferred_element_type=jnp.float32)
        n = jnp.minimum(cnt - base, BLK)
        full = n // 8

        @pl.loop(0, full)
        def _(i):
            for u in range(8):
                copy(i * 8 + u, rows_ref[base + i * 8 + u]).start()

        pl.loop(full * 8, n)(lambda q: copy(q, rows_ref[base + q]).start())
        for bit in range(9):

            @pl.when((n >> bit) & 1 == 1)
            def _():
                copy(0, 0, 1 << bit).wait()


def solution(mesh):
    groups = mesh.shape["tp"]

    def swap(v, bit):
        return lax.ppermute(v, "tp", [(i, i ^ bit) for i in range(groups)])

    def local(ids, emb, g, w, du, dres):
        r = lax.axis_index("tp")
        mb, t = ids.shape
        vl, d = emb.shape
        f = w.shape[1]
        tl = t // groups
        hd = d // 2
        tc = t // 4
        k, c = r & 1, r >> 1
        gf = g.astype(jnp.float32)
        kc = jnp.stack([k, c]).astype(jnp.int32)
        de_shape = jax.ShapeDtypeStruct((vl, d), jnp.float32)
        zero_scratch = [pltpu.VMEM((ZR, d), jnp.float32), pltpu.SemaphoreType.DMA]

        def half_shape(nj):
            return jax.ShapeDtypeStruct((nj, mb, tc, hd), jnp.bfloat16)

        def pdn(js):
            out = pl.pallas_call(
                functools.partial(pdn_kernel, js),
                out_shape=(jax.ShapeDtypeStruct((mb, tl, d), jnp.bfloat16),) * (2 * len(js)),
                in_specs=[SMEM, VMEM, VMEM],
                out_specs=(VMEM,) * (2 * len(js)),
                cost_estimate=pl.CostEstimate(flops=5_000_000 * len(js), bytes_accessed=8_000_000, transcendentals=0),
                compiler_params=pltpu.CompilerParams(vmem_limit_bytes=20 * 2**20),
            )(c.reshape(1), du, w)
            return {j: out[2 * i:2 * i + 2] for i, j in enumerate(js)}

        def pick(a, b):
            return jnp.where(k == 0, a, b)

        def f32(v):
            return v.astype(jnp.float32)

        def reduce_to_home(pairs, dt):
            def part(j, h):
                a, b = pairs[j]
                return a[:, h * tl:(h + 1) * tl].astype(dt) + b[:, h * tl:(h + 1) * tl].astype(dt)

            dx_ = swap(part(3, 0), 2)
            dy_ = swap(part(3, 1), 4)
            ex = swap(part(1, 0), 2)
            ey = swap(part(2, 1), 4)
            pairs = dict(pairs)
            pairs[2], dx_ = lax.optimization_barrier((pairs[2], dx_))
            pairs[1], dy_ = lax.optimization_barrier((pairs[1], dy_))
            fy = swap(part(2, 0) + dx_, 4)
            fx = swap(part(1, 1) + dy_, 2)
            pairs[0], ex, ey = lax.optimization_barrier((pairs[0], ex, ey))
            return part(0, 0) + ex + fy, part(0, 1) + ey + fx

        def to_rows(mine, other):
            return jnp.where(k == 0, jnp.concatenate([mine, other], -1), jnp.concatenate([other, mine], -1))

        def gather_all(own):
            x1, y0 = swap(own[1], 2), swap(own[0], 4)
            x0, y1 = swap(own[0], 2), swap(own[1], 4)
            d1, d0 = swap(x1, 4), swap(y0, 2)
            out = {0: own, 2: (x0, x1), 4: (y0, y1), 6: (d0, d1)}
            for j in (0, 2, 4, 6):
                out[j + 1] = tuple(swap(b, 1) for b in out[j])
            return out

        flat = ids.reshape(-1)
        n = flat.shape[0]
        loc = flat - r * vl
        own = (loc >= 0) & (loc < vl)
        diag = []
        for q in range(2):
            diag.append(pl.pallas_call(
                functools.partial(pdn_first_kernel, 3, q * hd),
                out_shape=(jax.ShapeDtypeStruct((mb, tl, hd), jnp.bfloat16),) * 2,
                in_specs=[SMEM, HBM, HBM],
                out_specs=(VMEM, VMEM),
                scratch_shapes=[
                    pltpu.VMEM((mb, tc, f), jnp.bfloat16),
                    pltpu.VMEM((hd, f), jnp.bfloat16),
                    pltpu.SemaphoreType.DMA,
                    pltpu.SemaphoreType.DMA((3,)),
                ],
                cost_estimate=pl.CostEstimate(flops=3_000_000, bytes_accessed=4_000_000, transcendentals=0),
                compiler_params=pltpu.CompilerParams(vmem_limit_bytes=60 * 2**20),
            )(c.reshape(1), du, w))
        part = {}
        part.update(pdn((1, 2)))
        part.update(pdn((0,)))
        d0, d1 = ([swap(diag[q][h], bit) for q in range(2)] for h, bit in ((0, 2), (1, 4)))
        ex, ey = swap(part[1][0], 2), swap(part[2][1], 4)
        tgt = jnp.where(own, 2 * (jnp.arange(n) % tc) + (loc & 1), -1).astype(jnp.int32)
        i0 = lax.broadcasted_iota(jnp.int32, (n, n), 0)
        i1 = lax.broadcasted_iota(jnp.int32, (n, n), 1)

        def by_piece(v):
            v = v.reshape(mb, 2, 2, 2, tl)
            for ax, bit in ((1, 4), (2, 2), (3, 1)):
                v = jnp.where((r & bit) > 0, jnp.flip(v, ax), v)
            return v.reshape(2, mb // 2, groups, tl).transpose(2, 0, 1, 3).reshape(-1)

        flat_p = by_piece(ids)
        loc_p = flat_p - r * vl
        own_p = (loc_p >= 0) & (loc_p < vl)
        first = jnp.min(jnp.where(flat_p[:, None] == flat_p[None, :], i0, n), axis=0)
        lead = own_p & (first == jnp.arange(n))
        pos = jnp.sum(jnp.where(lead[:, None] & (i0 < i1), 1, 0), axis=0)
        pos_of_first = jnp.sum(jnp.where((i0 == first[None, :]), pos[:, None], 0), axis=0)
        slot = jnp.where(own_p, pos_of_first, -1).astype(jnp.int32)
        rows = jnp.sum(jnp.where(lead[:, None] & (pos[:, None] == i1), loc_p[:, None], 0), axis=0).astype(jnp.int32)
        cnt = jnp.sum(lead.astype(jnp.int32)).reshape(1)
        n_owned = jnp.sum(own.astype(jnp.int32)).reshape(1)
        own_pos = jnp.sum(jnp.where(own[:, None] & (i0 < i1), 1, 0), axis=0)
        owned = jnp.sum(jnp.where(own[:, None] & (own_pos[:, None] == i1), i0, 0), axis=0).astype(jnp.int32)
        d0, d1, loc, tgt, slot, rows, cnt, owned, n_owned = lax.optimization_barrier(
            (d0, d1, loc, tgt, slot, rows, cnt, owned, n_owned)
        )

        def relay(mine, far, bit):
            left, right = f32(mine[..., :hd]) + f32(far[0]), f32(mine[..., hd:]) + f32(far[1])
            got = swap(pick(right, left), 1)
            v = pick(left, right) + got
            return swap(v[:CUT], bit), v[CUT:]

        (fy, ly), (fx, lx) = relay(part[2][0], d0, 4), relay(part[1][1], d1, 2)

        mine, far, near, de = pl.pallas_call(
            lookup_kernel,
            out_shape=(half_shape(4), half_shape(1), half_shape(3), de_shape),
            in_specs=[SMEM, SMEM, SMEM, SMEM, VMEM, ANY],
            out_specs=(VMEM, VMEM, VMEM, ANY),
            scratch_shapes=[pltpu.VMEM((2 * n, d), jnp.bfloat16), pltpu.SemaphoreType.DMA] + zero_scratch,
            cost_estimate=pl.CostEstimate(flops=40_000_000, bytes_accessed=60_000_000, transcendentals=0),
            compiler_params=pltpu.CompilerParams(vmem_limit_bytes=32 * 2**20),
            name="look",
        )(kc, owned, n_owned, loc, tgt.reshape(n, 1), emb)
        for first, last in ((LOOKUP_SHARE, ZERO_A), (ZERO_A, ZERO_B)):
            de = pl.pallas_call(
                functools.partial(zero_kernel, first, last),
                out_shape=de_shape,
                in_specs=[ANY],
                out_specs=ANY,
                scratch_shapes=zero_scratch,
                input_output_aliases={0: 0},
                cost_estimate=pl.CostEstimate(flops=10_000_000, bytes_accessed=20_000_000, transcendentals=0),
                compiler_params=pltpu.CompilerParams(vmem_limit_bytes=4 * 2**20),
            )(de)
        far, near = swap(far, 1), swap(near, 1)
        xpairs = {j: (mine[j], far[0] if j == 3 else near[j]) for j in range(4)}

        ly, lx = swap(ly, 4), swap(lx, 2)

        def widen(v):
            return to_rows(v, jnp.zeros_like(v))

        ex, ey, fy, fx, ly, lx = lax.optimization_barrier((ex, ey, fy, fx, ly, lx))
        v0 = f32(part[0][0]) + f32(ex) + widen(jnp.concatenate([fy, ly], axis=0))
        v1 = f32(part[0][1]) + f32(ey) + widen(jnp.concatenate([fx, lx], axis=0))
        keep, give = pick(v0, v1), pick(v1, v0)
        dn = keep + swap(give, 1)
        x0, x1 = reduce_to_home(xpairs, jnp.bfloat16)
        xo = gather_all((x0, x1))
        x = to_rows(jnp.where(k == 0, x0, x1), jnp.where(k == 0, xo[1][0], xo[1][1]))

        ns, u = [], None
        for j in range(4):
            more = (de,) if u is None else (u, de)
            nj, u, de = pl.pallas_call(
                functools.partial(norm_kernel, j),
                out_shape=(jax.ShapeDtypeStruct((d, mb * tc), jnp.bfloat16), jax.ShapeDtypeStruct((mb, t, f), jnp.bfloat16), de_shape),
                in_specs=[SMEM] + [VMEM] * 6 + [ANY] * len(more),
                out_specs=(VMEM, ANY, ANY),
                scratch_shapes=[
                    pltpu.VMEM((mb * tc, d), jnp.bfloat16),
                    pltpu.VMEM((mb, tc, f), jnp.bfloat16),
                    pltpu.SemaphoreType.DMA,
                ] + zero_scratch,
                input_output_aliases={7 + i: 3 - len(more) + i for i in range(len(more))},
                cost_estimate=pl.CostEstimate(flops=8_000_000, bytes_accessed=12_000_000, transcendentals=0),
                compiler_params=pltpu.CompilerParams(vmem_limit_bytes=24 * 2**20),
            )(kc, g.reshape(1, d), w, *(xo[2 * j + q][h] for h in range(2) for q in range(2)), *more)
            ns.append(nj)
        dw = pl.pallas_call(
            dw_kernel,
            out_shape=jax.ShapeDtypeStruct((d, f), jnp.float32),
            in_specs=[SMEM] + [VMEM] * 5,
            out_specs=ANY,
            scratch_shapes=[
                pltpu.VMEM((n, f), jnp.bfloat16),
                pltpu.VMEM((2, 512, f), jnp.float32),
                pltpu.SemaphoreType.DMA((2,)),
            ],
            cost_estimate=pl.CostEstimate(flops=30_000_000, bytes_accessed=40_000_000, transcendentals=0),
            compiler_params=pltpu.CompilerParams(vmem_limit_bytes=24 * 2**20),
            name="dw",
        )(c.reshape(1), du, *ns)

        xf = x.astype(jnp.float32)
        rs = lax.rsqrt(jnp.mean(xf * xf, axis=-1, keepdims=True) + EPS)
        nh = xf * rs
        gdn = gf * dn
        dxn = rs * (gdn - nh * jnp.mean(nh * gdn, axis=-1, keepdims=True))
        dx = (dres.astype(jnp.float32) + dxn).astype(jnp.bfloat16)
        dg = jnp.sum(dn * nh, axis=(0, 1))
        dxo = gather_all((dx[:mb // 2], dx[mb // 2:]))
        dxs = [b for j in range(8) for b in dxo[j]]
        for bit in (1, 2, 4):
            dg = dg + swap(dg, bit)

        de = pl.pallas_call(
            scatter_kernel,
            out_shape=de_shape,
            in_specs=[SMEM, SMEM, VMEM] + [VMEM] * 16 + [ANY],
            out_specs=ANY,
            scratch_shapes=[
                pltpu.VMEM((BLK, d), jnp.float32),
                pltpu.SemaphoreType.DMA,
            ],
            input_output_aliases={19: 0},
            compiler_params=pltpu.CompilerParams(vmem_limit_bytes=28 * 2**20),
            name="put",
        )(rows, cnt, slot.reshape(1, n), *dxs, de)
        return u, x, de, dw, dg

    return jax.shard_map(
        local,
        mesh=mesh,
        in_specs=(P("dp", None), P("tp", None), P(None), P(None, "tp"), P("dp", None, "tp"), P("dp", "tp", None)),
        out_specs=(P("dp", None, "tp"), P("dp", "tp", None), P(("dp", "tp"), None), P(None, ("dp", "tp")), P("dp")),
        check_vma=False,
    )
```

```python
import functools

import jax
import jax.numpy as jnp
from jax import lax
from jax.experimental import pallas as pl
from jax.experimental.pallas import tpu as pltpu
from jax.sharding import PartitionSpec as P

EPS = 1e-6
ANY = pl.BlockSpec(memory_space=pl.ANY)
VMEM = pl.BlockSpec(memory_space=pltpu.VMEM)
SMEM = pl.BlockSpec(memory_space=pltpu.SMEM)
HBM = pl.BlockSpec(memory_space=pltpu.HBM)
ZR = 128
BLK = 256
ZERO_FIRST, LOOKUP_EARLY, LOOKUP_SHARE, ZERO_A, ZERO_B, NORM_SHARE = 6, 14, 24, 36, 52, 3


def zero_fill(de, z, sem, first, last):

    def copy(i):
        return pltpu.make_async_copy(z, de.at[pl.ds(pl.multiple_of(i * ZR, ZR), ZR)], sem)

    def start(clear=True):
        if clear:
            z[...] = jnp.zeros_like(z)
        pl.loop(first, last)(lambda i: copy(i).start())

    def wait():
        pl.loop(first, last)(lambda i: copy(i).wait())

    return start, wait


def zero_kernel(first, last, *refs):
    de, z, sem = refs[-3:]
    start, wait = zero_fill(de, z, sem, first, last)
    start()
    wait()


def pdn_first_kernel(j, col0, c_ref, du_hbm, w_hbm, h0, h1, du_ref, w_ref, sem, wsem):
    c = c_ref[0]
    mb, tc, _ = du_ref.shape
    tl = tc // 2
    wc = 512
    steps = w_ref.shape[0] // wc
    z = pl.multiple_of(jnp.bitwise_xor(c, j) * tc, tc)
    rows_in = pltpu.make_async_copy(du_hbm.at[:, pl.ds(z, tc), :], du_ref, sem)
    rows_in.start()
    loads = [
        pltpu.make_async_copy(w_hbm.at[pl.ds(col0 + n * wc, wc)], w_ref.at[pl.ds(n * wc, wc)], wsem.at[n]) for n in range(steps)
    ]
    for cp in loads:
        cp.start()
    rows_in.wait()
    rows = du_ref[...].reshape(mb * tc, du_ref.shape[2])
    for n in range(steps):
        loads[n].wait()
        cols = slice(n * wc, (n + 1) * wc)
        v = lax.dot_general(rows, w_ref[cols, :], (((1,), (1,)), ((), ())), preferred_element_type=jnp.float32)
        v = v.astype(jnp.bfloat16).reshape(mb, tc, wc)
        h0[:, :, cols] = v[:, :tl]
        h1[:, :, cols] = v[:, tl:]


def pdn_kernel(js, c_ref, du_ref, w_ref, *outs):
    c = c_ref[0]
    mb, t, _ = du_ref.shape
    tc, wc = t // 4, 512
    tl = tc // 2
    for i, j in enumerate(js):
        z = pl.multiple_of(jnp.bitwise_xor(c, j) * tc, tc)
        rows = jnp.concatenate([du_ref[m, pl.ds(z, tc), :] for m in range(mb)], axis=0)
        for n in range(w_ref.shape[0] // wc):
            cols = slice(n * wc, (n + 1) * wc)
            v = lax.dot_general(rows, w_ref[cols, :], (((1,), (1,)), ((), ())), preferred_element_type=jnp.float32)
            v = v.astype(jnp.bfloat16).reshape(mb, tc, wc)
            for h in range(2):
                outs[2 * i + h][:, :, cols] = v[:, h * tl:(h + 1) * tl]


def lookup_kernel(kc_ref, list_ref, cnt_ref, loc_ref, tgt_ref, emb, de_in, mine_ref, far_ref, near_ref, de, buf, sem, z, zsem):
    del de_in
    k, c = kc_ref[0], kc_ref[1]
    _, d = emb.shape
    nj, mb, tc, hd = mine_ref.shape
    n = nj * mb * tc
    step = 64
    start, wait = zero_fill(de, z, zsem, ZERO_FIRST, LOOKUP_EARLY)
    late_start, late_wait = zero_fill(de, z, zsem, LOOKUP_EARLY, LOOKUP_SHARE)
    start()

    @pl.loop(0, 2 * n // step)
    def _(i):
        buf[pl.ds(pl.multiple_of(i * step, step), step), :] = jnp.zeros((step, d), buf.dtype)

    def copy(t, l):
        src = emb.at[pl.ds(pl.multiple_of((l >> 1) * 2, 2), 2)]
        return pltpu.make_async_copy(src, buf.at[pl.ds(pl.multiple_of(t * 2, 2), 2)], sem)

    cnt = cnt_ref[0]

    @pl.loop(0, cnt)
    def _(q):
        t = list_ref[q]
        copy(t, loc_ref[t]).start()

    @pl.loop(0, cnt)
    def _(i):
        copy(0, 0).wait()

    late_start(False)

    for j in range(nj):
        theirs = far_ref.at[0] if j == 3 else near_ref.at[j]
        zc = jnp.bitwise_xor(c, j)

        @pl.loop(0, mb)
        def _(m):
            t0 = m * (nj * tc) + zc * tc
            tgt = tgt_ref[pl.ds(pl.multiple_of(t0, tc), tc), :]
            sel = (lax.broadcasted_iota(jnp.int32, (tc, 2 * tc), 1) == tgt).astype(jnp.bfloat16)
            rows = pl.ds(pl.multiple_of(2 * t0, 2 * tc), 2 * tc)
            for out, half in ((theirs, 1 - k), (mine_ref.at[j], k)):
                v = buf[rows, pl.ds(pl.multiple_of(half * hd, 128), hd)]
                out[m] = jnp.dot(sel, v, preferred_element_type=jnp.float32).astype(jnp.bfloat16)

    wait()
    late_wait()


def norm_kernel(j, kc_ref, g_ref, w_ref, *refs):
    blocks, (nt_ref, u_ref, de, n_ref, stage, sem, z, zsem) = refs[:4], refs[-8:]
    k = kc_ref[0]
    d = nt_ref.shape[0]
    mb, tl, hd = blocks[0].shape
    tc = 2 * tl
    first = ZERO_B + j * NORM_SHARE
    start, wait = zero_fill(de, z, zsem, first, first + NORM_SHARE)
    start()
    at = [pl.ds(pl.multiple_of(jnp.bitwise_xor(k, q) * hd, 128), hd) for q in range(2)]
    gf = [g_ref[:, at[q]].astype(jnp.float32) for q in range(2)]

    @pl.loop(0, mb)
    def _(m):
        for h in range(2):
            xf = [blocks[2 * h + q][m].astype(jnp.float32) for q in range(2)]
            total = sum(jnp.sum(v * v, axis=-1, keepdims=True) for v in xf)
            rs = lax.rsqrt(total * (1.0 / d) + EPS)
            for q in range(2):
                to = pl.ds(pl.multiple_of(m * tc + h * tl, tl), tl)
                n_ref[to, at[q]] = (xf[q] * rs * gf[q]).astype(jnp.bfloat16)

    v = jnp.dot(n_ref[...], w_ref[...], preferred_element_type=jnp.float32)
    stage[...] = v.astype(jnp.bfloat16).reshape(stage.shape)
    rows = pl.ds(pl.multiple_of(jnp.bitwise_xor(kc_ref[1], j) * tc, tc), tc)
    copy = pltpu.make_async_copy(stage, u_ref.at[:, rows, :], sem)
    copy.start()
    wc = 512

    @pl.loop(0, d // wc)
    def _(i):
        c = pl.ds(pl.multiple_of(i * wc, wc), wc)
        nt_ref[c, :] = n_ref[:, c].T

    copy.wait()
    wait()


def dw_kernel(c_ref, du_ref, *refs):
    ns, (dw, right, stage, sem) = refs[:4], refs[-4:]
    mb, _, _ = du_ref.shape
    d, kj = ns[0].shape
    tc = kj // mb
    for j in range(4):
        rows = pl.ds(pl.multiple_of(jnp.bitwise_xor(c_ref[0], j) * tc, tc), tc)
        for m in range(mb):
            right[j * kj + m * tc:j * kj + (m + 1) * tc, :] = du_ref[m, rows, :]
    dc = stage.shape[1]

    def copy(i, q):
        return pltpu.make_async_copy(stage.at[q], dw.at[pl.ds(pl.multiple_of(i * dc, dc), dc)], sem.at[q])

    @pl.loop(0, d // dc)
    def _(i):
        q = lax.rem(i, 2)

        @pl.when(i >= 2)
        def _():
            copy(i - 2, q).wait()

        c = pl.ds(pl.multiple_of(i * dc, dc), dc)
        left = jnp.concatenate([n[c, :] for n in ns], axis=1)
        stage[q] = jnp.dot(left, right[...], preferred_element_type=jnp.float32)
        copy(i, q).start()

    for q in range(2):
        copy(d // dc - 2 + q, q).wait()


def scatter_kernel(rows_ref, cnt_ref, slot_ref, *refs):
    blocks, (de, stage, out_sem) = refs[:16], refs[-3:]
    hb, tl, d = blocks[0].shape
    kb = hb * tl
    cnt = cnt_ref[0]
    cc = 512

    def copy(q, r, size=1):
        return pltpu.make_async_copy(stage.at[pl.ds(q, size)], de.at[pl.ds(r, size)], out_sem)

    @pl.loop(0, (cnt + BLK - 1) // BLK)
    def _(b):
        base = b * BLK
        ids = lax.broadcasted_iota(jnp.int32, (BLK, len(blocks) * kb), 0) + base
        oh = (ids == slot_ref[...]).astype(jnp.bfloat16)
        for i in range(d // cc):
            cols = slice(i * cc, (i + 1) * cc)
            right = jnp.concatenate([v[:, :, cols].reshape(kb, cc) for v in blocks], axis=0)
            stage[:, cols] = jnp.dot(oh, right, preferred_element_type=jnp.float32)
        n = jnp.minimum(cnt - base, BLK)
        full = n // 8

        @pl.loop(0, full)
        def _(i):
            for u in range(8):
                copy(i * 8 + u, rows_ref[base + i * 8 + u]).start()

        pl.loop(full * 8, n)(lambda q: copy(q, rows_ref[base + q]).start())
        for bit in range(9):

            @pl.when((n >> bit) & 1 == 1)
            def _():
                copy(0, 0, 1 << bit).wait()


def solution(mesh):
    groups = mesh.shape["tp"]

    def swap(v, bit):
        return lax.ppermute(v, "tp", [(i, i ^ bit) for i in range(groups)])

    def local(ids, emb, g, w, du, dres):
        r = lax.axis_index("tp")
        mb, t = ids.shape
        vl, d = emb.shape
        f = w.shape[1]
        tl = t // groups
        hd = d // 2
        tc = t // 4
        k, c = r & 1, r >> 1
        gf = g.astype(jnp.float32)
        kc = jnp.stack([k, c]).astype(jnp.int32)
        de_shape = jax.ShapeDtypeStruct((vl, d), jnp.float32)
        zero_scratch = [pltpu.VMEM((ZR, d), jnp.float32), pltpu.SemaphoreType.DMA]

        def half_shape(nj):
            return jax.ShapeDtypeStruct((nj, mb, tc, hd), jnp.bfloat16)

        def zeros(first, last, *de):
            return pl.pallas_call(
                functools.partial(zero_kernel, first, last),
                out_shape=de_shape,
                in_specs=[ANY] * len(de),
                out_specs=ANY,
                scratch_shapes=zero_scratch,
                input_output_aliases={0: 0} if de else {},
                cost_estimate=pl.CostEstimate(flops=10_000_000, bytes_accessed=20_000_000, transcendentals=0),
                compiler_params=pltpu.CompilerParams(vmem_limit_bytes=4 * 2**20),
            )(*de)

        def pdn(js):
            out = pl.pallas_call(
                functools.partial(pdn_kernel, js),
                out_shape=(jax.ShapeDtypeStruct((mb, tl, d), jnp.bfloat16),) * (2 * len(js)),
                in_specs=[SMEM, VMEM, VMEM],
                out_specs=(VMEM,) * (2 * len(js)),
                cost_estimate=pl.CostEstimate(flops=5_000_000 * len(js), bytes_accessed=8_000_000, transcendentals=0),
                compiler_params=pltpu.CompilerParams(vmem_limit_bytes=20 * 2**20),
            )(c.reshape(1), du, w)
            return {j: out[2 * i:2 * i + 2] for i, j in enumerate(js)}

        def pick(a, b):
            return jnp.where(k == 0, a, b)

        def f32(v):
            return v.astype(jnp.float32)

        def reduce_to_home(pairs, dt):
            def part(j, h):
                a, b = pairs[j]
                return a[:, h * tl:(h + 1) * tl].astype(dt) + b[:, h * tl:(h + 1) * tl].astype(dt)

            dx_ = swap(part(3, 0), 2)
            dy_ = swap(part(3, 1), 4)
            ex = swap(part(1, 0), 2)
            ey = swap(part(2, 1), 4)
            pairs = dict(pairs)
            pairs[2], dx_ = lax.optimization_barrier((pairs[2], dx_))
            pairs[1], dy_ = lax.optimization_barrier((pairs[1], dy_))
            fy = swap(part(2, 0) + dx_, 4)
            fx = swap(part(1, 1) + dy_, 2)
            pairs[0], ex, ey = lax.optimization_barrier((pairs[0], ex, ey))
            return part(0, 0) + ex + fy, part(0, 1) + ey + fx

        def to_rows(mine, other):
            return jnp.where(k == 0, jnp.concatenate([mine, other], -1), jnp.concatenate([other, mine], -1))

        def gather_all(own):
            x1, y0 = swap(own[1], 2), swap(own[0], 4)
            x0, y1 = swap(own[0], 2), swap(own[1], 4)
            d1, d0 = swap(x1, 4), swap(y0, 2)
            out = {0: own, 2: (x0, x1), 4: (y0, y1), 6: (d0, d1)}
            for j in (0, 2, 4, 6):
                out[j + 1] = tuple(swap(b, 1) for b in out[j])
            return out

        flat = ids.reshape(-1)
        n = flat.shape[0]
        loc = flat - r * vl
        own = (loc >= 0) & (loc < vl)
        diag = []
        for q in range(2):
            diag.append(pl.pallas_call(
                functools.partial(pdn_first_kernel, 3, q * hd),
                out_shape=(jax.ShapeDtypeStruct((mb, tl, hd), jnp.bfloat16),) * 2,
                in_specs=[SMEM, HBM, HBM],
                out_specs=(VMEM, VMEM),
                scratch_shapes=[
                    pltpu.VMEM((mb, tc, f), jnp.bfloat16),
                    pltpu.VMEM((hd, f), jnp.bfloat16),
                    pltpu.SemaphoreType.DMA,
                    pltpu.SemaphoreType.DMA((3,)),
                ],
                cost_estimate=pl.CostEstimate(flops=3_000_000, bytes_accessed=4_000_000, transcendentals=0),
                compiler_params=pltpu.CompilerParams(vmem_limit_bytes=60 * 2**20),
            )(c.reshape(1), du, w))
        part = {}
        part.update(pdn((1, 2)))
        part.update(pdn((0,)))
        de = zeros(0, ZERO_FIRST)
        d0, d1 = ([swap(diag[q][h], bit) for q in range(2)] for h, bit in ((0, 2), (1, 4)))
        ex, ey = swap(part[1][0], 2), swap(part[2][1], 4)
        tgt = jnp.where(own, 2 * (jnp.arange(n) % tc) + (loc & 1), -1).astype(jnp.int32)
        i0 = lax.broadcasted_iota(jnp.int32, (n, n), 0)
        i1 = lax.broadcasted_iota(jnp.int32, (n, n), 1)

        def by_piece(v):
            v = v.reshape(mb, 2, 2, 2, tl)
            for ax, bit in ((1, 4), (2, 2), (3, 1)):
                v = jnp.where((r & bit) > 0, jnp.flip(v, ax), v)
            return v.reshape(2, mb // 2, groups, tl).transpose(2, 0, 1, 3).reshape(-1)

        flat_p = by_piece(ids)
        loc_p = flat_p - r * vl
        own_p = (loc_p >= 0) & (loc_p < vl)
        first = jnp.min(jnp.where(flat_p[:, None] == flat_p[None, :], i0, n), axis=0)
        lead = own_p & (first == jnp.arange(n))
        pos = jnp.sum(jnp.where(lead[:, None] & (i0 < i1), 1, 0), axis=0)
        pos_of_first = jnp.sum(jnp.where((i0 == first[None, :]), pos[:, None], 0), axis=0)
        slot = jnp.where(own_p, pos_of_first, -1).astype(jnp.int32)
        rows = jnp.sum(jnp.where(lead[:, None] & (pos[:, None] == i1), loc_p[:, None], 0), axis=0).astype(jnp.int32)
        cnt = jnp.sum(lead.astype(jnp.int32)).reshape(1)
        n_owned = jnp.sum(own.astype(jnp.int32)).reshape(1)
        own_pos = jnp.sum(jnp.where(own[:, None] & (i0 < i1), 1, 0), axis=0)
        owned = jnp.sum(jnp.where(own[:, None] & (own_pos[:, None] == i1), i0, 0), axis=0).astype(jnp.int32)
        d0, d1, loc, tgt, slot, rows, cnt, owned, n_owned = lax.optimization_barrier(
            (d0, d1, loc, tgt, slot, rows, cnt, owned, n_owned)
        )

        def relay(mine, far, bit):
            left, right = f32(mine[..., :hd]) + f32(far[0]), f32(mine[..., hd:]) + f32(far[1])
            got = swap(pick(right, left), 1)
            return swap(pick(left, right) + got, bit)

        fy, fx = relay(part[2][0], d0, 4), relay(part[1][1], d1, 2)

        mine, far, near, de = pl.pallas_call(
            lookup_kernel,
            out_shape=(half_shape(4), half_shape(1), half_shape(3), de_shape),
            in_specs=[SMEM, SMEM, SMEM, SMEM, VMEM, ANY, ANY],
            input_output_aliases={6: 3},
            out_specs=(VMEM, VMEM, VMEM, ANY),
            scratch_shapes=[pltpu.VMEM((2 * n, d), jnp.bfloat16), pltpu.SemaphoreType.DMA] + zero_scratch,
            cost_estimate=pl.CostEstimate(flops=40_000_000, bytes_accessed=60_000_000, transcendentals=0),
            compiler_params=pltpu.CompilerParams(vmem_limit_bytes=32 * 2**20),
            name="look",
        )(kc, owned, n_owned, loc, tgt.reshape(n, 1), emb, de)
        de = zeros(LOOKUP_SHARE, ZERO_A, de)
        de = zeros(ZERO_A, ZERO_B, de)
        far, near = swap(far, 1), swap(near, 1)
        xpairs = {j: (mine[j], far[0] if j == 3 else near[j]) for j in range(4)}

        def widen(v):
            return to_rows(v, jnp.zeros_like(v))

        v0 = f32(part[0][0]) + f32(ex) + widen(fy)
        v1 = f32(part[0][1]) + f32(ey) + widen(fx)
        dn = pick(v0, v1) + swap(pick(v1, v0), 1)
        x0, x1 = reduce_to_home(xpairs, jnp.bfloat16)
        xo = gather_all((x0, x1))
        x = to_rows(jnp.where(k == 0, x0, x1), jnp.where(k == 0, xo[1][0], xo[1][1]))

        ns, u = [], None
        for j in range(4):
            more = (de,) if u is None else (u, de)
            nj, u, de = pl.pallas_call(
                functools.partial(norm_kernel, j),
                out_shape=(jax.ShapeDtypeStruct((d, mb * tc), jnp.bfloat16), jax.ShapeDtypeStruct((mb, t, f), jnp.bfloat16), de_shape),
                in_specs=[SMEM] + [VMEM] * 6 + [ANY] * len(more),
                out_specs=(VMEM, ANY, ANY),
                scratch_shapes=[
                    pltpu.VMEM((mb * tc, d), jnp.bfloat16),
                    pltpu.VMEM((mb, tc, f), jnp.bfloat16),
                    pltpu.SemaphoreType.DMA,
                ] + zero_scratch,
                input_output_aliases={7 + i: 3 - len(more) + i for i in range(len(more))},
                cost_estimate=pl.CostEstimate(flops=8_000_000, bytes_accessed=12_000_000, transcendentals=0),
                compiler_params=pltpu.CompilerParams(vmem_limit_bytes=24 * 2**20),
            )(kc, g.reshape(1, d), w, *(xo[2 * j + q][h] for h in range(2) for q in range(2)), *more)
            ns.append(nj)
        dw = pl.pallas_call(
            dw_kernel,
            out_shape=jax.ShapeDtypeStruct((d, f), jnp.float32),
            in_specs=[SMEM] + [VMEM] * 5,
            out_specs=ANY,
            scratch_shapes=[
                pltpu.VMEM((n, f), jnp.bfloat16),
                pltpu.VMEM((2, 512, f), jnp.float32),
                pltpu.SemaphoreType.DMA((2,)),
            ],
            cost_estimate=pl.CostEstimate(flops=30_000_000, bytes_accessed=40_000_000, transcendentals=0),
            compiler_params=pltpu.CompilerParams(vmem_limit_bytes=24 * 2**20),
            name="dw",
        )(c.reshape(1), du, *ns)

        xf = x.astype(jnp.float32)
        rs = lax.rsqrt(jnp.mean(xf * xf, axis=-1, keepdims=True) + EPS)
        nh = xf * rs
        gdn = gf * dn
        dxn = rs * (gdn - nh * jnp.mean(nh * gdn, axis=-1, keepdims=True))
        dx = (dres.astype(jnp.float32) + dxn).astype(jnp.bfloat16)
        dg = jnp.sum(dn * nh, axis=(0, 1))
        dxo = gather_all((dx[:mb // 2], dx[mb // 2:]))
        dxs = [b for j in range(8) for b in dxo[j]]
        for bit in (1, 2, 4):
            dg = dg + swap(dg, bit)

        de = pl.pallas_call(
            scatter_kernel,
            out_shape=de_shape,
            in_specs=[SMEM, SMEM, VMEM] + [VMEM] * 16 + [ANY],
            out_specs=ANY,
            scratch_shapes=[
                pltpu.VMEM((BLK, d), jnp.float32),
                pltpu.SemaphoreType.DMA,
            ],
            input_output_aliases={19: 0},
            compiler_params=pltpu.CompilerParams(vmem_limit_bytes=28 * 2**20),
            name="put",
        )(rows, cnt, slot.reshape(1, n), *dxs, de)
        return u, x, de, dw, dg

    return jax.shard_map(
        local,
        mesh=mesh,
        in_specs=(P("dp", None), P("tp", None), P(None), P(None, "tp"), P("dp", None, "tp"), P("dp", "tp", None)),
        out_specs=(P("dp", None, "tp"), P("dp", "tp", None), P(("dp", "tp"), None), P(None, ("dp", "tp")), P("dp")),
        check_vma=False,
    )
```

```python
import functools

import jax
import jax.numpy as jnp
from jax import lax
from jax.experimental import pallas as pl
from jax.experimental.pallas import tpu as pltpu
from jax.sharding import PartitionSpec as P

EPS = 1e-6
ANY = pl.BlockSpec(memory_space=pl.ANY)
VMEM = pl.BlockSpec(memory_space=pltpu.VMEM)
SMEM = pl.BlockSpec(memory_space=pltpu.SMEM)
HBM = pl.BlockSpec(memory_space=pltpu.HBM)
ZR = 128
BLK = 256
ZERO_FIRST, LOOKUP_EARLY, LOOKUP_SHARE, ZERO_A, ZERO_B, NORM_SHARE = 2, 10, 22, 33, 48, 4


def zero_fill(de, z, sem, first, last):

    def copy(i):
        return pltpu.make_async_copy(z, de.at[pl.ds(pl.multiple_of(i * ZR, ZR), ZR)], sem)

    def start(clear=True):
        if clear:
            z[...] = jnp.zeros_like(z)
        pl.loop(first, last)(lambda i: copy(i).start())

    def wait():
        pl.loop(first, last)(lambda i: copy(i).wait())

    return start, wait


def zero_kernel(first, last, *refs):
    de, z, sem = refs[-3:]
    start, wait = zero_fill(de, z, sem, first, last)
    start()
    wait()


def pdn_first_kernel(j, col0, c_ref, du_hbm, w_hbm, h0, h1, du_ref, w_ref, sem, wsem):
    c = c_ref[0]
    mb, tc, _ = du_ref.shape
    tl = tc // 2
    wc = 512
    steps = w_ref.shape[0] // wc
    z = pl.multiple_of(jnp.bitwise_xor(c, j) * tc, tc)
    rows_in = pltpu.make_async_copy(du_hbm.at[:, pl.ds(z, tc), :], du_ref, sem)
    rows_in.start()
    loads = [
        pltpu.make_async_copy(w_hbm.at[pl.ds(col0 + n * wc, wc)], w_ref.at[pl.ds(n * wc, wc)], wsem.at[n]) for n in range(steps)
    ]
    for cp in loads:
        cp.start()
    rows_in.wait()
    rows = du_ref[...].reshape(mb * tc, du_ref.shape[2])
    for n in range(steps):
        loads[n].wait()
        cols = slice(n * wc, (n + 1) * wc)
        v = lax.dot_general(rows, w_ref[cols, :], (((1,), (1,)), ((), ())), preferred_element_type=jnp.float32)
        v = v.astype(jnp.bfloat16).reshape(mb, tc, wc)
        h0[:, :, cols] = v[:, :tl]
        h1[:, :, cols] = v[:, tl:]


def pdn_kernel(js, c_ref, du_ref, w_ref, *outs):
    c = c_ref[0]
    mb, t, _ = du_ref.shape
    tc, wc = t // 4, 512
    tl = tc // 2
    for i, j in enumerate(js):
        z = pl.multiple_of(jnp.bitwise_xor(c, j) * tc, tc)
        rows = jnp.concatenate([du_ref[m, pl.ds(z, tc), :] for m in range(mb)], axis=0)
        for n in range(w_ref.shape[0] // wc):
            cols = slice(n * wc, (n + 1) * wc)
            v = lax.dot_general(rows, w_ref[cols, :], (((1,), (1,)), ((), ())), preferred_element_type=jnp.float32)
            v = v.astype(jnp.bfloat16).reshape(mb, tc, wc)
            for h in range(2):
                outs[2 * i + h][:, :, cols] = v[:, h * tl:(h + 1) * tl]


def lookup_kernel(kc_ref, list_ref, cnt_ref, loc_ref, tgt_ref, emb, de_in, mine_ref, far_ref, near_ref, de, buf, sem, z, zsem):
    del de_in
    k, c = kc_ref[0], kc_ref[1]
    _, d = emb.shape
    nj, mb, tc, hd = mine_ref.shape
    n = nj * mb * tc
    step = 64
    start, wait = zero_fill(de, z, zsem, ZERO_FIRST, LOOKUP_EARLY)
    late_start, late_wait = zero_fill(de, z, zsem, LOOKUP_EARLY, LOOKUP_SHARE)
    start()

    @pl.loop(0, 2 * n // step)
    def _(i):
        buf[pl.ds(pl.multiple_of(i * step, step), step), :] = jnp.zeros((step, d), buf.dtype)

    def copy(t, l):
        src = emb.at[pl.ds(pl.multiple_of((l >> 1) * 2, 2), 2)]
        return pltpu.make_async_copy(src, buf.at[pl.ds(pl.multiple_of(t * 2, 2), 2)], sem)

    cnt = cnt_ref[0]

    @pl.loop(0, cnt)
    def _(q):
        t = list_ref[q]
        copy(t, loc_ref[t]).start()

    @pl.loop(0, cnt)
    def _(i):
        copy(0, 0).wait()

    late_start(False)

    for j in range(nj):
        theirs = far_ref.at[0] if j == 3 else near_ref.at[j]
        zc = jnp.bitwise_xor(c, j)

        @pl.loop(0, mb)
        def _(m):
            t0 = m * (nj * tc) + zc * tc
            tgt = tgt_ref[pl.ds(pl.multiple_of(t0, tc), tc), :]
            sel = (lax.broadcasted_iota(jnp.int32, (tc, 2 * tc), 1) == tgt).astype(jnp.bfloat16)
            rows = pl.ds(pl.multiple_of(2 * t0, 2 * tc), 2 * tc)
            for out, half in ((theirs, 1 - k), (mine_ref.at[j], k)):
                v = buf[rows, pl.ds(pl.multiple_of(half * hd, 128), hd)]
                out[m] = jnp.dot(sel, v, preferred_element_type=jnp.float32).astype(jnp.bfloat16)

    wait()
    late_wait()


def norm_kernel(j, kc_ref, g_ref, w_ref, *refs):
    blocks, (nt_ref, u_ref, de, n_ref, stage, sem, z, zsem) = refs[:4], refs[-8:]
    k = kc_ref[0]
    d = nt_ref.shape[0]
    mb, tl, hd = blocks[0].shape
    tc = 2 * tl
    first = ZERO_B + j * NORM_SHARE
    start, wait = zero_fill(de, z, zsem, first, first + NORM_SHARE)
    start()
    at = [pl.ds(pl.multiple_of(jnp.bitwise_xor(k, q) * hd, 128), hd) for q in range(2)]
    gf = [g_ref[:, at[q]].astype(jnp.float32) for q in range(2)]

    @pl.loop(0, mb)
    def _(m):
        for h in range(2):
            xf = [blocks[2 * h + q][m].astype(jnp.float32) for q in range(2)]
            total = sum(jnp.sum(v * v, axis=-1, keepdims=True) for v in xf)
            rs = lax.rsqrt(total * (1.0 / d) + EPS)
            for q in range(2):
                to = pl.ds(pl.multiple_of(m * tc + h * tl, tl), tl)
                n_ref[to, at[q]] = (xf[q] * rs * gf[q]).astype(jnp.bfloat16)

    v = jnp.dot(n_ref[...], w_ref[...], preferred_element_type=jnp.float32)
    stage[...] = v.astype(jnp.bfloat16).reshape(stage.shape)
    rows = pl.ds(pl.multiple_of(jnp.bitwise_xor(kc_ref[1], j) * tc, tc), tc)
    copy = pltpu.make_async_copy(stage, u_ref.at[:, rows, :], sem)
    copy.start()
    wc = 512

    @pl.loop(0, d // wc)
    def _(i):
        c = pl.ds(pl.multiple_of(i * wc, wc), wc)
        nt_ref[c, :] = n_ref[:, c].T

    copy.wait()
    wait()


def dw_kernel(c_ref, du_ref, *refs):
    ns, (dw, right, stage, sem) = refs[:4], refs[-4:]
    mb, _, _ = du_ref.shape
    d, kj = ns[0].shape
    tc = kj // mb
    for j in range(4):
        rows = pl.ds(pl.multiple_of(jnp.bitwise_xor(c_ref[0], j) * tc, tc), tc)
        for m in range(mb):
            right[j * kj + m * tc:j * kj + (m + 1) * tc, :] = du_ref[m, rows, :]
    dc = stage.shape[1]

    def copy(i, q):
        return pltpu.make_async_copy(stage.at[q], dw.at[pl.ds(pl.multiple_of(i * dc, dc), dc)], sem.at[q])

    @pl.loop(0, d // dc)
    def _(i):
        q = lax.rem(i, 2)

        @pl.when(i >= 2)
        def _():
            copy(i - 2, q).wait()

        c = pl.ds(pl.multiple_of(i * dc, dc), dc)
        left = jnp.concatenate([n[c, :] for n in ns], axis=1)
        stage[q] = jnp.dot(left, right[...], preferred_element_type=jnp.float32)
        copy(i, q).start()

    for q in range(2):
        copy(d // dc - 2 + q, q).wait()


def scatter_kernel(rows_ref, cnt_ref, slot_ref, *refs):
    blocks, (de, stage, out_sem) = refs[:16], refs[-3:]
    hb, tl, d = blocks[0].shape
    kb = hb * tl
    cnt = cnt_ref[0]
    cc = 512

    def copy(q, r, size=1):
        return pltpu.make_async_copy(stage.at[pl.ds(q, size)], de.at[pl.ds(r, size)], out_sem)

    @pl.loop(0, (cnt + BLK - 1) // BLK)
    def _(b):
        base = b * BLK
        ids = lax.broadcasted_iota(jnp.int32, (BLK, len(blocks) * kb), 0) + base
        oh = (ids == slot_ref[...]).astype(jnp.bfloat16)
        for i in range(d // cc):
            cols = slice(i * cc, (i + 1) * cc)
            right = jnp.concatenate([v[:, :, cols].reshape(kb, cc) for v in blocks], axis=0)
            stage[:, cols] = jnp.dot(oh, right, preferred_element_type=jnp.float32)
        n = jnp.minimum(cnt - base, BLK)
        full = n // 8

        @pl.loop(0, full)
        def _(i):
            for u in range(8):
                copy(i * 8 + u, rows_ref[base + i * 8 + u]).start()

        pl.loop(full * 8, n)(lambda q: copy(q, rows_ref[base + q]).start())
        for bit in range(9):

            @pl.when((n >> bit) & 1 == 1)
            def _():
                copy(0, 0, 1 << bit).wait()


def solution(mesh):
    groups = mesh.shape["tp"]

    def swap(v, bit):
        return lax.ppermute(v, "tp", [(i, i ^ bit) for i in range(groups)])

    def local(ids, emb, g, w, du, dres):
        r = lax.axis_index("tp")
        mb, t = ids.shape
        vl, d = emb.shape
        f = w.shape[1]
        tl = t // groups
        hd = d // 2
        tc = t // 4
        k, c = r & 1, r >> 1
        gf = g.astype(jnp.float32)
        kc = jnp.stack([k, c]).astype(jnp.int32)
        de_shape = jax.ShapeDtypeStruct((vl, d), jnp.float32)
        zero_scratch = [pltpu.VMEM((ZR, d), jnp.float32), pltpu.SemaphoreType.DMA]

        def half_shape(nj):
            return jax.ShapeDtypeStruct((nj, mb, tc, hd), jnp.bfloat16)

        def zeros(first, last, *de):
            return pl.pallas_call(
                functools.partial(zero_kernel, first, last),
                out_shape=de_shape,
                in_specs=[ANY] * len(de),
                out_specs=ANY,
                scratch_shapes=zero_scratch,
                input_output_aliases={0: 0} if de else {},
                cost_estimate=pl.CostEstimate(flops=10_000_000, bytes_accessed=20_000_000, transcendentals=0),
                compiler_params=pltpu.CompilerParams(vmem_limit_bytes=4 * 2**20),
            )(*de)

        def pdn(js):
            out = pl.pallas_call(
                functools.partial(pdn_kernel, js),
                out_shape=(jax.ShapeDtypeStruct((mb, tl, d), jnp.bfloat16),) * (2 * len(js)),
                in_specs=[SMEM, VMEM, VMEM],
                out_specs=(VMEM,) * (2 * len(js)),
                cost_estimate=pl.CostEstimate(flops=5_000_000 * len(js), bytes_accessed=8_000_000, transcendentals=0),
                compiler_params=pltpu.CompilerParams(vmem_limit_bytes=20 * 2**20),
            )(c.reshape(1), du, w)
            return {j: out[2 * i:2 * i + 2] for i, j in enumerate(js)}

        def pick(a, b):
            return jnp.where(k == 0, a, b)

        def f32(v):
            return v.astype(jnp.float32)

        def reduce_to_home(pairs, dt):
            def part(j, h):
                a, b = pairs[j]
                return a[:, h * tl:(h + 1) * tl].astype(dt) + b[:, h * tl:(h + 1) * tl].astype(dt)

            dx_ = swap(part(3, 0), 2)
            dy_ = swap(part(3, 1), 4)
            ex = swap(part(1, 0), 2)
            ey = swap(part(2, 1), 4)
            pairs = dict(pairs)
            pairs[2], dx_ = lax.optimization_barrier((pairs[2], dx_))
            pairs[1], dy_ = lax.optimization_barrier((pairs[1], dy_))
            fy = swap(part(2, 0) + dx_, 4)
            fx = swap(part(1, 1) + dy_, 2)
            pairs[0], ex, ey = lax.optimization_barrier((pairs[0], ex, ey))
            return part(0, 0) + ex + fy, part(0, 1) + ey + fx

        def to_rows(mine, other):
            return jnp.where(k == 0, jnp.concatenate([mine, other], -1), jnp.concatenate([other, mine], -1))

        def gather_all(own):
            x1, y0 = swap(own[1], 2), swap(own[0], 4)
            x0, y1 = swap(own[0], 2), swap(own[1], 4)
            d1, d0 = swap(x1, 4), swap(y0, 2)
            out = {0: own, 2: (x0, x1), 4: (y0, y1), 6: (d0, d1)}
            for j in (0, 2, 4, 6):
                out[j + 1] = tuple(swap(b, 1) for b in out[j])
            return out

        flat = ids.reshape(-1)
        n = flat.shape[0]
        loc = flat - r * vl
        own = (loc >= 0) & (loc < vl)
        diag = []
        for q in range(2):
            diag.append(pl.pallas_call(
                functools.partial(pdn_first_kernel, 3, q * hd),
                out_shape=(jax.ShapeDtypeStruct((mb, tl, hd), jnp.bfloat16),) * 2,
                in_specs=[SMEM, HBM, HBM],
                out_specs=(VMEM, VMEM),
                scratch_shapes=[
                    pltpu.VMEM((mb, tc, f), jnp.bfloat16),
                    pltpu.VMEM((hd, f), jnp.bfloat16),
                    pltpu.SemaphoreType.DMA,
                    pltpu.SemaphoreType.DMA((3,)),
                ],
                cost_estimate=pl.CostEstimate(flops=3_000_000, bytes_accessed=4_000_000, transcendentals=0),
                compiler_params=pltpu.CompilerParams(vmem_limit_bytes=60 * 2**20),
            )(c.reshape(1), du, w))
        part = {}
        part.update(pdn((1, 2)))
        part.update(pdn((0,)))
        de = zeros(0, ZERO_FIRST)
        d0, d1 = ([swap(diag[q][h], bit) for q in range(2)] for h, bit in ((0, 2), (1, 4)))
        ex, ey = swap(part[1][0], 2), swap(part[2][1], 4)
        tgt = jnp.where(own, 2 * (jnp.arange(n) % tc) + (loc & 1), -1).astype(jnp.int32)
        i0 = lax.broadcasted_iota(jnp.int32, (n, n), 0)
        i1 = lax.broadcasted_iota(jnp.int32, (n, n), 1)

        def by_piece(v):
            v = v.reshape(mb, 2, 2, 2, tl)
            for ax, bit in ((1, 4), (2, 2), (3, 1)):
                v = jnp.where((r & bit) > 0, jnp.flip(v, ax), v)
            return v.reshape(2, mb // 2, groups, tl).transpose(2, 0, 1, 3).reshape(-1)

        flat_p = by_piece(ids)
        loc_p = flat_p - r * vl
        own_p = (loc_p >= 0) & (loc_p < vl)
        first = jnp.min(jnp.where(flat_p[:, None] == flat_p[None, :], i0, n), axis=0)
        lead = own_p & (first == jnp.arange(n))
        pos = jnp.sum(jnp.where(lead[:, None] & (i0 < i1), 1, 0), axis=0)
        pos_of_first = jnp.sum(jnp.where((i0 == first[None, :]), pos[:, None], 0), axis=0)
        slot = jnp.where(own_p, pos_of_first, -1).astype(jnp.int32)
        rows = jnp.sum(jnp.where(lead[:, None] & (pos[:, None] == i1), loc_p[:, None], 0), axis=0).astype(jnp.int32)
        cnt = jnp.sum(lead.astype(jnp.int32)).reshape(1)
        n_owned = jnp.sum(own.astype(jnp.int32)).reshape(1)
        own_pos = jnp.sum(jnp.where(own[:, None] & (i0 < i1), 1, 0), axis=0)
        owned = jnp.sum(jnp.where(own[:, None] & (own_pos[:, None] == i1), i0, 0), axis=0).astype(jnp.int32)
        d0, d1, loc, tgt, slot, rows, cnt, owned, n_owned = lax.optimization_barrier(
            (d0, d1, loc, tgt, slot, rows, cnt, owned, n_owned)
        )

        def relay(mine, far, bit):
            left, right = f32(mine[..., :hd]) + f32(far[0]), f32(mine[..., hd:]) + f32(far[1])
            got = swap(pick(right, left), 1)
            return swap(pick(left, right) + got, bit)

        fy, fx = relay(part[2][0], d0, 4), relay(part[1][1], d1, 2)

        mine, far, near, de = pl.pallas_call(
            lookup_kernel,
            out_shape=(half_shape(4), half_shape(1), half_shape(3), de_shape),
            in_specs=[SMEM, SMEM, SMEM, SMEM, VMEM, ANY, ANY],
            input_output_aliases={6: 3},
            out_specs=(VMEM, VMEM, VMEM, ANY),
            scratch_shapes=[pltpu.VMEM((2 * n, d), jnp.bfloat16), pltpu.SemaphoreType.DMA] + zero_scratch,
            cost_estimate=pl.CostEstimate(flops=40_000_000, bytes_accessed=60_000_000, transcendentals=0),
            compiler_params=pltpu.CompilerParams(vmem_limit_bytes=22 * 2**20),
            name="look",
        )(kc, owned, n_owned, loc, tgt.reshape(n, 1), emb, de)
        de = zeros(LOOKUP_SHARE, ZERO_A, de)
        de = zeros(ZERO_A, ZERO_B, de)
        far, near = swap(far, 1), swap(near, 1)
        xpairs = {j: (mine[j], far[0] if j == 3 else near[j]) for j in range(4)}

        def widen(v):
            return to_rows(v, jnp.zeros_like(v))

        v0 = f32(part[0][0]) + f32(ex) + widen(fy)
        v1 = f32(part[0][1]) + f32(ey) + widen(fx)
        dn = pick(v0, v1) + swap(pick(v1, v0), 1)
        x0, x1 = reduce_to_home(xpairs, jnp.bfloat16)
        xo = gather_all((x0, x1))
        x = to_rows(jnp.where(k == 0, x0, x1), jnp.where(k == 0, xo[1][0], xo[1][1]))

        ns, u = [], None
        for j in range(4):
            more = (de,) if u is None else (u, de)
            nj, u, de = pl.pallas_call(
                functools.partial(norm_kernel, j),
                out_shape=(jax.ShapeDtypeStruct((d, mb * tc), jnp.bfloat16), jax.ShapeDtypeStruct((mb, t, f), jnp.bfloat16), de_shape),
                in_specs=[SMEM] + [VMEM] * 6 + [ANY] * len(more),
                out_specs=(VMEM, ANY, ANY),
                scratch_shapes=[
                    pltpu.VMEM((mb * tc, d), jnp.bfloat16),
                    pltpu.VMEM((mb, tc, f), jnp.bfloat16),
                    pltpu.SemaphoreType.DMA,
                ] + zero_scratch,
                input_output_aliases={7 + i: 3 - len(more) + i for i in range(len(more))},
                cost_estimate=pl.CostEstimate(flops=8_000_000, bytes_accessed=12_000_000, transcendentals=0),
                compiler_params=pltpu.CompilerParams(vmem_limit_bytes=14 * 2**20),
            )(kc, g.reshape(1, d), w, *(xo[2 * j + q][h] for h in range(2) for q in range(2)), *more)
            ns.append(nj)
        dw = pl.pallas_call(
            dw_kernel,
            out_shape=jax.ShapeDtypeStruct((d, f), jnp.float32),
            in_specs=[SMEM] + [VMEM] * 5,
            out_specs=ANY,
            scratch_shapes=[
                pltpu.VMEM((n, f), jnp.bfloat16),
                pltpu.VMEM((2, 512, f), jnp.float32),
                pltpu.SemaphoreType.DMA((2,)),
            ],
            cost_estimate=pl.CostEstimate(flops=30_000_000, bytes_accessed=40_000_000, transcendentals=0),
            compiler_params=pltpu.CompilerParams(vmem_limit_bytes=16 * 2**20),
            name="dw",
        )(c.reshape(1), du, *ns)

        xf = x.astype(jnp.float32)
        rs = lax.rsqrt(jnp.mean(xf * xf, axis=-1, keepdims=True) + EPS)
        nh = xf * rs
        gdn = gf * dn
        dxn = rs * (gdn - nh * jnp.mean(nh * gdn, axis=-1, keepdims=True))
        dx = (dres.astype(jnp.float32) + dxn).astype(jnp.bfloat16)
        dg = jnp.sum(dn * nh, axis=(0, 1))
        dxo = gather_all((dx[:mb // 2], dx[mb // 2:]))
        dxs = [b for j in range(8) for b in dxo[j]]
        for bit in (1, 2, 4):
            dg = dg + swap(dg, bit)

        de = pl.pallas_call(
            scatter_kernel,
            out_shape=de_shape,
            in_specs=[SMEM, SMEM, VMEM] + [VMEM] * 16 + [ANY],
            out_specs=ANY,
            scratch_shapes=[
                pltpu.VMEM((BLK, d), jnp.float32),
                pltpu.SemaphoreType.DMA,
            ],
            input_output_aliases={19: 0},
            compiler_params=pltpu.CompilerParams(vmem_limit_bytes=28 * 2**20),
            name="put",
        )(rows, cnt, slot.reshape(1, n), *dxs, de)
        return u, x, de, dw, dg

    return jax.shard_map(
        local,
        mesh=mesh,
        in_specs=(P("dp", None), P("tp", None), P(None), P(None, "tp"), P("dp", None, "tp"), P("dp", "tp", None)),
        out_specs=(P("dp", None, "tp"), P("dp", "tp", None), P(("dp", "tp"), None), P(None, ("dp", "tp")), P("dp")),
        check_vma=False,
    )
```

```python
import functools

import jax
import jax.numpy as jnp
from jax import lax
from jax.experimental import pallas as pl
from jax.experimental.pallas import tpu as pltpu
from jax.sharding import PartitionSpec as P

EPS = 1e-6
ANY = pl.BlockSpec(memory_space=pl.ANY)
VMEM = pl.BlockSpec(memory_space=pltpu.VMEM)
SMEM = pl.BlockSpec(memory_space=pltpu.SMEM)
HBM = pl.BlockSpec(memory_space=pltpu.HBM)
ZR = 128
BLK = 256
LOOKUP_EARLY, LOOKUP_SHARE, ZERO_A, ZERO_B, NORM_SHARE = 8, 22, 34, 52, 3


def zero_fill(de, z, sem, first, last):

    def copy(i):
        return pltpu.make_async_copy(z, de.at[pl.ds(pl.multiple_of(i * ZR, ZR), ZR)], sem)

    def start(clear=True):
        if clear:
            z[...] = jnp.zeros_like(z)
        pl.loop(first, last)(lambda i: copy(i).start())

    def wait():
        pl.loop(first, last)(lambda i: copy(i).wait())

    return start, wait


def zero_kernel(first, last, de_in, de, z, sem):
    del de_in
    start, wait = zero_fill(de, z, sem, first, last)
    start()
    wait()


def pdn_first_kernel(j, c_ref, du_hbm, w_hbm, h0, h1, du_ref, w_ref, sem, wsem):
    c = c_ref[0]
    mb, tc, _ = du_ref.shape
    tl = tc // 2
    wc = 512
    steps = w_hbm.shape[0] // wc
    z = pl.multiple_of(jnp.bitwise_xor(c, j) * tc, tc)
    rows_in = pltpu.make_async_copy(du_hbm.at[:, pl.ds(z, tc), :], du_ref, sem)
    rows_in.start()
    loads = [pltpu.make_async_copy(w_hbm.at[pl.ds(n * wc, wc)], w_ref.at[pl.ds(n * wc, wc)], wsem.at[n]) for n in range(steps)]
    for cp in loads[:3]:
        cp.start()
    rows_in.wait()
    rows = du_ref[...].reshape(mb * tc, du_ref.shape[2])
    for n in range(steps):
        loads[n].wait()
        if n + 3 < steps:
            loads[n + 3].start()
        cols = slice(n * wc, (n + 1) * wc)
        v = lax.dot_general(rows, w_ref[cols, :], (((1,), (1,)), ((), ())), preferred_element_type=jnp.float32)
        v = v.astype(jnp.bfloat16).reshape(mb, tc, wc)
        h0[:, :, cols] = v[:, :tl]
        h1[:, :, cols] = v[:, tl:]


def pdn_kernel(js, c_ref, du_ref, w_ref, *outs):
    c = c_ref[0]
    mb, t, _ = du_ref.shape
    tc, wc = t // 4, 512
    tl = tc // 2
    for i, j in enumerate(js):
        z = pl.multiple_of(jnp.bitwise_xor(c, j) * tc, tc)
        rows = jnp.concatenate([du_ref[m, pl.ds(z, tc), :] for m in range(mb)], axis=0)
        for n in range(w_ref.shape[0] // wc):
            cols = slice(n * wc, (n + 1) * wc)
            v = lax.dot_general(rows, w_ref[cols, :], (((1,), (1,)), ((), ())), preferred_element_type=jnp.float32)
            v = v.astype(jnp.bfloat16).reshape(mb, tc, wc)
            for h in range(2):
                outs[2 * i + h][:, :, cols] = v[:, h * tl:(h + 1) * tl]


def lookup_kernel(kc_ref, list_ref, cnt_ref, loc_ref, tgt_ref, emb, mine_ref, far_ref, near_ref, de, buf, sem, z, zsem):
    k, c = kc_ref[0], kc_ref[1]
    _, d = emb.shape
    nj, mb, tc, hd = mine_ref.shape
    n = nj * mb * tc
    step = 64
    start, wait = zero_fill(de, z, zsem, 0, LOOKUP_EARLY)
    late_start, late_wait = zero_fill(de, z, zsem, LOOKUP_EARLY, LOOKUP_SHARE)
    start()

    @pl.loop(0, 2 * n // step)
    def _(i):
        buf[pl.ds(pl.multiple_of(i * step, step), step), :] = jnp.zeros((step, d), buf.dtype)

    def copy(t, l):
        src = emb.at[pl.ds(pl.multiple_of((l >> 1) * 2, 2), 2)]
        return pltpu.make_async_copy(src, buf.at[pl.ds(pl.multiple_of(t * 2, 2), 2)], sem)

    cnt = cnt_ref[0]

    @pl.loop(0, cnt)
    def _(q):
        t = list_ref[q]
        copy(t, loc_ref[t]).start()

    @pl.loop(0, cnt)
    def _(i):
        copy(0, 0).wait()

    late_start(False)

    for j in range(nj):
        theirs = far_ref.at[0] if j == 3 else near_ref.at[j]
        zc = jnp.bitwise_xor(c, j)

        @pl.loop(0, mb)
        def _(m):
            t0 = m * (nj * tc) + zc * tc
            tgt = tgt_ref[pl.ds(pl.multiple_of(t0, tc), tc), :]
            sel = (lax.broadcasted_iota(jnp.int32, (tc, 2 * tc), 1) == tgt).astype(jnp.bfloat16)
            rows = pl.ds(pl.multiple_of(2 * t0, 2 * tc), 2 * tc)
            for out, half in ((theirs, 1 - k), (mine_ref.at[j], k)):
                v = buf[rows, pl.ds(pl.multiple_of(half * hd, 128), hd)]
                out[m] = jnp.dot(sel, v, preferred_element_type=jnp.float32).astype(jnp.bfloat16)

    wait()
    late_wait()


def norm_kernel(j, kc_ref, g_ref, w_ref, *refs):
    blocks, (nt_ref, u_ref, de, n_ref, stage, sem, z, zsem) = refs[:4], refs[-8:]
    k = kc_ref[0]
    d = nt_ref.shape[0]
    mb, tl, hd = blocks[0].shape
    tc = 2 * tl
    first = ZERO_B + j * NORM_SHARE
    start, wait = zero_fill(de, z, zsem, first, first + NORM_SHARE)
    start()
    at = [pl.ds(pl.multiple_of(jnp.bitwise_xor(k, q) * hd, 128), hd) for q in range(2)]
    gf = [g_ref[:, at[q]].astype(jnp.float32) for q in range(2)]

    @pl.loop(0, mb)
    def _(m):
        for h in range(2):
            xf = [blocks[2 * h + q][m].astype(jnp.float32) for q in range(2)]
            total = sum(jnp.sum(v * v, axis=-1, keepdims=True) for v in xf)
            rs = lax.rsqrt(total * (1.0 / d) + EPS)
            for q in range(2):
                to = pl.ds(pl.multiple_of(m * tc + h * tl, tl), tl)
                n_ref[to, at[q]] = (xf[q] * rs * gf[q]).astype(jnp.bfloat16)

    v = jnp.dot(n_ref[...], w_ref[...], preferred_element_type=jnp.float32)
    stage[...] = v.astype(jnp.bfloat16).reshape(stage.shape)
    rows = pl.ds(pl.multiple_of(jnp.bitwise_xor(kc_ref[1], j) * tc, tc), tc)
    copy = pltpu.make_async_copy(stage, u_ref.at[:, rows, :], sem)
    copy.start()
    wc = 512

    @pl.loop(0, d // wc)
    def _(i):
        c = pl.ds(pl.multiple_of(i * wc, wc), wc)
        nt_ref[c, :] = n_ref[:, c].T

    copy.wait()
    wait()


def dw_kernel(c_ref, du_ref, *refs):
    ns, (dw, de, right, stage, sem, z, zsem) = refs[:4], refs[-7:]
    mb, _, _ = du_ref.shape
    d, kj = ns[0].shape
    tc = kj // mb
    start, wait = zero_fill(de, z, zsem, ZERO_B + 4 * NORM_SHARE, de.shape[0] // ZR)
    start()
    for j in range(4):
        rows = pl.ds(pl.multiple_of(jnp.bitwise_xor(c_ref[0], j) * tc, tc), tc)
        for m in range(mb):
            right[j * kj + m * tc:j * kj + (m + 1) * tc, :] = du_ref[m, rows, :]
    dc = stage.shape[1]

    def copy(i, q):
        return pltpu.make_async_copy(stage.at[q], dw.at[pl.ds(pl.multiple_of(i * dc, dc), dc)], sem.at[q])

    @pl.loop(0, d // dc)
    def _(i):
        q = lax.rem(i, 2)

        @pl.when(i >= 2)
        def _():
            copy(i - 2, q).wait()

        c = pl.ds(pl.multiple_of(i * dc, dc), dc)
        left = jnp.concatenate([n[c, :] for n in ns], axis=1)
        stage[q] = jnp.dot(left, right[...], preferred_element_type=jnp.float32)
        copy(i, q).start()

    for q in range(2):
        copy(d // dc - 2 + q, q).wait()
    wait()


def scatter_kernel(rows_ref, cnt_ref, slot_ref, *refs):
    blocks, (de, stage, out_sem) = refs[:16], refs[-3:]
    hb, tl, d = blocks[0].shape
    kb = hb * tl
    cnt = cnt_ref[0]
    cc = 512

    def copy(q, r, size=1):
        return pltpu.make_async_copy(stage.at[pl.ds(q, size)], de.at[pl.ds(r, size)], out_sem)

    @pl.loop(0, (cnt + BLK - 1) // BLK)
    def _(b):
        base = b * BLK
        ids = lax.broadcasted_iota(jnp.int32, (BLK, len(blocks) * kb), 0) + base
        oh = (ids == slot_ref[...]).astype(jnp.bfloat16)
        for i in range(d // cc):
            cols = slice(i * cc, (i + 1) * cc)
            right = jnp.concatenate([v[:, :, cols].reshape(kb, cc) for v in blocks], axis=0)
            stage[:, cols] = jnp.dot(oh, right, preferred_element_type=jnp.float32)
        n = jnp.minimum(cnt - base, BLK)
        full = n // 8

        @pl.loop(0, full)
        def _(i):
            for u in range(8):
                copy(i * 8 + u, rows_ref[base + i * 8 + u]).start()

        pl.loop(full * 8, n)(lambda q: copy(q, rows_ref[base + q]).start())
        for bit in range(9):

            @pl.when((n >> bit) & 1 == 1)
            def _():
                copy(0, 0, 1 << bit).wait()


def solution(mesh):
    groups = mesh.shape["tp"]

    def swap(v, bit):
        return lax.ppermute(v, "tp", [(i, i ^ bit) for i in range(groups)])

    def local(ids, emb, g, w, du, dres):
        r = lax.axis_index("tp")
        mb, t = ids.shape
        vl, d = emb.shape
        f = w.shape[1]
        tl = t // groups
        hd = d // 2
        tc = t // 4
        k, c = r & 1, r >> 1
        gf = g.astype(jnp.float32)
        kc = jnp.stack([k, c]).astype(jnp.int32)
        de_shape = jax.ShapeDtypeStruct((vl, d), jnp.float32)
        zero_scratch = [pltpu.VMEM((ZR, d), jnp.float32), pltpu.SemaphoreType.DMA]

        def half_shape(nj):
            return jax.ShapeDtypeStruct((nj, mb, tc, hd), jnp.bfloat16)

        def pdn(js):
            out = pl.pallas_call(
                functools.partial(pdn_kernel, js),
                out_shape=(jax.ShapeDtypeStruct((mb, tl, d), jnp.bfloat16),) * (2 * len(js)),
                in_specs=[SMEM, VMEM, VMEM],
                out_specs=(VMEM,) * (2 * len(js)),
                cost_estimate=pl.CostEstimate(flops=5_000_000 * len(js), bytes_accessed=8_000_000, transcendentals=0),
                compiler_params=pltpu.CompilerParams(vmem_limit_bytes=20 * 2**20),
            )(c.reshape(1), du, w)
            return {j: out[2 * i:2 * i + 2] for i, j in enumerate(js)}

        def pick(a, b):
            return jnp.where(k == 0, a, b)

        def f32(v):
            return v.astype(jnp.float32)

        def reduce_to_home(pairs, dt):
            def part(j, h):
                a, b = pairs[j]
                return a[:, h * tl:(h + 1) * tl].astype(dt) + b[:, h * tl:(h + 1) * tl].astype(dt)

            dx_ = swap(part(3, 0), 2)
            dy_ = swap(part(3, 1), 4)
            ex = swap(part(1, 0), 2)
            ey = swap(part(2, 1), 4)
            pairs = dict(pairs)
            pairs[2], dx_ = lax.optimization_barrier((pairs[2], dx_))
            pairs[1], dy_ = lax.optimization_barrier((pairs[1], dy_))
            fy = swap(part(2, 0) + dx_, 4)
            fx = swap(part(1, 1) + dy_, 2)
            pairs[0], ex, ey = lax.optimization_barrier((pairs[0], ex, ey))
            return part(0, 0) + ex + fy, part(0, 1) + ey + fx

        def to_rows(mine, other):
            return jnp.where(k == 0, jnp.concatenate([mine, other], -1), jnp.concatenate([other, mine], -1))

        def gather_all(own):
            x1, y0 = swap(own[1], 2), swap(own[0], 4)
            x0, y1 = swap(own[0], 2), swap(own[1], 4)
            d1, d0 = swap(x1, 4), swap(y0, 2)
            out = {0: own, 2: (x0, x1), 4: (y0, y1), 6: (d0, d1)}
            for j in (0, 2, 4, 6):
                out[j + 1] = tuple(swap(b, 1) for b in out[j])
            return out

        flat = ids.reshape(-1)
        n = flat.shape[0]
        loc = flat - r * vl
        own = (loc >= 0) & (loc < vl)
        part = {3: pl.pallas_call(
            functools.partial(pdn_first_kernel, 3),
            out_shape=(jax.ShapeDtypeStruct((mb, tl, d), jnp.bfloat16),) * 2,
            in_specs=[SMEM, HBM, HBM],
            out_specs=(VMEM, VMEM),
            scratch_shapes=[
                pltpu.VMEM((mb, tc, f), jnp.bfloat16),
                pltpu.VMEM((d, f), jnp.bfloat16),
                pltpu.SemaphoreType.DMA,
                pltpu.SemaphoreType.DMA((6,)),
            ],
            cost_estimate=pl.CostEstimate(flops=5_000_000, bytes_accessed=8_000_000, transcendentals=0),
            compiler_params=pltpu.CompilerParams(vmem_limit_bytes=60 * 2**20),
            name="pa",
        )(c.reshape(1), du, w)}
        part.update(pdn((1, 2)))
        part.update(pdn((0,)))
        d0, d1 = swap(part[3][0], 2), swap(part[3][1], 4)
        ex, ey = swap(part[1][0], 2), swap(part[2][1], 4)
        tgt = jnp.where(own, 2 * (jnp.arange(n) % tc) + (loc & 1), -1).astype(jnp.int32)
        i0 = lax.broadcasted_iota(jnp.int32, (n, n), 0)
        i1 = lax.broadcasted_iota(jnp.int32, (n, n), 1)

        def by_piece(v):
            v = v.reshape(mb, 2, 2, 2, tl)
            for ax, bit in ((1, 4), (2, 2), (3, 1)):
                v = jnp.where((r & bit) > 0, jnp.flip(v, ax), v)
            return v.reshape(2, mb // 2, groups, tl).transpose(2, 0, 1, 3).reshape(-1)

        flat_p = by_piece(ids)
        loc_p = flat_p - r * vl
        own_p = (loc_p >= 0) & (loc_p < vl)
        first = jnp.min(jnp.where(flat_p[:, None] == flat_p[None, :], i0, n), axis=0)
        lead = own_p & (first == jnp.arange(n))
        pos = jnp.sum(jnp.where(lead[:, None] & (i0 < i1), 1, 0), axis=0)
        pos_of_first = jnp.sum(jnp.where((i0 == first[None, :]), pos[:, None], 0), axis=0)
        slot = jnp.where(own_p, pos_of_first, -1).astype(jnp.int32)
        rows = jnp.sum(jnp.where(lead[:, None] & (pos[:, None] == i1), loc_p[:, None], 0), axis=0).astype(jnp.int32)
        cnt = jnp.sum(lead.astype(jnp.int32)).reshape(1)
        n_owned = jnp.sum(own.astype(jnp.int32)).reshape(1)
        own_pos = jnp.sum(jnp.where(own[:, None] & (i0 < i1), 1, 0), axis=0)
        owned = jnp.sum(jnp.where(own[:, None] & (own_pos[:, None] == i1), i0, 0), axis=0).astype(jnp.int32)
        d0, d1, loc, tgt, slot, rows, cnt, owned, n_owned = lax.optimization_barrier(
            (d0, d1, loc, tgt, slot, rows, cnt, owned, n_owned)
        )
        ty, tx = f32(part[2][0]) + f32(d0), f32(part[1][1]) + f32(d1)
        gy = swap(pick(ty[..., hd:], ty[..., :hd]), 1)
        gx = swap(pick(tx[..., hd:], tx[..., :hd]), 1)
        fy = swap(pick(ty[..., :hd], ty[..., hd:]) + gy, 4)
        fx = swap(pick(tx[..., :hd], tx[..., hd:]) + gx, 2)

        mine, far, near, de = pl.pallas_call(
            lookup_kernel,
            out_shape=(half_shape(4), half_shape(1), half_shape(3), de_shape),
            in_specs=[SMEM, SMEM, SMEM, SMEM, VMEM, ANY],
            out_specs=(VMEM, VMEM, VMEM, ANY),
            scratch_shapes=[pltpu.VMEM((2 * n, d), jnp.bfloat16), pltpu.SemaphoreType.DMA] + zero_scratch,
            cost_estimate=pl.CostEstimate(flops=40_000_000, bytes_accessed=60_000_000, transcendentals=0),
            compiler_params=pltpu.CompilerParams(vmem_limit_bytes=32 * 2**20),
            name="look",
        )(kc, owned, n_owned, loc, tgt.reshape(n, 1), emb)
        for first, last in ((LOOKUP_SHARE, ZERO_A), (ZERO_A, ZERO_B)):
            de = pl.pallas_call(
                functools.partial(zero_kernel, first, last),
                out_shape=de_shape,
                in_specs=[ANY],
                out_specs=ANY,
                scratch_shapes=zero_scratch,
                input_output_aliases={0: 0},
                cost_estimate=pl.CostEstimate(flops=10_000_000, bytes_accessed=20_000_000, transcendentals=0),
                compiler_params=pltpu.CompilerParams(vmem_limit_bytes=4 * 2**20),
            )(de)
        far, near = swap(far, 1), swap(near, 1)
        xpairs = {j: (mine[j], far[0] if j == 3 else near[j]) for j in range(4)}

        def widen(v):
            o = jnp.zeros_like(v)
            return to_rows(v, o)

        v0 = f32(part[0][0]) + f32(ex) + widen(fy)
        v1 = f32(part[0][1]) + f32(ey) + widen(fx)
        dn = pick(v0, v1) + swap(pick(v1, v0), 1)
        x0, x1 = reduce_to_home(xpairs, jnp.bfloat16)
        xo = gather_all((x0, x1))
        x = to_rows(jnp.where(k == 0, x0, x1), jnp.where(k == 0, xo[1][0], xo[1][1]))

        ns, u = [], None
        for j in range(4):
            more = (de,) if u is None else (u, de)
            nj, u, de = pl.pallas_call(
                functools.partial(norm_kernel, j),
                out_shape=(jax.ShapeDtypeStruct((d, mb * tc), jnp.bfloat16), jax.ShapeDtypeStruct((mb, t, f), jnp.bfloat16), de_shape),
                in_specs=[SMEM] + [VMEM] * 6 + [ANY] * len(more),
                out_specs=(VMEM, ANY, ANY),
                scratch_shapes=[
                    pltpu.VMEM((mb * tc, d), jnp.bfloat16),
                    pltpu.VMEM((mb, tc, f), jnp.bfloat16),
                    pltpu.SemaphoreType.DMA,
                ] + zero_scratch,
                input_output_aliases={7 + i: 3 - len(more) + i for i in range(len(more))},
                cost_estimate=pl.CostEstimate(flops=8_000_000, bytes_accessed=12_000_000, transcendentals=0),
                compiler_params=pltpu.CompilerParams(vmem_limit_bytes=24 * 2**20),
            )(kc, g.reshape(1, d), w, *(xo[2 * j + q][h] for h in range(2) for q in range(2)), *more)
            ns.append(nj)
        dw, de = pl.pallas_call(
            dw_kernel,
            out_shape=(jax.ShapeDtypeStruct((d, f), jnp.float32), de_shape),
            in_specs=[SMEM] + [VMEM] * 5 + [ANY],
            out_specs=(ANY, ANY),
            scratch_shapes=[
                pltpu.VMEM((n, f), jnp.bfloat16),
                pltpu.VMEM((2, 512, f), jnp.float32),
                pltpu.SemaphoreType.DMA((2,)),
            ] + zero_scratch,
            input_output_aliases={6: 1},
            cost_estimate=pl.CostEstimate(flops=30_000_000, bytes_accessed=40_000_000, transcendentals=0),
            compiler_params=pltpu.CompilerParams(vmem_limit_bytes=24 * 2**20),
            name="dw",
        )(c.reshape(1), du, *ns, de)

        xf = x.astype(jnp.float32)
        rs = lax.rsqrt(jnp.mean(xf * xf, axis=-1, keepdims=True) + EPS)
        nh = xf * rs
        gdn = gf * dn
        dxn = rs * (gdn - nh * jnp.mean(nh * gdn, axis=-1, keepdims=True))
        dx = (dres.astype(jnp.float32) + dxn).astype(jnp.bfloat16)
        dg = jnp.sum(dn * nh, axis=(0, 1))
        dxo = gather_all((dx[:mb // 2], dx[mb // 2:]))
        dxs = [b for j in range(8) for b in dxo[j]]
        for bit in (1, 2, 4):
            dg = dg + swap(dg, bit)

        de = pl.pallas_call(
            scatter_kernel,
            out_shape=de_shape,
            in_specs=[SMEM, SMEM, VMEM] + [VMEM] * 16 + [ANY],
            out_specs=ANY,
            scratch_shapes=[
                pltpu.VMEM((BLK, d), jnp.float32),
                pltpu.SemaphoreType.DMA,
            ],
            input_output_aliases={19: 0},
            compiler_params=pltpu.CompilerParams(vmem_limit_bytes=28 * 2**20),
            name="put",
        )(rows, cnt, slot.reshape(1, n), *dxs, de)
        return u, x, de, dw, dg

    return jax.shard_map(
        local,
        mesh=mesh,
        in_specs=(P("dp", None), P("tp", None), P(None), P(None, "tp"), P("dp", None, "tp"), P("dp", "tp", None)),
        out_specs=(P("dp", None, "tp"), P("dp", "tp", None), P(("dp", "tp"), None), P(None, ("dp", "tp")), P("dp")),
        check_vma=False,
    )
```
